32 devices in a mesh: gx: 16 (over z, y, x), gy: 2 (over core).
Axes of the slice: x: 2, y: 2, z: 4, core: 2. Of those that a mesh axis runs over, the one named last changes fastest.
Arguments:
- moisture_ratio: float32 [2, 128, 256], P(None, 'gx', 'gy'), may hold values from 11 to 14
- kelvin_warmth: float32 [2, 128, 256], P(None, 'gx', 'gy'), may hold values from 286 to 292
- droplet_size_micron: float32 [8, 2, 128, 256], P(None, None, 'gx', 'gy'), may hold values from 0.5 to 25
- weighting_factor: float32 [8, 2, 128, 256], P(None, None, 'gx', 'gy'), may hold values from 0.1 to 2
- dry_nucleus_size: float32 [8, 2, 128, 256], P(None, None, 'gx', 'gy'), may hold values from 0.02 to 0.3
- fractional_offset_east: float32 [8, 2, 128, 256], P(None, None, 'gx', 'gy'), may hold values from 0 to 1
- fractional_offset_north: float32 [8, 2, 128, 256], P(None, None, 'gx', 'gy'), may hold values from 0 to 1
- encounter_permutation: int32 [8, 2, 128, 256], P(None, None, 'gx', 'gy'), may hold values from 0 to 7, as said below
- departing_eastwest_lists: int32 [16, 2, 2048], P('gx', None, 'gy'), may hold values from -1 to 16383, as said below
- departing_northsouth_lists: int32 [16, 2, 96], P('gx', None, 'gy'), may hold values from -1 to 16383, as said below
- departing_diagonal_lists: int32 [16, 4, 16], P('gx', None, 'gy'), may hold values from -1 to 16383, as said below
Outputs:
- resulting_moisture_ratio: float32 [2, 128, 256], P(None, 'gx', 'gy')
- resulting_kelvin_value: float32 [2, 128, 256], P(None, 'gx', 'gy')
- resulting_droplet_size: float32 [8, 2, 128, 256], P(None, None, 'gx', 'gy')
- resulting_weighting_factor: float32 [8, 2, 128, 256], P(None, None, 'gx', 'gy')
- arrival_particle_records: float32 [5, 16, 4352], P(None, 'gx', 'gy')
- arrival_box_index: int32 [16, 4352], P('gx', 'gy')
The draws below stay inside these ranges and needn't reach their ends.
Inputs may be any that keep to these rules, and one draw needn't show every extreme that they name: `encounter_permutation`: along the first dimension, the 8 entries of each cell are a permutation of 0 to 7. `departing_eastwest_lists`: each list holds live slot numbers of its own device first and -1 after them, at most 1024 live, and some list of some device is full. Row 0 names only droplets of cells with i = 7, row 1 only i = 0, both only 0 < j < 127. No slot is named twice among all lists of a device. `departing_northsouth_lists`: each list holds live slot numbers of its own device first and -1 after them, at most 48 live, and some list of some device is full. Row 0 names only droplets of cells with j = 127, row 1 only j = 0, both only 0 < i < 7. `departing_diagonal_lists`: each list holds live slot numbers of its own device first and -1 after them, at most 8 live, and some list of some device is full. Row r names only droplets of the corner cell that its move points to: i = 7 for rows 0 and 1, i = 0 for rows 2 and 3, j = 127 for rows 0 and 2, j = 0 for rows 1 and 3.
All inputs are finite; a program needn't handle non-finite values.
Results may differ from the reference program's by a relative error of at most 0.0003.
Values sent between devices are 32-bit elements; how exact they have to be, the bound alone decides.
A program may use at most 64 MiB of HBM per device.

```python
import math
import jax
import jax.numpy as jnp
from jax import lax

NUMBER_OF_TIERS = 2
SD = 8
NEWTON = 4
CX = 8
CY = 128
GRID_WIDTH_EAST = 128
GRID_WIDTH_NORTH = 256
DROPS = 16384
KX = 1024
KY = 48
KC = 8
NARR = 2176
N_GX = 16
N_GY = 2


def draw_lists(key, list_rows, list_length, eligible, slot_of):
    grid_x = GRID_WIDTH_EAST // CX
    grid_y = GRID_WIDTH_NORTH // CY
    total_lists = grid_x * list_rows * grid_y
    keys = jax.random.split(key, total_lists)
    chosen = jax.vmap(lambda single: jax.random.permutation(single, eligible)[:list_length])(keys)
    chosen = chosen.reshape(grid_x, list_rows, grid_y, list_length).astype(jnp.int32)
    direction = lax.broadcasted_iota(jnp.int32, chosen.shape, 1)
    slots = slot_of(chosen, direction).astype(jnp.int32)
    live_count = jax.random.randint(jax.random.fold_in(key, 1), (grid_x, list_rows, grid_y, 1), list_length // 4, list_length + 1)
    fullest = jax.random.randint(jax.random.fold_in(key, 2), (), 0, total_lists)
    list_id = (lax.broadcasted_iota(jnp.int32, live_count.shape, 0) * list_rows + lax.broadcasted_iota(jnp.int32, live_count.shape, 1)) * grid_y + lax.broadcasted_iota(jnp.int32, live_count.shape, 2)
    live_count = jnp.where(list_id == fullest, list_length, live_count)
    position = lax.broadcasted_iota(jnp.int32, chosen.shape, 3)
    result = jnp.where(position < live_count, slots, -1)
    return result.reshape(grid_x, list_rows, grid_y * list_length).astype(jnp.int32)


def draw_departing_eastwest_lists(key, part):
    inner_width = CY - 2

    def slot_of(chosen, direction):
        stack_level = chosen // inner_width
        index_y = chosen % inner_width + 1
        index_x = jnp.where(direction == 0, CX - 1, 0)
        return (stack_level * CX + index_x) * CY + index_y
    return draw_lists(jax.random.fold_in(key, 11), 2, KX, SD * NUMBER_OF_TIERS * inner_width, slot_of)


def draw_departing_northsouth_lists(key, part):
    inner_width = CX - 2

    def slot_of(chosen, direction):
        stack_level = chosen // inner_width
        index_x = chosen % inner_width + 1
        index_y = jnp.where(direction == 0, CY - 1, 0)
        return (stack_level * CX + index_x) * CY + index_y
    return draw_lists(jax.random.fold_in(key, 12), 2, KY, SD * NUMBER_OF_TIERS * inner_width, slot_of)


def draw_departing_diagonal_lists(key, part):

    def slot_of(chosen, direction):
        index_x = jnp.where(direction < 2, CX - 1, 0)
        index_y = jnp.where(direction % 2 == 0, CY - 1, 0)
        return (chosen * CX + index_x) * CY + index_y
    return draw_lists(jax.random.fold_in(key, 13), 4, KC, SD * NUMBER_OF_TIERS, slot_of)


def draw_encounter_permutation(key, part):
    shape_all = (SD, NUMBER_OF_TIERS, GRID_WIDTH_EAST, GRID_WIDTH_NORTH)
    scores = jax.random.randint(jax.random.fold_in(key, 14), shape_all, 0, 1 << 20) * SD + lax.broadcasted_iota(jnp.int32, shape_all, 0)
    return jnp.argsort(scores, axis=0).astype(jnp.int32)


def block_scale(own_key, extent, cuts, smallest, largest):
    level = 1.0
    for axis_at, blocks in cuts:
        steps = jax.random.uniform(jax.random.fold_in(jax.random.fold_in(own_key, 6), axis_at), (blocks,), jnp.float32, smallest / len(cuts), largest / len(cuts))
        level = level * jnp.repeat(jnp.exp(steps), extent[axis_at] // blocks).reshape((-1,) + (1,) * (len(extent) - 1 - axis_at))
    return level


def setup_inputs(seed: int = 0) -> dict:
    seeds = jax.random.split(jax.random.key(seed), 12)
    return {
        "moisture_ratio": jnp.clip(11.0 + 3.0 * jax.random.uniform(seeds[0], (NUMBER_OF_TIERS, GRID_WIDTH_EAST, GRID_WIDTH_NORTH), jnp.float32) ** block_scale(seeds[0], (NUMBER_OF_TIERS, GRID_WIDTH_EAST, GRID_WIDTH_NORTH), ((1, 16), (2, 2)), -0.2, 0.2), 11.0, 14.0),
        "kelvin_warmth": jnp.clip(286.0 + 6.0 * jax.random.uniform(seeds[1], (NUMBER_OF_TIERS, GRID_WIDTH_EAST, GRID_WIDTH_NORTH), jnp.float32) ** block_scale(seeds[1], (NUMBER_OF_TIERS, GRID_WIDTH_EAST, GRID_WIDTH_NORTH), ((1, 16), (2, 2)), -0.2, 0.2), 286.0, 292.0),
        "droplet_size_micron": jnp.clip(jnp.exp(math.log(25.0) - 3.912023 * jax.random.uniform(seeds[2], (SD, NUMBER_OF_TIERS, GRID_WIDTH_EAST, GRID_WIDTH_NORTH), jnp.float32) ** block_scale(seeds[2], (SD, NUMBER_OF_TIERS, GRID_WIDTH_EAST, GRID_WIDTH_NORTH), ((2, 16), (3, 2)), -0.2, 0.2)), 0.5, 25.0),
        "weighting_factor": jnp.clip(jnp.exp(math.log(2.0) - 2.9957323 * jax.random.uniform(seeds[3], (SD, NUMBER_OF_TIERS, GRID_WIDTH_EAST, GRID_WIDTH_NORTH), jnp.float32) ** block_scale(seeds[3], (SD, NUMBER_OF_TIERS, GRID_WIDTH_EAST, GRID_WIDTH_NORTH), ((2, 16), (3, 2)), -0.2, 0.2)), 0.1, 2.0),
        "dry_nucleus_size": jnp.clip(jnp.exp(math.log(0.3) - 2.7080503 * jax.random.uniform(seeds[4], (SD, NUMBER_OF_TIERS, GRID_WIDTH_EAST, GRID_WIDTH_NORTH), jnp.float32) ** block_scale(seeds[4], (SD, NUMBER_OF_TIERS, GRID_WIDTH_EAST, GRID_WIDTH_NORTH), ((2, 16), (3, 2)), -0.2, 0.2)), 0.02, 0.3),
        "fractional_offset_east": jnp.clip(1.0 * jax.random.uniform(seeds[5], (SD, NUMBER_OF_TIERS, GRID_WIDTH_EAST, GRID_WIDTH_NORTH), jnp.float32) ** block_scale(seeds[5], (SD, NUMBER_OF_TIERS, GRID_WIDTH_EAST, GRID_WIDTH_NORTH), ((2, 16), (3, 2)), -0.2, 0.2), 0.0, 1.0),
        "fractional_offset_north": jnp.clip(1.0 * jax.random.uniform(seeds[6], (SD, NUMBER_OF_TIERS, GRID_WIDTH_EAST, GRID_WIDTH_NORTH), jnp.float32) ** block_scale(seeds[6], (SD, NUMBER_OF_TIERS, GRID_WIDTH_EAST, GRID_WIDTH_NORTH), ((2, 16), (3, 2)), -0.2, 0.2), 0.0, 1.0),
        "encounter_permutation": draw_encounter_permutation(jax.random.fold_in(seeds[11], 71), 0),
        "departing_eastwest_lists": draw_departing_eastwest_lists(jax.random.fold_in(seeds[11], 71), 0),
        "departing_northsouth_lists": draw_departing_northsouth_lists(jax.random.fold_in(seeds[11], 71), 0),
        "departing_diagonal_lists": draw_departing_diagonal_lists(jax.random.fold_in(seeds[11], 71), 0),
    }


MIX_HORIZONTAL = 0.2
MIX_VERTICAL = 0.05
EXCESS_FACTOR = 4.2222
CURVATURE = 0.0012
KAPPA_SOLUTE = 0.6
GROWTH_STEP = 200.0
COLLIDE_RATE = 4e-07
VAPOUR_PER_SOURCE = 0.001
WARMING_FACTOR = 0.00249

def moisture_excess(moisture_ratio, kelvin_warmth):
    maximum_list_length = EXCESS_FACTOR * jnp.exp(17.27 * (kelvin_warmth - 273.15) / (kelvin_warmth - 35.86))
    return moisture_ratio / maximum_list_length - 1.0

def kernel_weights(offset):
    return (jnp.maximum(0.5 - offset, 0.0), 1.0 - jnp.abs(offset - 0.5), jnp.maximum(offset - 0.5, 0.0))

def vertical_mix(centre, level_axis):
    levels = centre.shape[level_axis]
    above = jnp.concatenate([lax.slice_in_dim(centre, 1, levels, axis=level_axis), lax.slice_in_dim(centre, levels - 1, levels, axis=level_axis)], level_axis)
    below = jnp.concatenate([lax.slice_in_dim(centre, 0, 1, axis=level_axis), lax.slice_in_dim(centre, 0, levels - 1, axis=level_axis)], level_axis)
    return above + below - 2.0 * centre

def domain_wide_stirring(field):
    horizontal = jnp.roll(field, 1, 1) + jnp.roll(field, -1, 1) + jnp.roll(field, 1, 2) + jnp.roll(field, -1, 2) - 4.0 * field
    return field + MIX_HORIZONTAL * horizontal + MIX_VERTICAL * vertical_mix(field, 0)

def grow_droplets(droplet_size_micron, dry_nucleus_size, forcing):
    initial = droplet_size_micron * droplet_size_micron
    solute = KAPPA_SOLUTE * dry_nucleus_size * dry_nucleus_size * dry_nucleus_size
    lowest = dry_nucleus_size * dry_nucleus_size
    wetted = initial
    for sweep in range(NEWTON):
        root_wet = jnp.sqrt(wetted)
        inverse = 1.0 / (wetted * root_wet)
        residue = wetted - initial - GROWTH_STEP * (forcing + solute * inverse)
        slope_value = 1.0 + 1.5 * GROWTH_STEP * solute * inverse / wetted
        wetted = jnp.maximum(wetted - residue / slope_value, lowest)
    return wetted

def coalesce(grown_radius, weighting_factor, encounter_permutation):
    ordered_radius = jnp.take_along_axis(grown_radius, encounter_permutation, axis=0)
    ordered_mult = jnp.take_along_axis(weighting_factor, encounter_permutation, axis=0)
    first_radius = ordered_radius[0::2]
    second_radius = ordered_radius[1::2]
    first_mult = ordered_mult[0::2]
    second_mult = ordered_mult[1::2]
    first_big = first_mult >= second_mult
    high_radius = jnp.where(first_big, first_radius, second_radius)
    low_radius = jnp.where(first_big, second_radius, first_radius)
    high_mult = jnp.where(first_big, first_mult, second_mult)
    low_mult = jnp.where(first_big, second_mult, first_mult)
    radius_sum = first_radius + second_radius
    kernel = COLLIDE_RATE * high_mult * radius_sum * radius_sum * jnp.abs(first_radius * first_radius - second_radius * second_radius)
    chance = 1.0 - jnp.exp(-kernel)
    merged_radius = jnp.cbrt(low_radius * low_radius * low_radius + chance * high_radius * high_radius * high_radius)
    reduced_mult = high_mult - chance * low_mult
    new_first_radius = jnp.where(first_big, high_radius, merged_radius)
    new_second_radius = jnp.where(first_big, merged_radius, high_radius)
    new_first_mult = jnp.where(first_big, reduced_mult, low_mult)
    new_second_mult = jnp.where(first_big, low_mult, reduced_mult)
    paired_radius = jnp.stack([new_first_radius, new_second_radius], 1).reshape(grown_radius.shape)
    paired_mult = jnp.stack([new_first_mult, new_second_mult], 1).reshape(grown_radius.shape)
    positions = lax.broadcasted_iota(jnp.int32, encounter_permutation.shape, 0)
    ranks = []
    for target in range(encounter_permutation.shape[0]):
        ranks.append(lax.optimization_barrier(jnp.sum(jnp.where(encounter_permutation == target, positions, 0), axis=0)))
    slot_rank = jnp.stack(ranks, 0).astype(jnp.int32)
    return (jnp.take_along_axis(paired_radius, slot_rank, axis=0), jnp.take_along_axis(paired_mult, slot_rank, axis=0))

def to_blocks(values):
    return values.reshape(SD, NUMBER_OF_TIERS, N_GX, CX, N_GY, CY).transpose(2, 4, 0, 1, 3, 5).reshape(N_GX, N_GY, DROPS)

def from_blocks(values):
    return values.reshape(N_GX, N_GY, SD, NUMBER_OF_TIERS, CX, CY).transpose(2, 3, 0, 4, 1, 5).reshape(SD, NUMBER_OF_TIERS, N_GX * CX, N_GY * CY)

def list_blocks(lists, list_rows, list_length):
    return lists.reshape(N_GX, list_rows, N_GY, list_length).transpose(0, 2, 1, 3)

def make_records(attr_table, lists, directions):
    list_rows = lists.shape[2]
    list_length = lists.shape[3]
    is_live = lists >= 0
    safe_slot = jnp.where(is_live, lists, 0).astype(jnp.int32)
    take_index = jnp.broadcast_to(safe_slot.reshape(N_GX, N_GY, 1, list_rows * list_length), (N_GX, N_GY, 5, list_rows * list_length))
    picked = jnp.take_along_axis(attr_table, take_index, axis=3)
    picked = picked.reshape(N_GX, N_GY, 5, list_rows, list_length).transpose(0, 1, 3, 2, 4)
    picked = jnp.where(is_live[:, :, :, None, :], picked, 0.0)
    cell_index = safe_slot % (NUMBER_OF_TIERS * CX * CY)
    level_index = cell_index // (CX * CY)
    index_x = cell_index // CY % CX
    index_y = cell_index % CY
    move_x = jnp.array([entry[0] for entry in directions], jnp.int32).reshape(1, 1, list_rows, 1)
    move_y = jnp.array([entry[1] for entry in directions], jnp.int32).reshape(1, 1, list_rows, 1)
    target = (level_index * CX + (index_x + move_x) % CX) * CY + (index_y + move_y) % CY
    target = jnp.where(is_live, target, -1).astype(attr_table.dtype)
    return jnp.concatenate([picked, target[:, :, :, None, :]], 3)

def reference(moisture_ratio, kelvin_warmth, droplet_size_micron, weighting_factor, dry_nucleus_size, fractional_offset_east, fractional_offset_north, encounter_permutation, departing_eastwest_lists, departing_northsouth_lists, departing_diagonal_lists):
    averaged_moisture_ratio = domain_wide_stirring(moisture_ratio)
    averaged_warmth_kelvin = domain_wide_stirring(kelvin_warmth)
    moisture_fraction = moisture_excess(averaged_moisture_ratio, averaged_warmth_kelvin)
    weight_x = kernel_weights(fractional_offset_east)
    weight_y = kernel_weights(fractional_offset_north)
    forcing = jnp.zeros_like(droplet_size_micron)
    for shift_x in range(3):
        for shift_y in range(3):
            shifted = jnp.roll(moisture_fraction, (1 - shift_x, 1 - shift_y), (1, 2))
            forcing = forcing + weight_x[shift_x] * weight_y[shift_y] * shifted[None]
    forcing = forcing - CURVATURE / droplet_size_micron
    wetted = grow_droplets(droplet_size_micron, dry_nucleus_size, forcing)
    condensed = weighting_factor * (wetted * jnp.sqrt(wetted) - droplet_size_micron * droplet_size_micron * droplet_size_micron)
    deposition_rate_term = jnp.zeros_like(moisture_ratio)
    for shift_x in range(3):
        for shift_y in range(3):
            deposit = lax.optimization_barrier(jnp.sum(weight_x[shift_x] * weight_y[shift_y] * condensed, axis=0))
            deposition_rate_term = deposition_rate_term + jnp.roll(deposit, (shift_x - 1, shift_y - 1), (1, 2))
    resulting_moisture_ratio = averaged_moisture_ratio - VAPOUR_PER_SOURCE * deposition_rate_term
    resulting_kelvin_value = averaged_warmth_kelvin + WARMING_FACTOR * deposition_rate_term
    grown_radius = jnp.sqrt(wetted)
    resulting_droplet_size, coalesced = coalesce(grown_radius, weighting_factor, encounter_permutation)
    lists_x = list_blocks(departing_eastwest_lists, 2, KX)
    lists_y = list_blocks(departing_northsouth_lists, 2, KY)
    lists_corner = list_blocks(departing_diagonal_lists, 4, KC)
    all_lists = jnp.concatenate([lists_x.reshape(N_GX, N_GY, -1), lists_y.reshape(N_GX, N_GY, -1), lists_corner.reshape(N_GX, N_GY, -1)], 2)
    grid_first = lax.broadcasted_iota(jnp.int32, all_lists.shape, 0)
    grid_second = lax.broadcasted_iota(jnp.int32, all_lists.shape, 1)
    whole_count = N_GX * N_GY * DROPS
    flat_slot = jnp.where(all_lists >= 0, (grid_first * N_GY + grid_second) * DROPS + all_lists, whole_count)
    departed = jnp.zeros((whole_count,), droplet_size_micron.dtype).at[flat_slot.reshape(-1)].set(1.0, mode='drop')
    departed = from_blocks(departed.reshape(N_GX, N_GY, DROPS))
    resulting_weighting_factor = jnp.where(departed > 0.0, 0.0, coalesced)
    attr_table = jnp.stack([to_blocks(resulting_droplet_size), to_blocks(coalesced), to_blocks(dry_nucleus_size), to_blocks(fractional_offset_east), to_blocks(fractional_offset_north)], 2)
    records_x = make_records(attr_table, lists_x, ((1, 0), (-1, 0)))
    records_y = make_records(attr_table, lists_y, ((0, 1), (0, -1)))
    records_corner = make_records(attr_table, lists_corner, ((1, 1), (1, -1), (-1, 1), (-1, -1)))
    from_west = jnp.roll(records_x[:, :, 0], 1, 0)
    from_east = jnp.roll(records_x[:, :, 1], -1, 0)
    from_south = jnp.roll(records_y[:, :, 0], 1, 1)
    from_north = jnp.roll(records_y[:, :, 1], -1, 1)
    south_west = jnp.roll(records_corner[:, :, 0], (1, 1), (0, 1))
    south_east = jnp.roll(records_corner[:, :, 2], (-1, 1), (0, 1))
    north_west = jnp.roll(records_corner[:, :, 1], (1, -1), (0, 1))
    north_east = jnp.roll(records_corner[:, :, 3], (-1, -1), (0, 1))
    arrivals = jnp.concatenate([from_west, from_east, from_south, from_north, south_west, south_east, north_west, north_east], 3)
    arrival_particle_records = arrivals[:, :, :5].transpose(2, 0, 1, 3).reshape(5, N_GX, N_GY * NARR)
    arrival_box_index = arrivals[:, :, 5].astype(jnp.int32).reshape(N_GX, N_GY * NARR)
    return (resulting_moisture_ratio, resulting_kelvin_value, resulting_droplet_size, resulting_weighting_factor, arrival_particle_records, arrival_box_index)
```

```python
import functools

import jax
import jax.numpy as jnp
from jax import lax
from jax.experimental import pallas as pl
from jax.experimental.pallas import tpu as pltpu
from jax.sharding import PartitionSpec as P

NEWTON = 4
MIX_HORIZONTAL = 0.2
MIX_VERTICAL = 0.05
EXCESS_FACTOR = 4.2222
CURVATURE = 0.0012
KAPPA_SOLUTE = 0.6
GROWTH_STEP = 200.0
COLLIDE_RATE = 4e-07
VAPOUR_PER_SOURCE = 0.001
WARMING_FACTOR = 0.00249

MESH = pl.DeviceIdType.MESH
SHIFTS = (-1, 0, 1)
MOVES = (1, -1)


def div(x, n):
    return lax.shift_right_arithmetic(x, jnp.int32(n.bit_length() - 1))


def mod(x, n):
    return lax.bitwise_and(x, jnp.int32(n - 1))


def iota(shape, dim):
    return lax.broadcasted_iota(jnp.int32, shape, dim)


def turn(x, shift, dim):
    shift %= x.shape[dim]
    return pltpu.roll(x, shift, dim) if shift else x


def kernel_weights(offset):
    return {
        -1: jnp.maximum(0.5 - offset, 0.0),
        0: 1.0 - jnp.abs(offset - 0.5),
        1: jnp.maximum(offset - 0.5, 0.0),
    }


def pieces(x):
    high = x.astype(jnp.bfloat16)
    rest = x - high.astype(jnp.float32)
    middle = rest.astype(jnp.bfloat16)
    low = (rest - middle.astype(jnp.float32)).astype(jnp.bfloat16)
    return high, middle, low


def pick(tables, hot_row, hot_lane):
    rows = tables[0].shape[0]
    split = [pieces(t) for t in tables]
    stacked = jnp.concatenate([s[n] for n in range(3) for s in split], 0)
    got = jnp.dot(stacked, hot_lane, preferred_element_type=jnp.float32)
    third = rows * len(tables)
    got = (got[:third] + got[third : 2 * third]) + got[2 * third :]
    return [
        jnp.sum(jnp.where(hot_row, got[n * rows : (n + 1) * rows], 0.0), 0, keepdims=True)
        for n in range(len(tables))
    ]


def grow(radius, weight, dry, wx, wy, window):
    forcing = -CURVATURE / radius
    for a in SHIFTS:
        across = sum(wy[b] * window[a, b] for b in SHIFTS)
        forcing = forcing + wx[a] * across
    initial = radius * radius
    lowest = dry * dry
    solute = KAPPA_SOLUTE * lowest * dry
    wetted = initial
    for sweep in range(NEWTON):
        inverse_root = lax.rsqrt(wetted)
        inverse_square = inverse_root * inverse_root
        pull = solute * (inverse_square * inverse_root)
        residue = wetted - initial - GROWTH_STEP * (forcing + pull)
        slope = 1.0 + (1.5 * GROWTH_STEP) * pull * inverse_square
        wetted = jnp.maximum(wetted - residue / slope, lowest)
    root = jnp.sqrt(wetted)
    return root, weight * (wetted * root - initial * radius)


def collide(r_p, r_q, m_p, m_q, big):
    r_hi, r_lo = jnp.where(big, r_p, r_q), jnp.where(big, r_q, r_p)
    m_hi, m_lo = jnp.where(big, m_p, m_q), jnp.where(big, m_q, m_p)
    total = r_p + r_q
    rate = COLLIDE_RATE * m_hi * total * total * jnp.abs(r_p * r_p - r_q * r_q)
    chance = 1.0 - jnp.exp(-rate)
    volume = r_lo * r_lo * r_lo + chance * r_hi * r_hi * r_hi
    merged = jnp.exp(jnp.log(volume) * (1.0 / 3.0))
    return r_hi, merged, m_hi - chance * m_lo, m_lo


def body(
    sizes,
    moist_in, warm_in, size_in, mult_in, dry_in, east_in, north_in, perm_in,
    lx_in, ly_in, lc_in,
    moist_out, warm_out, size_out, mult_out, rec_out, box_out,
    state, drops, perm, lx, ly, lc,
    state_pack, state_x, state_y, state_c,
    list_pack, list_x, row_pack, row_x,
    dep_out, dep_in, edge, edge_in, mask, coal,
    in_sem, x_send, x_recv, c_send, c_recv, y_send, y_recv,
):
    levels, cx, cy, sd, kx, ky, kc, nx, ny = sizes
    me_x = lax.axis_index("gx")
    me_y = lax.axis_index("gy")
    ys = (1,) if ny == 2 else (1, -1)
    half = cx // 2

    def at(d):
        return (lax.rem(me_x + d[0] + nx, nx), lax.rem(me_y + d[1] + ny, ny))

    loads = []

    def load(source, target):
        copy = pltpu.make_async_copy(source, target, in_sem.at[len(loads)])
        copy.start()
        loads.append(copy)

    load(moist_in, state.at[0])
    load(warm_in, state.at[1])
    for n, source in enumerate((size_in, mult_in, dry_in, east_in, north_in)):
        load(source, drops.at[n])
    load(perm_in, perm)
    load(lx_in.at[0], lx)
    load(ly_in.at[0], ly)
    load(lc_in.at[0], lc)

    friends = [(dx, 0) for dx in MOVES] + [(dx, dy) for dx in MOVES for dy in ys] + [(0, dy) for dy in ys]
    barrier = pltpu.get_barrier_semaphore()
    for d in friends:
        pl.semaphore_signal(barrier, inc=1, device_id=at(d), device_id_type=MESH)

    sends = []

    def send(source, target, s_sem, r_sem, d):
        copy = pltpu.make_async_remote_copy(
            src_ref=source, dst_ref=target, send_sem=s_sem, recv_sem=r_sem,
            device_id=at(d), device_id_type=MESH,
        )
        copy.start()
        sends.append(copy)
        return copy

    line = iota((cx, cy), 0)
    lane = iota((cx, cy), 1)
    low_half = line < half

    loads[0].wait()
    loads[1].wait()
    for f in range(2):
        first, second = state[f, 0], turn(state[f, 1], half, 0)
        state_pack[0, f] = jnp.where(low_half, second, first)
        state_pack[1, f] = jnp.where(low_half, first, second)

    pl.semaphore_wait(barrier, len(friends))

    early = []
    for s, dx in enumerate(MOVES):
        early.append(send(state_pack.at[s], state_x.at[s], x_send.at[s, 0], x_recv.at[s, 0], (dx, 0)))
    for s, dx in enumerate(MOVES):
        for t, dy in enumerate(ys):
            early.append(
                send(state_pack.at[s], state_c.at[s, t], c_send.at[s, t], c_recv.at[s, t], (dx, dy))
            )
    for t, dy in enumerate(ys):
        early.append(send(state, state_y.at[t], y_send.at[t, 0], y_recv.at[t, 0], (0, dy)))

    for copy in loads[2:]:
        copy.wait()
    rows = sd * levels
    block = cx * cy
    tall = levels * cx
    lists = []
    late = []
    for s, (dx, side) in enumerate(zip(MOVES, (cx - 1, 0))):
        list_pack[s, :, 0:kx] = lx[s : s + 1, :]
        list_pack[s, :, kx:] = jnp.concatenate(
            [lc[2 * s : 2 * s + 1, :], lc[2 * s + 1 : 2 * s + 2, :], jnp.full((1, 128 - 2 * kc), -1, jnp.int32)], 1
        )
        lists.append(send(list_pack.at[s], list_x.at[s], x_send.at[s, 1], x_recv.at[s, 1], (dx, 0)))
    for s, (dx, side) in enumerate(zip(MOVES, (cx - 1, 0))):
        for l in range(levels):
            picked = pl.ds(l * cx + side, sd, stride=tall)
            for n in range(5):
                row_pack[s, n, pl.ds(l * sd, sd), :] = drops[n, picked, :]
            row_pack[s, 5, pl.ds(l * sd, sd), :] = perm[picked, :].astype(jnp.float32)
        late.append(send(row_pack.at[s], row_x.at[s], x_send.at[s, 2], x_recv.at[s, 2], (dx, 0)))

    mask[...] = jnp.zeros_like(mask)
    for r, side in enumerate((cx - 1, 0)):
        slots = lx[r : r + 1, :]
        hot_row = iota((rows, kx), 0) == div(slots, block)
        hot_lane = jnp.where(iota((cy, kx), 0) == mod(slots, cy), 1.0, 0.0).astype(jnp.bfloat16)
        named = lax.dot_general(
            jnp.where(hot_row, 1.0, 0.0).astype(jnp.bfloat16), hot_lane,
            (((1,), (1,)), ((), ())), preferred_element_type=jnp.float32,
        )
        mask[pl.ds(side, rows, stride=cx), :] = named

    width = 2 * ky + 4 * kc
    lane_e = iota((1, width), 1)
    high = (lane_e < ky) | ((lane_e >= 2 * ky) & (lane_e < 2 * ky + 2 * kc))
    high_all = jnp.broadcast_to(high, (rows * cx, width))
    slots = jnp.concatenate(
        [ly[0:1, :], ly[1:2, :], lc[0:1, :], lc[2:3, :], lc[1:2, :], lc[3:4, :]], 1
    )
    named_e = iota((rows * cx, width), 0) == div(slots, cy)
    hot_e = jnp.where(named_e, 1.0, 0.0)
    left_high = jnp.max(jnp.where(high_all, hot_e, 0.0), 1, keepdims=True)
    left_low = jnp.max(jnp.where(high_all, 0.0, hot_e), 1, keepdims=True)
    lane_all = iota((rows * cx, cy), 1)
    mask[...] = mask[...] + jnp.where(
        lane_all == cy - 1, left_high, jnp.where(lane_all == 0, left_low, 0.0)
    )
    named_y = named_e & (iota((rows * cx, width), 1) < 2 * ky)

    def pick_y(table):
        both = jnp.where(high_all, table[:, cy - 1 : cy], table[:, 0:1])
        return jnp.sum(jnp.where(named_y, both, 0.0), 0, keepdims=True)

    fixed_y = [pick_y(drops[n]) for n in (2, 3, 4)]

    for copy in lists:
        copy.wait_recv()
    hots = []
    corners = []
    for s, dx in enumerate(MOVES):
        slots = list_x[s, :, 0:kx]
        live = slots >= 0
        j = mod(slots, cy)
        level = mod(div(slots, block), levels)
        row = jnp.where(live, level * sd + div(slots, block * levels), -1)
        hot_row = iota((rows, kx), 0) == row
        hot_lane = jnp.where(iota((cy, kx), 0) == j, 1.0, 0.0).astype(jnp.bfloat16)
        hots.append((hot_row, hot_lane))
        target = (level * cx + mod(mod(div(slots, cy), cx) + dx, cx)) * cy + j
        box_out[:, pl.ds(s * kx, kx)] = jnp.where(live, target, -1)
        corners.append(list_x[s, :, kx:])
    blank = jnp.full((1, 2 * ky), -1, jnp.int32)
    corner = [c[:, n * kc : (n + 1) * kc] for n in range(2) for c in corners]
    slots = jnp.concatenate([ly[0:1, :], ly[1:2, :]] + corner, 1)
    move_y = jnp.where(high, 1, -1)
    which = div(lane_e - 2 * ky, kc)
    move_x = jnp.where(lane_e < 2 * ky, 0, jnp.where(mod(which, 2) == 0, 1, -1))
    level = mod(div(slots, block), levels)
    target = (level * cx + mod(mod(div(slots, cy), cx) + move_x, cx)) * cy + mod(mod(slots, cy) + move_y, cy)
    edge[5:6, :] = jnp.where(slots >= 0, target, -1).astype(jnp.float32)
    edge[6:8, :] = jnp.zeros((2, width), jnp.float32)
    row = jnp.where((slots >= 0) & (lane_e >= 2 * ky), level * sd + div(slots, block * levels), -1)
    named_c = [
        (iota((rows, width), 0) == row) & (mod(div(iota((rows, width), 1) - 2 * ky, kc), 2) == s) for s in range(2)
    ]
    high_c = high_all[:rows]

    def pick_c(s, table):
        both = jnp.where(high_c, table[:, cy - 1 : cy], table[:, 0:1])
        return jnp.sum(jnp.where(named_c[s], both, 0.0), 0, keepdims=True)

    for copy in early:
        copy.wait_recv()

    def blend(parts):
        return parts[0] if len(parts) == 1 else jnp.where(lane < cy // 2, parts[1], parts[0])

    wide = []
    for f in range(2):
        wide.append([])
        for l in range(levels):
            def beyond(up, down):
                return jnp.where(low_half, turn(down, half * l, 0), turn(up, half * l, 0))

            across = beyond(state_x[0, f], state_x[1, f])
            far = blend([beyond(state_c[0, t, f], state_c[1, t, f]) for t in range(len(ys))])
            side_y = blend([state_y[t, f, l] for t in range(len(ys))])
            own_half = jnp.concatenate([state[f, l], across], 0)
            wide[f].append(jnp.concatenate([own_half, jnp.concatenate([side_y, far], 0)], 1))
    mixed = []
    for f in range(2):
        mixed.append([])
        for l in range(levels):
            centre = wide[f][l]
            horizontal = (
                turn(centre, -1, 0) + turn(centre, 1, 0) + turn(centre, -1, 1) + turn(centre, 1, 1)
                - 4.0 * centre
            )
            vertical = wide[f][min(l + 1, levels - 1)] + wide[f][max(l - 1, 0)] - 2.0 * centre
            mixed[f].append(centre + MIX_HORIZONTAL * horizontal + MIX_VERTICAL * vertical)
    window = {(a, b): [] for a in SHIFTS for b in SHIFTS}
    beside = [[{}, {}] for l in range(levels)]
    for l in range(levels):
        vapour, warmth = mixed[0][l], mixed[1][l]
        humid = vapour / (
            EXCESS_FACTOR * jnp.exp(17.27 * (warmth - 273.15) / (warmth - 35.86))
        ) - 1.0
        for b in SHIFTS:
            column = turn(humid, -b, 1)[:, :cy]
            for a in SHIFTS:
                window[a, b].append(turn(column, -a, 0)[:cx])
                for s, home in enumerate((2 * cx - 1, cx)):
                    r = (home + a) % (2 * cx)
                    beside[l][s][a, b] = jnp.broadcast_to(column[r : r + 1], (sd, cy))
        moist_out[l] = vapour[:cx, :cy]
        warm_out[l] = warmth[:cx, :cy]
    window = {key: jnp.concatenate(parts, 0) for key, parts in window.items()}

    grown = []
    mult = []
    deposit = {}
    for k in range(sd):
        part = pl.ds(k * tall, tall)
        weight = drops[1, part, :]
        wx = kernel_weights(drops[3, part, :])
        wy = kernel_weights(drops[4, part, :])
        root, condensed = grow(drops[0, part, :], weight, drops[2, part, :], wx, wy, window)
        for a in SHIFTS:
            along = wx[a] * condensed
            for b in SHIFTS:
                term = wy[b] * along
                deposit[a, b] = term if k == 0 else deposit[a, b] + term
        grown.append(root)
        mult.append(weight)

    order = [perm[k * tall : (k + 1) * tall, :] for k in range(sd)]
    hit = [[order[p] == m for m in range(sd)] for p in range(sd)]

    def member(values, p):
        got = values[0]
        for m in range(1, sd):
            got = jnp.where(hit[p][m], values[m], got)
        return got

    after_radius = []
    after_mult = []
    for pair in range(sd // 2):
        p, q = 2 * pair, 2 * pair + 1
        m_p, m_q = member(mult, p), member(mult, q)
        big = m_p >= m_q
        kept, merged, reduced, m_lo = collide(member(grown, p), member(grown, q), m_p, m_q, big)
        after_radius += [jnp.where(big, kept, merged), jnp.where(big, merged, kept)]
        after_mult += [jnp.where(big, reduced, m_lo), jnp.where(big, m_lo, reduced)]
    for m in range(sd):
        part = pl.ds(m * tall, tall)
        radius, weight = after_radius[0], after_mult[0]
        for p in range(1, sd):
            radius = jnp.where(hit[p][m], after_radius[p], radius)
            weight = jnp.where(hit[p][m], after_mult[p], weight)
        size_out[part, :] = radius
        coal[part, :] = weight
        mult_out[part, :] = jnp.where(mask[part, :] > 0.0, 0.0, weight)

    for copy in late:
        copy.wait_recv()

    slot_k = iota((sd, cy), 0)
    even = mod(slot_k, 2) == 0
    arrive = [[{}, {}] for l in range(levels)]
    tables = [[], []]
    for s in range(2):
        parts = []
        for l in range(levels):
            radius, weight, dry, east, north, turns = (row_x[s, n, pl.ds(l * sd, sd), :] for n in range(6))
            wx, wy = kernel_weights(east), kernel_weights(north)
            root, condensed = grow(radius, weight, dry, wx, wy, beside[l][s])
            along = wx[MOVES[s]] * condensed
            for b in SHIFTS:
                arrive[l][s][b] = jnp.sum(wy[b] * along, 0, keepdims=True)

            def spot(x, m):
                return jnp.broadcast_to(x[m : m + 1], (sd, cy))

            r_p, m_p = spot(root, 0), spot(weight, 0)
            for m in range(1, sd):
                chosen = turns == float(m)
                r_p = jnp.where(chosen, spot(root, m), r_p)
                m_p = jnp.where(chosen, spot(weight, m), m_p)
            r_q = jnp.where(even, turn(r_p, -1, 0), turn(r_p, 1, 0))
            m_q = jnp.where(even, turn(m_p, -1, 0), turn(m_p, 1, 0))
            big = (m_p > m_q) | (even & (m_p == m_q))
            kept, merged, reduced, m_lo = collide(r_p, r_q, m_p, m_q, big)
            radius = jnp.where(big, kept, merged)
            weight = jnp.where(big, reduced, m_lo)
            radius_k, weight_k = spot(radius, 0), spot(weight, 0)
            wanted = slot_k.astype(jnp.float32)
            for p in range(1, sd):
                chosen = spot(turns, p) == wanted
                radius_k = jnp.where(chosen, spot(radius, p), radius_k)
                weight_k = jnp.where(chosen, spot(weight, p), weight_k)
            parts.append((radius_k, weight_k))
        tables[s] = [jnp.concatenate([p[n] for p in parts], 0) for n in range(2)]
        tables[s] += [row_x[s, n, :, :] for n in (2, 3, 4)]

    def spread(parts, size, dim, index):
        back = turn(parts[-1], -1, dim)
        ahead = turn(parts[1], 1, dim)
        inner = parts[0] + jnp.where(index == size - 1, 0.0, back) + jnp.where(index == 0, 0.0, ahead)
        outer = jnp.where(index == size - 1, back, jnp.where(index == 0, ahead, 0.0))
        return inner, outer

    own = []
    for l in range(levels):
        inner = {}
        for b in SHIFTS:
            parts = {a: deposit[a, b][l * cx : (l + 1) * cx] for a in SHIFTS}
            inner[b], _ = spread(parts, cx, 0, line)
            inner[b] = inner[b] + jnp.where(
                line == 0, arrive[l][0][b], jnp.where(line == cx - 1, arrive[l][1][b], 0.0)
            )
        kept, leaving = spread(inner, cy, 1, lane)
        own.append(kept)
        dep_out[l] = leaving
    deposits = []
    for t, dy in enumerate(ys):
        deposits.append(send(dep_out, dep_in.at[t], y_send.at[t, 1], y_recv.at[t, 1], (0, dy)))

    for n in range(5):
        face = pick_y((size_out, coal)[n][...]) if n < 2 else fixed_y[n - 2]
        edge[n : n + 1, :] = face + pick_c(0, tables[0][n]) + pick_c(1, tables[1][n])
    edges = []
    for t, dy in enumerate(ys):
        edges.append(send(edge, edge_in.at[t], y_send.at[t, 2], y_recv.at[t, 2], (0, dy)))

    for s in range(2):
        got = pick(tables[s], *hots[s])
        for n in range(5):
            rec_out[n, :, pl.ds(s * kx, kx)] = got[n]

    for copy in deposits:
        copy.wait_recv()
    for l in range(levels):
        if len(ys) == 1:
            total = own[l] + dep_in[0, l]
        else:
            total = own[l] + jnp.where(
                lane == 0, dep_in[0, l], jnp.where(lane == cy - 1, dep_in[1, l], 0.0)
            )
        moist_out[l] = moist_out[l] - VAPOUR_PER_SOURCE * total
        warm_out[l] = warm_out[l] + WARMING_FACTOR * total

    for copy in edges:
        copy.wait_recv()
    came = edge_in[0]
    if len(ys) == 2:
        came = jnp.where(jnp.broadcast_to(high, (8, width)), came, edge_in[1])
    for n in range(5):
        rec_out[n, :, pl.ds(2 * kx, width)] = came[n : n + 1, :]
    box_out[:, pl.ds(2 * kx, width)] = came[5:6, :].astype(jnp.int32)

    for copy in sends:
        copy.wait_send()


def publish(*refs):
    count = len(refs) // 2
    sems = refs[-1]
    copies = [
        pltpu.make_async_copy(refs[n], refs[count + n], sems.at[n]) for n in range(count)
    ]
    for copy in copies:
        copy.start()
    for copy in copies:
        copy.wait()


def per_device(nx, ny, moist, warm, size, mult, dry, east, north, perm, lx, ly, lc):
    levels, cx, cy = moist.shape
    sd = size.shape[0]
    kx, ky, kc = lx.shape[2], ly.shape[2], lc.shape[2]
    narr = 2 * kx + 2 * ky + 4 * kc
    width = 2 * ky + 4 * kc
    slots = sd * levels * cx
    flat = [x.reshape(slots, cy) for x in (size, mult, dry, east, north, perm)]
    f32, i32 = jnp.float32, jnp.int32
    any_space = pl.BlockSpec(memory_space=pl.ANY)
    vmem_space = pl.BlockSpec(memory_space=pltpu.VMEM)
    dma = pltpu.SemaphoreType.DMA
    shapes = (
        ((levels, cx, cy), f32),
        ((levels, cx, cy), f32),
        ((slots, cy), f32),
        ((slots, cy), f32),
        ((5, 1, narr), f32),
        ((1, narr), i32),
    )
    n_y = 1 if ny == 2 else 2
    outs = pl.pallas_call(
        functools.partial(body, (levels, cx, cy, sd, kx, ky, kc, nx, ny)),
        out_shape=tuple(pltpu.VMEM(*s) for s in shapes),
        in_specs=[any_space] * 11,
        out_specs=[vmem_space] * 6,
        scratch_shapes=[
            pltpu.VMEM((2, levels, cx, cy), f32),
            pltpu.VMEM((5, slots, cy), f32),
            pltpu.VMEM((slots, cy), i32),
            pltpu.VMEM((2, kx), i32),
            pltpu.VMEM((2, ky), i32),
            pltpu.VMEM((4, kc), i32),
            pltpu.VMEM((2, 2, cx, cy), f32),
            pltpu.VMEM((2, 2, cx, cy), f32),
            pltpu.VMEM((n_y, 2, levels, cx, cy), f32),
            pltpu.VMEM((2, n_y, 2, cx, cy), f32),
            pltpu.VMEM((2, 1, kx + 128), i32),
            pltpu.VMEM((2, 1, kx + 128), i32),
            pltpu.VMEM((2, 6, sd * levels, cy), f32),
            pltpu.VMEM((2, 6, sd * levels, cy), f32),
            pltpu.VMEM((levels, cx, cy), f32),
            pltpu.VMEM((n_y, levels, cx, cy), f32),
            pltpu.VMEM((8, width), f32),
            pltpu.VMEM((n_y, 8, width), f32),
            pltpu.VMEM((slots, cy), f32),
            pltpu.VMEM((slots, cy), f32),
            dma((11,)),
            dma((2, 3)), dma((2, 3)), dma((2, n_y)), dma((2, n_y)), dma((n_y, 3)), dma((n_y, 3)),
        ],
        compiler_params=pltpu.CompilerParams(collective_id=0, has_side_effects=True),
    )(moist, warm, *flat, lx, ly, lc)
    outs = pl.pallas_call(
        publish,
        out_shape=tuple(jax.ShapeDtypeStruct(*s) for s in shapes),
        in_specs=[vmem_space] * 6,
        out_specs=[any_space] * 6,
        scratch_shapes=[dma((6,))],
    )(*[pltpu.with_memory_space_constraint(x, pltpu.VMEM) for x in outs])
    return (
        outs[0], outs[1], outs[2].reshape(size.shape), outs[3].reshape(size.shape), outs[4], outs[5],
    )


def solution(mesh):
    cell, drop, lists = P(None, "gx", "gy"), P(None, None, "gx", "gy"), P("gx", None, "gy")
    return jax.shard_map(
        functools.partial(per_device, mesh.shape["gx"], mesh.shape["gy"]),
        mesh=mesh,
        in_specs=(cell,) * 2 + (drop,) * 6 + (lists,) * 3,
        out_specs=(cell, cell, drop, drop, cell, P("gx", "gy")),
        check_vma=False,
    )
```

```python
import functools
import math

import jax
import jax.numpy as jnp
from jax import lax
from jax.experimental import pallas as pl
from jax.experimental.pallas import tpu as pltpu
from jax.sharding import PartitionSpec as P

NEWTON = 4
MIX_HORIZONTAL = 0.2
MIX_VERTICAL = 0.05
EXCESS_FACTOR = 4.2222
CURVATURE = 0.0012
KAPPA_SOLUTE = 0.6
GROWTH_STEP = 200.0
COLLIDE_RATE = 4e-07
VAPOUR_PER_SOURCE = 0.001
WARMING_FACTOR = 0.00249
LOG2E = math.log2(math.e)

MESH = pl.DeviceIdType.MESH
SHIFTS = (-1, 0, 1)
SIDES = (1, -1)
MOVES = (1, -1)


def div(x, n):
    return lax.shift_right_arithmetic(x, jnp.int32(n.bit_length() - 1))


def mod(x, n):
    return lax.bitwise_and(x, jnp.int32(n - 1))


def iota(shape, dim):
    return lax.broadcasted_iota(jnp.int32, shape, dim)


def turn(x, shift, dim):
    shift %= x.shape[dim]
    return pltpu.roll(x, shift, dim) if shift else x


def take(x, index, dim):
    return jnp.take_along_axis(x, index, axis=dim)


def kernel_weights(offset):
    return {
        -1: jnp.maximum(0.5 - offset, 0.0),
        0: 1.0 - jnp.abs(offset - 0.5),
        1: jnp.maximum(offset - 0.5, 0.0),
    }


def prepare(radius, dry):
    inverse = 1.0 / radius
    square = inverse * inverse
    lowest = dry * dry
    strength = (1.5 * GROWTH_STEP * KAPPA_SOLUTE) * (lowest * dry)
    pull = strength * (square * inverse)
    area = radius * radius
    return (
        area - (GROWTH_STEP * CURVATURE) * inverse,
        (5.0 / 3.0) * pull,
        1.0 / (1.0 + pull * square),
        strength,
        lowest,
        area * radius,
    )


def settle(level, top, inverse_slope, strength, lowest):
    wetted = jnp.maximum((level + top) * inverse_slope, lowest)
    for sweep in range(NEWTON - 1):
        inverse_root = lax.rsqrt(wetted)
        square = inverse_root * inverse_root
        pull = strength * (square * inverse_root)
        wetted = jnp.maximum((level + (5.0 / 3.0) * pull) / (1.0 + pull * square), lowest)
    root = wetted * lax.rsqrt(wetted)
    return root, wetted * root


def differences(field):
    near = {(a, b): turn(turn(field, -b, 1), -a, 0) for a in SHIFTS for b in SHIFTS}
    terms = {(0, 0): field}
    for s in SIDES:
        terms[s, 0] = near[s, 0] - field
        terms[0, s] = near[0, s] - field
    for a in SIDES:
        for b in SIDES:
            terms[a, b] = near[a, b] - near[a, 0] - terms[0, b]
    return terms


def interpolate(terms, east, north, reach_x, reach_y):
    right, up = east > 0.5, north > 0.5
    slope_x = jnp.where(right, terms[1, 0], terms[-1, 0])
    slope_y = jnp.where(up, terms[0, 1], terms[0, -1])
    twist = jnp.where(
        right, jnp.where(up, terms[1, 1], terms[1, -1]), jnp.where(up, terms[-1, 1], terms[-1, -1])
    )
    return terms[0, 0] + reach_x * slope_x + reach_y * (slope_y + reach_x * twist)


def match(weight, other, first):
    big = (weight > other) | ((weight == other) & first)
    rate = (-COLLIDE_RATE * LOG2E) * jnp.where(big, weight, other)
    return rate, jnp.where(big, other, 0.0)


def collide(radius, cube, other, rate, eaten):
    total = radius + other
    chance = 1.0 - jnp.exp2(rate * (total * total) * (total * jnp.abs(radius - other)))
    volume = cube + chance * (other * other * other)
    merged = jnp.exp2(jnp.log(volume) * (LOG2E / 3.0))
    return jnp.where(eaten > 0.0, radius, merged), chance * eaten


def body(
    sizes,
    moist_in, warm_in, size_in, mult_in, dry_in, east_in, north_in, perm_in,
    lx_in, ly_in, lc_in,
    moist_out, warm_out, size_out, mult_out, rec_out, box_out,
    state, drops, perm, lx, ly, lc,
    state_pack, state_x, state_y, diag_pack, diag_in,
    list_pack, list_x, list_c, row_pack, row_x, corner_pack, corner_in,
    dep_out, dep_in, edge, edge_in, mask, coal,
    ready, share, bits, near, late_x,
    in_sem, x_send, x_recv, c_send, c_recv, y_send, y_recv,
):
    levels, cx, cy, sd, kx, ky, kc, nx, ny = sizes
    me_x = lax.axis_index("gx")
    me_y = lax.axis_index("gy")
    ys = (1,) if ny == 2 else (1, -1)
    half = cx // 2
    rows = sd * levels
    block = cx * cy
    tall = levels * cx
    deep = kx // cy

    def at(d):
        return (lax.rem(me_x + d[0] + nx, nx), lax.rem(me_y + d[1] + ny, ny))

    loads = []

    def load(source, target):
        copy = pltpu.make_async_copy(source, target, in_sem.at[len(loads)])
        copy.start()
        loads.append(copy)

    load(moist_in, state.at[0])
    load(warm_in, state.at[1])
    for n, source in enumerate((size_in, mult_in, dry_in, east_in, north_in)):
        load(source, drops.at[n])
    load(perm_in, perm)
    load(lx_in.at[0], lx)
    load(ly_in.at[0], ly)
    load(lc_in.at[0], lc)

    friends = [(dx, 0) for dx in MOVES] + [(dx, dy) for dx in MOVES for dy in ys] + [(0, dy) for dy in ys]
    barrier = pltpu.get_barrier_semaphore()
    for d in friends:
        pl.semaphore_signal(barrier, inc=1, device_id=at(d), device_id_type=MESH)

    sends = []

    def send(source, target, s_sem, r_sem, d):
        copy = pltpu.make_async_remote_copy(
            src_ref=source, dst_ref=target, send_sem=s_sem, recv_sem=r_sem,
            device_id=at(d), device_id_type=MESH,
        )
        copy.start()
        sends.append(copy)
        return copy

    line = iota((cx, cy), 0)
    lane = iota((cx, cy), 1)
    low_half = line < half
    middle = (lane >= cy // 4) & (lane < 3 * cy // 4)

    loads[0].wait()
    loads[1].wait()
    for s in range(2):
        tiles = []
        for f in range(2):
            first, second = state[f, 0], turn(state[f, 1], half, 0)
            tiles.append(jnp.where(low_half, second, first) if s == 0 else jnp.where(low_half, first, second))
            state_pack[s, f] = tiles[f]
        diag_pack[s] = jnp.where(middle, turn(tiles[1], cy // 2, 1), tiles[0])

    pl.semaphore_wait(barrier, len(friends))

    early = []
    for s, dx in enumerate(MOVES):
        early.append(send(state_pack.at[s], state_x.at[s], x_send.at[s, 0], x_recv.at[s, 0], (dx, 0)))
    for s, dx in enumerate(MOVES):
        for t, dy in enumerate(ys):
            early.append(
                send(diag_pack.at[s], diag_in.at[s, t], c_send.at[s, t, 0], c_recv.at[s, t, 0], (dx, dy))
            )
    for t, dy in enumerate(ys):
        early.append(send(state, state_y.at[t], y_send.at[t, 0], y_recv.at[t, 0], (0, dy)))

    for copy in loads[2:]:
        copy.wait()
    late = []
    for s, (dx, side) in enumerate(zip(MOVES, (cx - 1, 0))):
        for l in range(levels):
            picked = pl.ds(l * cx + side, sd, stride=tall)
            for n in range(5):
                row_pack[s, n, pl.ds(l * sd, sd), :] = drops[n, picked, :]
            row_pack[s, 5, pl.ds(l * sd, sd), :] = perm[picked, :].astype(jnp.float32)
        late.append(send(row_pack.at[s], row_x.at[s], x_send.at[s, 2], x_recv.at[s, 2], (dx, 0)))
    for s, dx in enumerate(MOVES):
        for c in range(deep):
            list_pack[s, c : c + 1, :] = lx[s : s + 1, c * cy : (c + 1) * cy]
        late.append(send(list_pack.at[s], list_x.at[s], x_send.at[s, 1], x_recv.at[s, 1], (dx, 0)))
    for s, dx in enumerate(MOVES):
        tile = None
        for n in range(6):
            for l in range(levels):
                spot = 8 * n + 4 * s + 2 * l
                moved = turn(row_pack[s, n, pl.ds(l * sd, sd), :], spot + 1, 1)
                tile = moved if tile is None else jnp.where((lane >= spot) & (lane < spot + 2), moved, tile)
        corner_pack[s] = tile
        for t, dy in enumerate(ys):
            late.append(
                send(corner_pack.at[s], corner_in.at[s, t], c_send.at[s, t, 1], c_recv.at[s, t, 1], (dx, dy))
            )
            late.append(send(lc, list_c.at[s, t], c_send.at[s, t, 2], c_recv.at[s, t, 2], (dx, dy)))

    order = [perm[k * tall : (k + 1) * tall, :] for k in range(sd)]
    for m in range(sd):
        part = pl.ds(m * tall, tall)
        weight = drops[1, part, :]
        partner = jnp.zeros((tall, cy), jnp.int32)
        first = jnp.zeros((tall, cy), jnp.int32)
        for p in range(sd):
            mine = order[p] == m
            partner = jnp.where(mine, order[p ^ 1], partner)
            if p % 2 == 0:
                first = jnp.where(mine, 1, first)
        other = drops[1, pl.ds(0, tall), :]
        for k in range(1, sd):
            other = jnp.where(partner == k, drops[1, pl.ds(k * tall, tall), :], other)
        rate, eaten = match(weight, other, first > 0)
        for n in range(3):
            bits[n, part, :] = mod(lax.shift_right_logical(partner, jnp.int32(n)), 2)
        for n, value in enumerate(prepare(drops[0, part, :], drops[2, part, :])):
            ready[n, part, :] = value
        east, north = drops[3, part, :], drops[4, part, :]
        ready[6, part, :] = jnp.abs(east - 0.5)
        ready[7, part, :] = jnp.abs(north - 0.5)
        ready[8, part, :] = rate
        ready[9, part, :] = eaten
        wx, wy = kernel_weights(east), kernel_weights(north)
        for a in SHIFTS:
            along = wx[a] * weight
            for b in SHIFTS:
                share[3 * a + b + 4, part, :] = wy[b] * along

    mask[...] = jnp.ones_like(mask)
    for r, side in enumerate((cx - 1, 0)):
        slots = lx[r : r + 1, :]
        hot_row = iota((rows, kx), 0) == div(slots, block)
        hot_lane = jnp.where(iota((cy, kx), 0) == mod(slots, cy), 1.0, 0.0).astype(jnp.bfloat16)
        named = lax.dot_general(
            jnp.where(hot_row, 1.0, 0.0).astype(jnp.bfloat16), hot_lane,
            (((1,), (1,)), ((), ())), preferred_element_type=jnp.float32,
        )
        mask[pl.ds(side, rows, stride=cx), :] = 1.0 - named

    width = 2 * ky + 4 * kc
    lane_e = iota((1, width), 1)
    high = (lane_e < ky) | ((lane_e >= 2 * ky) & (lane_e < 2 * ky + 2 * kc))
    high_all = jnp.broadcast_to(high, (rows * cx, width))
    slots = jnp.concatenate(
        [ly[0:1, :], ly[1:2, :], lc[0:1, :], lc[2:3, :], lc[1:2, :], lc[3:4, :]], 1
    )
    named_e = iota((rows * cx, width), 0) == div(slots, cy)
    hot_e = jnp.where(named_e, 1.0, 0.0)
    left_high = jnp.max(jnp.where(high_all, hot_e, 0.0), 1, keepdims=True)
    left_low = jnp.max(jnp.where(high_all, 0.0, hot_e), 1, keepdims=True)
    lane_all = iota((rows * cx, cy), 1)
    mask[...] = mask[...] * (
        1.0 - jnp.where(lane_all == cy - 1, left_high, jnp.where(lane_all == 0, left_low, 0.0))
    )

    face = lane_e < 2 * ky
    face_pile = jnp.broadcast_to(jnp.where(face, div(slots, block), -1), (cx, width))
    face_line = line == mod(div(slots, cy), cx)
    face_lane = jnp.broadcast_to(jnp.where(high, cy - 1, 0), (cx, width))

    def pick_y(ref):
        got = jnp.zeros((cx, width), jnp.float32)
        for n in range(rows):
            got = jnp.where(face_pile == n, take(ref[pl.ds(n * cx, cx), :], face_lane, 1), got)
        return jnp.sum(jnp.where(face_line, got, 0.0), 0, keepdims=True)

    def land(slots, move_x, move_y):
        level = mod(div(slots, block), levels)
        i = mod(mod(div(slots, cy), cx) + move_x, cx)
        target = (level * cx + i) * cy + mod(mod(slots, cy) + move_y, cy)
        return jnp.where(slots >= 0, target, -1)

    for n in (2, 3, 4):
        edge[n : n + 1, :] = pick_y(drops.at[n])
    edge[5:6, :] = land(slots, 0, jnp.where(high, 1, -1)).astype(jnp.float32)
    edge[6:8, :] = jnp.zeros((2, width), jnp.float32)

    for copy in early:
        copy.wait_recv()

    def blend(parts, pick_second):
        return parts[0] if len(parts) == 1 else jnp.where(pick_second, parts[1], parts[0])

    left_lanes = lane < cy // 2
    fields = []
    for f in range(2):
        fields.append([])
        for l in range(levels):
            def beyond(up, down):
                return jnp.where(low_half, turn(down, half * l, 0), turn(up, half * l, 0))

            across = beyond(state_x[0, f], state_x[1, f])
            tiles = [[turn(diag_in[s, t], f * (cy // 2), 1) for s in range(2)] for t in range(len(ys))]
            far = blend([beyond(*pair) for pair in tiles], left_lanes)
            side_y = blend([state_y[t, f, l] for t in range(len(ys))], left_lanes)
            own_half = jnp.concatenate([state[f, l], across], 0)
            fields[f].append(jnp.concatenate([own_half, jnp.concatenate([side_y, far], 0)], 1))
    mixed = []
    for f in range(2):
        mixed.append([])
        for l in range(levels):
            centre = fields[f][l]
            around = turn(centre, -1, 0) + turn(centre, 1, 0) + turn(centre, -1, 1) + turn(centre, 1, 1)
            stacked = fields[f][min(l + 1, levels - 1)] + fields[f][max(l - 1, 0)]
            mixed[f].append(
                (1.0 - 4.0 * MIX_HORIZONTAL - 2.0 * MIX_VERTICAL) * centre
                + MIX_HORIZONTAL * around + MIX_VERTICAL * stacked
            )
    keys = [(a, b) for a in SHIFTS for b in SHIFTS]
    terms = []
    for l in range(levels):
        vapour, warmth = mixed[0][l], mixed[1][l]
        decay = jnp.exp2((-17.27 * LOG2E) * (warmth - 273.15) / (warmth - 35.86))
        terms.append(differences((GROWTH_STEP / EXCESS_FACTOR) * (vapour * decay) - GROWTH_STEP))
        moist_out[l] = vapour[:cx, :cy]
        warm_out[l] = warmth[:cx, :cy]
    window = {key: jnp.concatenate([t[key][:cx, :cy] for t in terms], 0) for key in keys}

    grown = []
    cubes = []
    deposit = {}
    for k in range(sd):
        part = pl.ds(k * tall, tall)
        base, top, inverse_slope, strength, lowest, cube = (ready[n, part, :] for n in range(6))
        level = base + interpolate(
            window, drops[3, part, :], drops[4, part, :], ready[6, part, :], ready[7, part, :]
        )
        root, volume = settle(level, top, inverse_slope, strength, lowest)
        gain = volume - cube
        for a, b in keys:
            term = share[3 * a + b + 4, part, :] * gain
            deposit[a, b] = term if k == 0 else deposit[a, b] + term
        grown.append(root)
        cubes.append(volume)

    def spread(parts, dim, index):
        size = parts[0].shape[dim]
        back = turn(parts[-1], -1, dim)
        ahead = turn(parts[1], 1, dim)
        inner = parts[0] + jnp.where(index == size - 1, 0.0, back) + jnp.where(index == 0, 0.0, ahead)
        outer = jnp.where(index == size - 1, back, jnp.where(index == 0, ahead, 0.0))
        return inner, outer

    own = []
    for l in range(levels):
        inner = {}
        for b in SHIFTS:
            inner[b], _ = spread({a: deposit[a, b][l * cx : (l + 1) * cx] for a in SHIFTS}, 0, line)
        kept, leaving = spread(inner, 1, lane)
        own.append(kept)
        dep_out[l] = leaving
    deposits = []
    for t, dy in enumerate(ys):
        deposits.append(send(dep_out, dep_in.at[t], y_send.at[t, 1], y_recv.at[t, 1], (0, dy)))

    for m in range(sd):
        part = pl.ds(m * tall, tall)
        found = grown
        for n in range(3):
            odd = bits[n, part, :] > 0
            found = [jnp.where(odd, found[2 * i + 1], found[2 * i]) for i in range(len(found) // 2)]
        radius, lost = collide(grown[m], cubes[m], found[0], ready[8, part, :], ready[9, part, :])
        weight = drops[1, part, :] - lost
        size_out[part, :] = radius
        coal[part, :] = weight
        mult_out[part, :] = mask[part, :] * weight

    edge[0:1, :] = pick_y(size_out)
    edge[1:2, :] = pick_y(coal)
    edges = []
    for t, dy in enumerate(ys):
        edges.append(send(edge, edge_in.at[t], y_send.at[t, 2], y_recv.at[t, 2], (0, dy)))

    for l in range(levels):
        for n, key in enumerate(keys):
            near[l, n] = terms[l][key][cx:, :cy]
    corner_window = {}
    for key in keys:
        built = None
        for s, home in enumerate((2 * cx - 1, cx)):
            for l in range(levels):
                spot = 4 * s + 2 * l
                moved = turn(jnp.broadcast_to(terms[l][key][home : home + 1, cy:], (sd, cy)), spot + 1, 1)
                built = moved if built is None else jnp.where(lane >= spot, moved, built)
        corner_window[key] = built

    for copy in late:
        copy.wait_recv()

    def pair_up(weight, turns):
        seat = iota((sd, cy), 0)
        rank = jnp.zeros((sd, cy), jnp.int32)
        for p in range(1, sd):
            rank = jnp.where(jnp.broadcast_to(turns[p : p + 1], (sd, cy)) == seat, p, rank)
        partner = take(turns, rank ^ 1, 0)
        return partner, match(weight, take(weight, partner, 0), mod(rank, 2) == 0)

    def finish(radius, weight, dry, east, north, turns, around):
        base, top, inverse_slope, strength, lowest, cube = prepare(radius, dry)
        level = base + interpolate(around, east, north, jnp.abs(east - 0.5), jnp.abs(north - 0.5))
        root, volume = settle(level, top, inverse_slope, strength, lowest)
        partner, (rate, eaten) = pair_up(weight, turns.astype(jnp.int32))
        after, lost = collide(root, volume, take(root, partner, 0), rate, eaten)
        return weight * (volume - cube), after, weight - lost

    arrive = [[None, None] for l in range(levels)]
    for s in range(2):
        home = cx - 1 if s == 0 else 0
        for l in range(levels):
            span = pl.ds(l * sd, sd)
            values = [row_x[s, n, span, :] for n in range(6)]
            around = {
                key: jnp.broadcast_to(near[l, n, home : home + 1, :], (sd, cy)) for n, key in enumerate(keys)
            }
            condensed, radius, weight = finish(*values, around)
            late_x[s, 0, span, :] = radius
            late_x[s, 1, span, :] = weight
            wx, wy = kernel_weights(values[3]), kernel_weights(values[4])
            along = wx[MOVES[s]] * condensed
            moved = {b: jnp.sum(wy[b] * along, 0, keepdims=True) for b in SHIFTS}
            arrive[l][s], _ = spread(moved, 1, lane[0:1])

    tile = [blend([corner_in[s, t] for t in range(len(ys))], mod(lane, 2) == 1) for s in range(2)]
    tile = jnp.where(mod(lane, 8) < 4, tile[0], tile[1])
    values = [turn(tile, -8 * n, 1) for n in range(6)]
    condensed, corner_radius, corner_weight = finish(*values, corner_window)
    wx, wy = kernel_weights(values[3]), kernel_weights(values[4])
    drop_x = jnp.where(mod(lane, 8) < 4, wx[1], wx[-1])
    drop_y = jnp.where(mod(lane, 2) == 0, wy[1], wy[-1])
    fallen = jnp.sum(drop_x * drop_y * condensed, 0, keepdims=True)
    for l in range(levels):
        for s in range(2):
            spot = 4 * s + 2 * l
            added = arrive[l][s] + jnp.where(
                lane[0:1] == 0, turn(fallen, -spot, 1),
                jnp.where(lane[0:1] == cy - 1, turn(fallen, cy - 2 - spot, 1), 0.0),
            )
            own[l] = own[l] + jnp.where(line == (0 if s == 0 else cx - 1), added, 0.0)

    for s, dx in enumerate(MOVES):
        slots = list_x[s]
        level = mod(div(slots, block), levels)
        row = jnp.where(slots >= 0, level * sd + div(slots, block * levels), -1)
        column = mod(slots, cy)
        for n in range(5):
            got = jnp.zeros((deep, cy), jnp.float32)
            for r in range(rows):
                source = late_x[s, n, r : r + 1, :] if n < 2 else row_x[s, n, r : r + 1, :]
                got = jnp.where(row == r, take(jnp.broadcast_to(source, (deep, cy)), column, 1), got)
            rec_out[n, :, pl.ds(s * kx, kx)] = got.reshape(1, kx)
        box_out[:, pl.ds(s * kx, kx)] = land(slots, dx, 0).reshape(1, kx)

    blank = jnp.full((1, 2 * ky), -1, jnp.int32)
    slots = jnp.concatenate(
        [blank] + [
            list_c[s, d if len(ys) == 2 else 0, 2 * s + d : 2 * s + d + 1, :] for d in range(2) for s in range(2)
        ],
        1,
    )
    which = div(lane_e - 2 * ky, kc)
    minus_x, minus_y = mod(which, 2), div(which, 2)
    level = mod(div(slots, block), levels)
    spot = jnp.broadcast_to(jnp.where(slots >= 0, 4 * minus_x + 2 * level + minus_y, 0), (sd, width))
    seat = jnp.where(slots >= 0, div(slots, block * levels), -1)
    corner_box = land(slots, 1 - 2 * minus_x, 1 - 2 * minus_y)
    corner_rec = [
        jnp.sum(jnp.where(iota((sd, width), 0) == seat, take(value, spot, 1), 0.0), 0, keepdims=True)
        for value in (corner_radius, corner_weight, values[2], values[3], values[4])
    ]

    for copy in deposits:
        copy.wait_recv()
    for l in range(levels):
        if len(ys) == 1:
            total = own[l] + dep_in[0, l]
        else:
            total = own[l] + jnp.where(
                lane == 0, dep_in[0, l], jnp.where(lane == cy - 1, dep_in[1, l], 0.0)
            )
        moist_out[l] = moist_out[l] - VAPOUR_PER_SOURCE * total
        warm_out[l] = warm_out[l] + WARMING_FACTOR * total

    for copy in edges:
        copy.wait_recv()
    came = blend([edge_in[t] for t in range(len(ys))], jnp.broadcast_to(lane_e >= ky, (8, width)))
    for n in range(5):
        rec_out[n, :, pl.ds(2 * kx, width)] = jnp.where(face, came[n : n + 1, :], corner_rec[n])
    box_out[:, pl.ds(2 * kx, width)] = jnp.where(face, came[5:6, :].astype(jnp.int32), corner_box)

    for copy in sends:
        copy.wait_send()


def publish(*refs):
    count = len(refs) // 2
    sems = refs[-1]
    copies = [
        pltpu.make_async_copy(refs[n], refs[count + n], sems.at[n]) for n in range(count)
    ]
    for copy in copies:
        copy.start()
    for copy in copies:
        copy.wait()


def per_device(nx, ny, moist, warm, size, mult, dry, east, north, perm, lx, ly, lc):
    levels, cx, cy = moist.shape
    sd = size.shape[0]
    kx, ky, kc = lx.shape[2], ly.shape[2], lc.shape[2]
    narr = 2 * kx + 2 * ky + 4 * kc
    width = 2 * ky + 4 * kc
    slots = sd * levels * cx
    flat = [x.reshape(slots, cy) for x in (size, mult, dry, east, north, perm)]
    f32, i32 = jnp.float32, jnp.int32
    any_space = pl.BlockSpec(memory_space=pl.ANY)
    vmem_space = pl.BlockSpec(memory_space=pltpu.VMEM)
    dma = pltpu.SemaphoreType.DMA
    shapes = (
        ((levels, cx, cy), f32),
        ((levels, cx, cy), f32),
        ((slots, cy), f32),
        ((slots, cy), f32),
        ((5, 1, narr), f32),
        ((1, narr), i32),
    )
    n_y = 1 if ny == 2 else 2
    outs = pl.pallas_call(
        functools.partial(body, (levels, cx, cy, sd, kx, ky, kc, nx, ny)),
        out_shape=tuple(pltpu.VMEM(*s) for s in shapes),
        in_specs=[any_space] * 11,
        out_specs=[vmem_space] * 6,
        scratch_shapes=[
            pltpu.VMEM((2, levels, cx, cy), f32),
            pltpu.VMEM((5, slots, cy), f32),
            pltpu.VMEM((slots, cy), i32),
            pltpu.VMEM((2, kx), i32),
            pltpu.VMEM((2, ky), i32),
            pltpu.VMEM((4, kc), i32),
            pltpu.VMEM((2, 2, cx, cy), f32),
            pltpu.VMEM((2, 2, cx, cy), f32),
            pltpu.VMEM((n_y, 2, levels, cx, cy), f32),
            pltpu.VMEM((2, cx, cy), f32),
            pltpu.VMEM((2, n_y, cx, cy), f32),
            pltpu.VMEM((2, kx // cy, cy), i32),
            pltpu.VMEM((2, kx // cy, cy), i32),
            pltpu.VMEM((2, n_y, 4, kc), i32),
            pltpu.VMEM((2, 6, sd * levels, cy), f32),
            pltpu.VMEM((2, 6, sd * levels, cy), f32),
            pltpu.VMEM((2, sd, cy), f32),
            pltpu.VMEM((2, n_y, sd, cy), f32),
            pltpu.VMEM((levels, cx, cy), f32),
            pltpu.VMEM((n_y, levels, cx, cy), f32),
            pltpu.VMEM((8, width), f32),
            pltpu.VMEM((n_y, 8, width), f32),
            pltpu.VMEM((slots, cy), f32),
            pltpu.VMEM((slots, cy), f32),
            pltpu.VMEM((10, slots, cy), f32),
            pltpu.VMEM((9, slots, cy), f32),
            pltpu.VMEM((3, slots, cy), i32),
            pltpu.VMEM((levels, 9, cx, cy), f32),
            pltpu.VMEM((2, 2, sd * levels, cy), f32),
            dma((11,)),
            dma((2, 3)), dma((2, 3)), dma((2, n_y, 3)), dma((2, n_y, 3)), dma((n_y, 3)), dma((n_y, 3)),
        ],
        compiler_params=pltpu.CompilerParams(collective_id=0, has_side_effects=True),
    )(moist, warm, *flat, lx, ly, lc)
    outs = pl.pallas_call(
        publish,
        out_shape=tuple(jax.ShapeDtypeStruct(*s) for s in shapes),
        in_specs=[vmem_space] * 6,
        out_specs=[any_space] * 6,
        scratch_shapes=[dma((6,))],
    )(*[pltpu.with_memory_space_constraint(x, pltpu.VMEM) for x in outs])
    return (
        outs[0], outs[1], outs[2].reshape(size.shape), outs[3].reshape(size.shape), outs[4], outs[5],
    )


def solution(mesh):
    cell, drop, lists = P(None, "gx", "gy"), P(None, None, "gx", "gy"), P("gx", None, "gy")
    return jax.shard_map(
        functools.partial(per_device, mesh.shape["gx"], mesh.shape["gy"]),
        mesh=mesh,
        in_specs=(cell,) * 2 + (drop,) * 6 + (lists,) * 3,
        out_specs=(cell, cell, drop, drop, cell, P("gx", "gy")),
        check_vma=False,
    )
```

```python
import functools
import math

import jax
import jax.numpy as jnp
from jax import lax
from jax.experimental import pallas as pl
from jax.experimental.pallas import tpu as pltpu
from jax.sharding import PartitionSpec as P

NEWTON = 4
MIX_HORIZONTAL = 0.2
MIX_VERTICAL = 0.05
EXCESS_FACTOR = 4.2222
CURVATURE = 0.0012
KAPPA_SOLUTE = 0.6
GROWTH_STEP = 200.0
COLLIDE_RATE = 4e-07
VAPOUR_PER_SOURCE = 0.001
WARMING_FACTOR = 0.00249
LOG2E = math.log2(math.e)

MESH = pl.DeviceIdType.MESH
SHIFTS = (-1, 0, 1)
SIDES = (1, -1)
MOVES = (1, -1)


def div(x, n):
    return lax.shift_right_arithmetic(x, jnp.int32(n.bit_length() - 1))


def mod(x, n):
    return lax.bitwise_and(x, jnp.int32(n - 1))


def iota(shape, dim):
    return lax.broadcasted_iota(jnp.int32, shape, dim)


def turn(x, shift, dim):
    shift %= x.shape[dim]
    return pltpu.roll(x, shift, dim) if shift else x


def take(x, index, dim):
    return jnp.take_along_axis(x, index, axis=dim)


def kernel_weights(offset):
    return {
        -1: jnp.maximum(0.5 - offset, 0.0),
        0: 1.0 - jnp.abs(offset - 0.5),
        1: jnp.maximum(offset - 0.5, 0.0),
    }


def prepare(radius, dry):
    inverse = 1.0 / radius
    square = inverse * inverse
    lowest = dry * dry
    strength = (1.5 * GROWTH_STEP * KAPPA_SOLUTE) * (lowest * dry)
    pull = strength * (square * inverse)
    area = radius * radius
    return (
        area - (GROWTH_STEP * CURVATURE) * inverse,
        (5.0 / 3.0) * pull,
        1.0 / (1.0 + pull * square),
        strength,
        lowest,
        area * radius,
    )


def settle(level, top, inverse_slope, strength, lowest):
    wetted = jnp.maximum((level + top) * inverse_slope, lowest)
    for sweep in range(NEWTON - 1):
        inverse_root = lax.rsqrt(wetted)
        square = inverse_root * inverse_root
        pull = strength * (square * inverse_root)
        wetted = jnp.maximum((level + (5.0 / 3.0) * pull) / (1.0 + pull * square), lowest)
    root = wetted * lax.rsqrt(wetted)
    return root, wetted * root


def differences(near):
    centre = near[0, 0]
    terms = {(0, 0): centre}
    for s in SIDES:
        terms[s, 0] = near[s, 0] - centre
        terms[0, s] = near[0, s] - centre
    for a in SIDES:
        for b in SIDES:
            terms[a, b] = near[a, b] - near[a, 0] - terms[0, b]
    return terms


def interpolate(terms, east, north, reach_x, reach_y):
    right, up = east > 0.5, north > 0.5
    slope_x = jnp.where(right, terms[1, 0], terms[-1, 0])
    slope_y = jnp.where(up, terms[0, 1], terms[0, -1])
    twist = jnp.where(
        right, jnp.where(up, terms[1, 1], terms[1, -1]), jnp.where(up, terms[-1, 1], terms[-1, -1])
    )
    return terms[0, 0] + reach_x * slope_x + reach_y * (slope_y + reach_x * twist)


def match(weight, other, first):
    big = (weight > other) | ((weight == other) & first)
    rate = (-COLLIDE_RATE * LOG2E) * jnp.where(big, weight, other)
    return rate, jnp.where(big, other, 0.0)


def collide(radius, cube, other, rate, eaten):
    total = radius + other
    chance = 1.0 - jnp.exp2(rate * (total * total) * (total * jnp.abs(radius - other)))
    volume = cube + chance * (other * other * other)
    merged = jnp.exp2(jnp.log(volume) * (LOG2E / 3.0))
    return jnp.where(eaten > 0.0, radius, merged), chance * eaten


def spread(parts, dim, index):
    size = parts[0].shape[dim]
    back, ahead = turn(parts[-1], -1, dim), turn(parts[1], 1, dim)
    return parts[0] + jnp.where(index == size - 1, 0.0, back) + jnp.where(index == 0, 0.0, ahead)


def body(
    sizes,
    moist_in, warm_in, size_in, mult_in, dry_in, east_in, north_in, perm_in,
    lx_in, ly_in, lc_in,
    moist_out, warm_out, size_out, mult_out, rec_out, box_out,
    state, drops, perm, lx, ly, lc,
    state_pack, state_x, state_y, diag_pack, diag_in,
    list_pack, list_x, row_pack, row_x, corner_pack, corner_in, col_pack, col_in,
    mask, ready, share, bits, near, late_x,
    in_sem, send_sem, recv_sem,
):
    levels, cx, cy, sd, kx, ky, kc, nx, ny = sizes
    me_x = lax.axis_index("gx")
    me_y = lax.axis_index("gy")
    ys = (1,) if ny == 2 else (1, -1)
    half = cx // 2
    rows = sd * levels
    slots_all = rows * cx
    block = cx * cy
    tall = levels * cx
    deep = kx // cy
    note = cy // 2

    def at(d):
        return (lax.rem(me_x + d[0] + nx, nx), lax.rem(me_y + d[1] + ny, ny))

    for n, source in enumerate((moist_in, warm_in)):
        pltpu.make_async_copy(source, state.at[n], in_sem.at[0]).start()
    for n, source in enumerate((size_in, mult_in, dry_in, east_in, north_in)):
        pltpu.make_async_copy(source, drops.at[n], in_sem.at[1]).start()
    pltpu.make_async_copy(perm_in, perm, in_sem.at[1]).start()
    lists = [
        pltpu.make_async_copy(source.at[0], target, in_sem.at[2 + n])
        for n, (source, target) in enumerate(((lx_in, lx), (ly_in, ly), (lc_in, lc)))
    ]
    for copy in lists:
        copy.start()

    friends = [(dx, 0) for dx in MOVES] + [(dx, dy) for dx in MOVES for dy in ys] + [(0, dy) for dy in ys]
    barrier = pltpu.get_barrier_semaphore()
    for d in friends:
        pl.semaphore_signal(barrier, inc=1, device_id=at(d), device_id_type=MESH)

    def wait_rows(count, sem):
        whole = ready.at[pl.ds(0, count), :]
        pltpu.make_async_copy(whole, whole, sem).wait()

    sent = [0]
    due = [0, 0, 0]

    def count_rows(ref):
        total = 1
        for n in ref.shape:
            total *= n
        return total // cy

    def send(source, target, group, d):
        pltpu.make_async_remote_copy(
            src_ref=source, dst_ref=target, send_sem=send_sem.at[0], recv_sem=recv_sem.at[group],
            device_id=at(d), device_id_type=MESH,
        ).start()
        sent[0] += count_rows(source)
        due[group] += count_rows(source)

    line = iota((cx, cy), 0)
    lane = iota((cx, cy), 1)
    low_half = line < half
    middle = (lane >= cy // 4) & (lane < 3 * cy // 4)

    wait_rows(2 * tall, in_sem.at[0])
    for s in range(2):
        tiles = []
        for f in range(2):
            first, second = state[f, 0], turn(state[f, 1], half, 0)
            tiles.append(jnp.where(low_half, second, first) if s == 0 else jnp.where(low_half, first, second))
            state_pack[s, f] = tiles[f]
        diag_pack[s] = jnp.where(middle, turn(tiles[1], cy // 2, 1), tiles[0])

    pl.semaphore_wait(barrier, len(friends))

    for s, dx in enumerate(MOVES):
        send(state_pack.at[s], state_x.at[s], 1 - s, (dx, 0))
        for t, dy in enumerate(ys):
            send(diag_pack.at[s], diag_in.at[s, t], 1 - s, (dx, dy))

    wait_rows(6 * slots_all, in_sem.at[1])
    for s, (dx, side) in enumerate(zip(MOVES, (cx - 1, 0))):
        for l in range(levels):
            picked = pl.ds(l * cx + side, sd, stride=tall)
            for n in range(5):
                row_pack[s, n, pl.ds(l * sd, sd), :] = drops[n, picked, :]
            row_pack[s, 5, pl.ds(l * sd, sd), :] = perm[picked, :].astype(jnp.float32)
        send(row_pack.at[s], row_x.at[s], 2 - 2 * s, (dx, 0))
    for copy in lists:
        copy.wait()
    for s, dx in enumerate(MOVES):
        for c in range(deep):
            list_pack[s, c : c + 1, :] = lx[s : s + 1, c * cy : (c + 1) * cy].astype(jnp.float32)
        send(list_pack.at[s], list_x.at[s], 2 - 2 * s, (dx, 0))
    for s, dx in enumerate(MOVES):
        tile = None
        for n in range(6):
            for l in range(levels):
                spot = 8 * n + 4 * s + 2 * l
                moved = turn(row_pack[s, n, pl.ds(l * sd, sd), :], spot + 1, 1)
                tile = moved if tile is None else jnp.where(lane >= spot, moved, tile)
        corner_pack[s] = tile
        corner_pack[s, 0:4, note : note + kc] = lc[...].astype(jnp.float32)
        for t, dy in enumerate(ys):
            send(corner_pack.at[s], corner_in.at[s, t], 2 - 2 * s, (dx, dy))
    for t, dy in enumerate(ys):
        send(state, state_y.at[t], 0, (0, dy))
    for n in range(6):
        tile = None
        for i in range(cx):
            for l in range(levels):
                picked = pl.ds(l * cx + i, sd, stride=tall)
                value = drops[n, picked, :] if n < 5 else perm[picked, :].astype(jnp.float32)
                spot = 4 * i + 2 * l
                moved = turn(value, spot + 1, 1)
                tile = moved if tile is None else jnp.where(lane >= spot, moved, tile)
        col_pack[n] = tile
    col_pack[5, 0:2, note : note + ky] = ly[...].astype(jnp.float32)
    for t, dy in enumerate(ys):
        send(col_pack, col_in.at[t], 0, (0, dy))

    def span(n, k):
        return pl.ds(n * slots_all + k * tall, tall)

    order = [perm[k * tall : (k + 1) * tall, :] for k in range(sd)]
    for m in range(sd):
        part = pl.ds(m * tall, tall)
        weight = drops[1, part, :]
        partner = jnp.zeros((tall, cy), jnp.int32)
        first = jnp.zeros((tall, cy), jnp.int32)
        for p in range(sd):
            mine = order[p] == m
            partner = jnp.where(mine, order[p ^ 1], partner)
            if p % 2 == 0:
                first = jnp.where(mine, 1, first)
        other = drops[1, pl.ds(0, tall), :]
        for k in range(1, sd):
            other = jnp.where(partner == k, drops[1, pl.ds(k * tall, tall), :], other)
        rate, eaten = match(weight, other, first > 0)
        for n in range(3):
            bits[n, part, :] = mod(lax.shift_right_logical(partner, jnp.int32(n)), 2)
        for n, value in enumerate(prepare(drops[0, part, :], drops[2, part, :])):
            ready[span(n, m), :] = value
        east, north = drops[3, part, :], drops[4, part, :]
        ready[span(6, m), :] = jnp.abs(east - 0.5)
        ready[span(7, m), :] = jnp.abs(north - 0.5)
        ready[span(8, m), :] = rate
        ready[span(9, m), :] = eaten
        wx, wy = kernel_weights(east), kernel_weights(north)
        for a in SHIFTS:
            along = wx[a] * weight
            for b in SHIFTS:
                share[3 * a + b + 4, part, :] = wy[b] * along

    mask[...] = jnp.ones_like(mask)
    for r, side in enumerate((cx - 1, 0)):
        slots = lx[r : r + 1, :]
        hot_row = iota((rows, kx), 0) == div(slots, block)
        hot_lane = jnp.where(iota((cy, kx), 0) == mod(slots, cy), 1.0, 0.0).astype(jnp.bfloat16)
        named = lax.dot_general(
            jnp.where(hot_row, 1.0, 0.0).astype(jnp.bfloat16), hot_lane,
            (((1,), (1,)), ((), ())), preferred_element_type=jnp.float32,
        )
        mask[pl.ds(side, rows, stride=cx), :] = 1.0 - named

    width = 2 * ky + 4 * kc
    lane_e = iota((1, width), 1)
    high = (lane_e < ky) | ((lane_e >= 2 * ky) & (lane_e < 2 * ky + 2 * kc))
    high_all = jnp.broadcast_to(high, (slots_all, width))
    slots = jnp.concatenate(
        [ly[0:1, :], ly[1:2, :], lc[0:1, :], lc[2:3, :], lc[1:2, :], lc[3:4, :]], 1
    )
    hot_e = jnp.where(iota((slots_all, width), 0) == div(slots, cy), 1.0, 0.0)
    left_high = jnp.max(jnp.where(high_all, hot_e, 0.0), 1, keepdims=True)
    left_low = jnp.max(jnp.where(high_all, 0.0, hot_e), 1, keepdims=True)
    lane_all = iota((slots_all, cy), 1)
    mask[...] = mask[...] * (
        1.0 - jnp.where(lane_all == cy - 1, left_high, jnp.where(lane_all == 0, left_low, 0.0))
    )

    def land(slots, move_x, move_y):
        level = mod(div(slots, block), levels)
        i = mod(mod(div(slots, cy), cx) + move_x, cx)
        target = (level * cx + i) * cy + mod(mod(slots, cy) + move_y, cy)
        return jnp.where(slots >= 0, target, -1)

    def blend(parts, pick_second):
        return parts[0] if len(parts) == 1 else jnp.where(pick_second, parts[1], parts[0])

    left_lanes = lane < cy // 2
    keys = [(a, b) for a in SHIFTS for b in SHIFTS]

    def climate(sides):
        def beyond(l, up, down):
            return jnp.where(low_half, turn(down, half * l, 0), turn(up, half * l, 0))

        fields = []
        for f in range(2):
            fields.append([])
            for l in range(levels):
                across = beyond(l, *(state_x[s, f] for s in sides))
                far = [
                    beyond(l, *(turn(diag_in[s, t], f * (cy // 2), 1) for s in sides)) for t in range(len(ys))
                ]
                side_y = [state_y[t, f, l] for t in range(len(ys))]
                own_half = jnp.concatenate([state[f, l], across], 0)
                other_half = jnp.concatenate([blend(side_y, left_lanes), blend(far, left_lanes)], 0)
                fields[f].append(jnp.concatenate([own_half, other_half], 1))
        mixed = []
        for f in range(2):
            mixed.append([])
            for l in range(levels):
                centre = fields[f][l]
                around = turn(centre, -1, 0) + turn(centre, 1, 0) + turn(centre, -1, 1) + turn(centre, 1, 1)
                stacked = fields[f][min(l + 1, levels - 1)] + fields[f][max(l - 1, 0)]
                mixed[f].append(
                    (1.0 - 4.0 * MIX_HORIZONTAL - 2.0 * MIX_VERTICAL) * centre
                    + MIX_HORIZONTAL * around + MIX_VERTICAL * stacked
                )
        shifted = []
        terms = []
        for l in range(levels):
            vapour, warmth = mixed[0][l], mixed[1][l]
            decay = jnp.exp2((-17.27 * LOG2E) * (warmth - 273.15) / (warmth - 35.86))
            humid = (GROWTH_STEP / EXCESS_FACTOR) * (vapour * decay) - GROWTH_STEP
            shifted.append({b: turn(humid, -b, 1) for b in SHIFTS})
            terms.append(differences({(a, b): turn(shifted[l][b][:, :cy], -a, 0) for a, b in keys}))
        return mixed, shifted, terms

    def pair_up(weight, turns):
        seat = iota((sd, cy), 0)
        rank = jnp.zeros((sd, cy), jnp.int32)
        for p in range(1, sd):
            rank = jnp.where(jnp.broadcast_to(turns[p : p + 1], (sd, cy)) == seat, p, rank)
        partner = take(turns, rank ^ 1, 0)
        return partner, match(weight, take(weight, partner, 0), mod(rank, 2) == 0)

    def finish(radius, weight, dry, east, north, turns, around):
        base, top, inverse_slope, strength, lowest, cube = prepare(radius, dry)
        level = base + interpolate(around, east, north, jnp.abs(east - 0.5), jnp.abs(north - 0.5))
        root, volume = settle(level, top, inverse_slope, strength, lowest)
        partner, (rate, eaten) = pair_up(weight, turns.astype(jnp.int32))
        after, lost = collide(root, volume, take(root, partner, 0), rate, eaten)
        return weight * (volume - cube), after, weight - lost

    def side_rows(s):
        home = cx - 1 if s == 0 else 0
        fallen = []
        for l in range(levels):
            stretch = pl.ds(l * sd, sd)
            values = [row_x[s, n, stretch, :] for n in range(6)]
            around = {
                key: jnp.broadcast_to(near[l, n, home : home + 1, :], (sd, cy)) for n, key in enumerate(keys)
            }
            condensed, radius, weight = finish(*values, around)
            late_x[s, 0, stretch, :] = radius
            late_x[s, 1, stretch, :] = weight
            wx, wy = kernel_weights(values[3]), kernel_weights(values[4])
            along = wx[MOVES[s]] * condensed
            fallen.append(spread({b: jnp.sum(wy[b] * along, 0, keepdims=True) for b in SHIFTS}, 1, lane[0:1]))
        return fallen

    def side_records(s):
        slots = list_x[s].astype(jnp.int32)
        level = mod(div(slots, block), levels)
        row = jnp.where(slots >= 0, level * sd + div(slots, block * levels), -1)
        column = mod(slots, cy)
        for n in (2, 3, 4, 0, 1):
            got = jnp.zeros((deep, cy), jnp.float32)
            for r in range(rows):
                source = late_x[s, n, r : r + 1, :] if n < 2 else row_x[s, n, r : r + 1, :]
                got = jnp.where(row == r, take(jnp.broadcast_to(source, (deep, cy)), column, 1), got)
            rec_out[n, :, pl.ds(s * kx, kx)] = got.reshape(1, kx)
        box_out[:, pl.ds(s * kx, kx)] = land(slots, MOVES[s], 0).reshape(1, kx)

    wait_rows(due[0], recv_sem.at[0])
    _, _, terms = climate((1, 1))
    for l in range(levels):
        for n, key in enumerate(keys):
            near[l, n] = terms[l][key][cx:]
    arrive = [None, side_rows(1)]
    side_records(1)

    wait_rows(due[1], recv_sem.at[1])
    mixed, shifted, terms = climate((0, 1))
    window = {key: jnp.concatenate([t[key][:cx] for t in terms], 0) for key in keys}
    for l in range(levels):
        for n, key in enumerate(keys):
            near[l, n] = terms[l][key][cx:]
        moist_out[l] = mixed[0][l][:cx, :cy]
        warm_out[l] = mixed[1][l][:cx, :cy]

    odd_lane = mod(lane, 2) == 1
    second_level = mod(div(lane, 2), 2) == 1
    ends = jnp.where(odd_lane, 0, cy - 1)
    step = mod(div(lane, 4), cx)
    column = {}
    for b in SHIFTS:
        tiles = []
        for piece in (slice(0, cx), slice(cx, 2 * cx)):
            pair = [take(shifted[l][b][piece, cy:], ends, 1) for l in range(levels)]
            tiles.append(take(jnp.where(second_level, pair[1], pair[0]), step, 0))
        column[b] = jnp.where(lane < 4 * cx, tiles[0], tiles[1])
    col_terms = differences({(a, b): turn(column[b], -4 * a, 1) for a, b in keys})

    grown = []
    cubes = []
    deposit = {}
    for k in range(sd):
        part = pl.ds(k * tall, tall)
        base, top, inverse_slope, strength, lowest, cube, reach_x, reach_y = (
            ready[span(n, k), :] for n in range(8)
        )
        level = base + interpolate(window, drops[3, part, :], drops[4, part, :], reach_x, reach_y)
        root, volume = settle(level, top, inverse_slope, strength, lowest)
        gain = volume - cube
        for a, b in keys:
            term = share[3 * a + b + 4, part, :] * gain
            deposit[a, b] = term if k == 0 else deposit[a, b] + term
        grown.append(root)
        cubes.append(volume)

    own = []
    for l in range(levels):
        inner = {b: spread({a: deposit[a, b][l * cx : (l + 1) * cx] for a in SHIFTS}, 0, line) for b in SHIFTS}
        own.append(spread(inner, 1, lane))

    for m in range(sd):
        part = pl.ds(m * tall, tall)
        found = grown
        for n in range(3):
            odd = bits[n, part, :] > 0
            found = [jnp.where(odd, found[2 * i + 1], found[2 * i]) for i in range(len(found) // 2)]
        radius, lost = collide(grown[m], cubes[m], found[0], ready[span(8, m), :], ready[span(9, m), :])
        size_out[part, :] = radius
        mult_out[part, :] = mask[part, :] * (drops[1, part, :] - lost)

    wait_rows(due[2], recv_sem.at[2])
    arrive[0] = side_rows(0)

    corner = [blend([corner_in[s, t] for t in range(len(ys))], odd_lane) for s in range(2)]
    values = []
    for n in range(6):
        beside = blend([col_in[t, n] for t in range(len(ys))], odd_lane)
        below = jnp.where(lane < 4 * cx, beside, turn(corner[1], 4 * (cx - 1) - 8 * n, 1))
        values.append(jnp.where(lane >= cy - 4, turn(corner[0], cy - 4 - 8 * n, 1), below))
    condensed, radius, weight = finish(*values, col_terms)
    wx, wy = kernel_weights(values[3]), kernel_weights(values[4])
    across = jnp.where(odd_lane, wy[-1], wy[1]) * condensed
    fallen = sum(turn(jnp.sum(wx[a] * across, 0, keepdims=True), 4 * a, 1) for a in SHIFTS)
    outer = jnp.where(lane == cy - 1, 1, 0)
    for l in range(levels):
        total = own[l] + jnp.where(line == 0, arrive[0][l], jnp.where(line == cx - 1, arrive[1][l], 0.0))
        sent_in = take(jnp.broadcast_to(fallen, (cx, cy)), 4 * line + 2 * l + outer, 1)
        total = total + jnp.where((lane == 0) | (lane == cy - 1), sent_in, 0.0)
        moist_out[l] = moist_out[l] - VAPOUR_PER_SOURCE * total
        warm_out[l] = warm_out[l] + WARMING_FACTOR * total

    side_records(0)

    slots = jnp.concatenate(
        [col_in[d if len(ys) == 2 else 0, 5, d : d + 1, note : note + ky] for d in range(2)]
        + [
            corner_in[s, d if len(ys) == 2 else 0, 2 * s + d : 2 * s + d + 1, note : note + kc]
            for d in range(2) for s in range(2)
        ],
        1,
    ).astype(jnp.int32)
    face = lane_e < 2 * ky
    which = div(lane_e - 2 * ky, kc)
    minus_x = mod(which, 2)
    minus_y = jnp.where(face, jnp.where(lane_e < ky, 0, 1), div(which, 2))
    move_x = jnp.where(face, 0, 1 - 2 * minus_x)
    live = slots >= 0
    level = mod(div(slots, block), levels)
    place = jnp.where(face, mod(div(slots, cy), cx), jnp.where(minus_x == 0, cy // 4 - 1, cx))
    spot = jnp.broadcast_to(jnp.where(live, 4 * place + 2 * level + minus_y, 0), (sd, width))
    seat = iota((sd, width), 0) == jnp.where(live, div(slots, block * levels), -1)
    for n, value in enumerate((radius, weight, values[2], values[3], values[4])):
        rec_out[n, :, pl.ds(2 * kx, width)] = jnp.sum(jnp.where(seat, take(value, spot, 1), 0.0), 0, keepdims=True)
    box_out[:, pl.ds(2 * kx, width)] = land(slots, move_x, 1 - 2 * minus_y)

    wait_rows(sent[0], send_sem.at[0])


def publish(*refs):
    count = len(refs) // 2
    sems = refs[-1]
    copies = [
        pltpu.make_async_copy(refs[n], refs[count + n], sems.at[n]) for n in range(count)
    ]
    for copy in copies:
        copy.start()
    for copy in copies:
        copy.wait()


def per_device(nx, ny, moist, warm, size, mult, dry, east, north, perm, lx, ly, lc):
    levels, cx, cy = moist.shape
    sd = size.shape[0]
    kx, ky, kc = lx.shape[2], ly.shape[2], lc.shape[2]
    narr = 2 * kx + 2 * ky + 4 * kc
    slots = sd * levels * cx
    flat = [x.reshape(slots, cy) for x in (size, mult, dry, east, north, perm)]
    f32, i32 = jnp.float32, jnp.int32
    any_space = pl.BlockSpec(memory_space=pl.ANY)
    vmem_space = pl.BlockSpec(memory_space=pltpu.VMEM)
    dma = pltpu.SemaphoreType.DMA
    shapes = (
        ((levels, cx, cy), f32),
        ((levels, cx, cy), f32),
        ((slots, cy), f32),
        ((slots, cy), f32),
        ((5, 1, narr), f32),
        ((1, narr), i32),
    )
    n_y = 1 if ny == 2 else 2
    outs = pl.pallas_call(
        functools.partial(body, (levels, cx, cy, sd, kx, ky, kc, nx, ny)),
        out_shape=tuple(pltpu.VMEM(*s) for s in shapes),
        in_specs=[any_space] * 11,
        out_specs=[vmem_space] * 6,
        scratch_shapes=[
            pltpu.VMEM((2, levels, cx, cy), f32),
            pltpu.VMEM((5, slots, cy), f32),
            pltpu.VMEM((slots, cy), i32),
            pltpu.VMEM((2, kx), i32),
            pltpu.VMEM((2, ky), i32),
            pltpu.VMEM((4, kc), i32),
            pltpu.VMEM((2, 2, cx, cy), f32),
            pltpu.VMEM((2, 2, cx, cy), f32),
            pltpu.VMEM((n_y, 2, levels, cx, cy), f32),
            pltpu.VMEM((2, cx, cy), f32),
            pltpu.VMEM((2, n_y, cx, cy), f32),
            pltpu.VMEM((2, kx // cy, cy), f32),
            pltpu.VMEM((2, kx // cy, cy), f32),
            pltpu.VMEM((2, 6, sd * levels, cy), f32),
            pltpu.VMEM((2, 6, sd * levels, cy), f32),
            pltpu.VMEM((2, sd, cy), f32),
            pltpu.VMEM((2, n_y, sd, cy), f32),
            pltpu.VMEM((6, sd, cy), f32),
            pltpu.VMEM((n_y, 6, sd, cy), f32),
            pltpu.VMEM((slots, cy), f32),
            pltpu.VMEM((10 * slots, cy), f32),
            pltpu.VMEM((9, slots, cy), f32),
            pltpu.VMEM((3, slots, cy), i32),
            pltpu.VMEM((levels, 9, cx, cy), f32),
            pltpu.VMEM((2, 2, sd * levels, cy), f32),
            dma((5,)), dma((1,)), dma((3,)),
        ],
        compiler_params=pltpu.CompilerParams(collective_id=0, has_side_effects=True),
    )(moist, warm, *flat, lx, ly, lc)
    outs = pl.pallas_call(
        publish,
        out_shape=tuple(jax.ShapeDtypeStruct(*s) for s in shapes),
        in_specs=[vmem_space] * 6,
        out_specs=[any_space] * 6,
        scratch_shapes=[dma((6,))],
    )(*[pltpu.with_memory_space_constraint(x, pltpu.VMEM) for x in outs])
    return (
        outs[0], outs[1], outs[2].reshape(size.shape), outs[3].reshape(size.shape), outs[4], outs[5],
    )


def solution(mesh):
    cell, drop, lists = P(None, "gx", "gy"), P(None, None, "gx", "gy"), P("gx", None, "gy")
    return jax.shard_map(
        functools.partial(per_device, mesh.shape["gx"], mesh.shape["gy"]),
        mesh=mesh,
        in_specs=(cell,) * 2 + (drop,) * 6 + (lists,) * 3,
        out_specs=(cell, cell, drop, drop, cell, P("gx", "gy")),
        check_vma=False,
    )
```

```python
import functools
import math

import jax
import jax.numpy as jnp
from jax import lax
from jax.experimental import pallas as pl
from jax.experimental.pallas import tpu as pltpu
from jax.sharding import PartitionSpec as P

NEWTON = 4
MIX_HORIZONTAL = 0.2
MIX_VERTICAL = 0.05
EXCESS_FACTOR = 4.2222
CURVATURE = 0.0012
KAPPA_SOLUTE = 0.6
GROWTH_STEP = 200.0
COLLIDE_RATE = 4e-07
VAPOUR_PER_SOURCE = 0.001
WARMING_FACTOR = 0.00249
LOG2E = math.log2(math.e)

MESH = pl.DeviceIdType.MESH
SHIFTS = (-1, 0, 1)
SIDES = (1, -1)
MOVES = (1, -1)


def div(x, n):
    return lax.shift_right_arithmetic(x, jnp.int32(n.bit_length() - 1))


def mod(x, n):
    return lax.bitwise_and(x, jnp.int32(n - 1))


def iota(shape, dim):
    return lax.broadcasted_iota(jnp.int32, shape, dim)


def turn(x, shift, dim):
    shift %= x.shape[dim]
    return pltpu.roll(x, shift, dim) if shift else x


def take(x, index, dim):
    return jnp.take_along_axis(x, index, axis=dim)


def kernel_weights(offset):
    return {
        -1: jnp.maximum(0.5 - offset, 0.0),
        0: 1.0 - jnp.abs(offset - 0.5),
        1: jnp.maximum(offset - 0.5, 0.0),
    }


def prepare(radius, dry):
    inverse = 1.0 / radius
    square = inverse * inverse
    lowest = dry * dry
    strength = (1.5 * GROWTH_STEP * KAPPA_SOLUTE) * (lowest * dry)
    pull = strength * (square * inverse)
    area = radius * radius
    return (
        area - (GROWTH_STEP * CURVATURE) * inverse,
        (5.0 / 3.0) * pull,
        1.0 / (1.0 + pull * square),
        strength,
        lowest,
        area * radius,
    )


def settle(level, top, inverse_slope, strength, lowest):
    wetted = jnp.maximum((level + top) * inverse_slope, lowest)
    for sweep in range(NEWTON - 1):
        inverse_root = lax.rsqrt(wetted)
        square = inverse_root * inverse_root
        pull = strength * (square * inverse_root)
        wetted = jnp.maximum((level + (5.0 / 3.0) * pull) / (1.0 + pull * square), lowest)
    root = wetted * lax.rsqrt(wetted)
    return root, wetted * root


def differences(near):
    centre = near[0, 0]
    terms = {(0, 0): centre}
    for s in SIDES:
        terms[s, 0] = near[s, 0] - centre
        terms[0, s] = near[0, s] - centre
    for a in SIDES:
        for b in SIDES:
            terms[a, b] = near[a, b] - near[a, 0] - terms[0, b]
    return terms


def interpolate(terms, east, north, reach_x, reach_y):
    right, up = east > 0.5, north > 0.5
    slope_x = jnp.where(right, terms[1, 0], terms[-1, 0])
    slope_y = jnp.where(up, terms[0, 1], terms[0, -1])
    twist = jnp.where(
        right, jnp.where(up, terms[1, 1], terms[1, -1]), jnp.where(up, terms[-1, 1], terms[-1, -1])
    )
    return terms[0, 0] + reach_x * slope_x + reach_y * (slope_y + reach_x * twist)


def match(weight, other, first):
    big = (weight > other) | ((weight == other) & first)
    rate = (-COLLIDE_RATE * LOG2E) * jnp.where(big, weight, other)
    return rate, jnp.where(big, other, 0.0)


def collide(radius, cube, other, rate, eaten):
    total = radius + other
    chance = 1.0 - jnp.exp2(rate * (total * total) * (total * jnp.abs(radius - other)))
    volume = cube + chance * (other * other * other)
    merged = jnp.exp2(jnp.log(volume) * (LOG2E / 3.0))
    return jnp.where(eaten > 0.0, radius, merged), chance * eaten


def spread(parts, dim, index):
    size = parts[0].shape[dim]
    back, ahead = turn(parts[-1], -1, dim), turn(parts[1], 1, dim)
    return parts[0] + jnp.where(index == size - 1, 0.0, back) + jnp.where(index == 0, 0.0, ahead)


def body(
    sizes,
    moist_in, warm_in, size_in, mult_in, dry_in, east_in, north_in, perm_in,
    size_cells, mult_cells, dry_cells, east_cells, north_cells, perm_cells,
    lx_in, ly_in, lc_in,
    moist_out, warm_out, size_out, mult_out, rec_out, box_out,
    state, drops, perm, lx, ly, lc,
    state_x, state_y, diag_in, list_pack, list_x,
    row_pack, row_x, turn_pack, turn_x, corner_pack, corner_in, col_pack, col_in,
    mask, ready, share, bits, near, late_x,
    in_sem, send_sem, recv_sem,
):
    levels, cx, cy, sd, kx, ky, kc, nx, ny = sizes
    me_x = lax.axis_index("gx")
    me_y = lax.axis_index("gy")
    ys = (1,) if ny == 2 else (1, -1)
    half = cx // 2
    rows = sd * levels
    slots_all = rows * cx
    block = cx * cy
    tall = levels * cx
    deep = kx // cy
    note = cy // 2
    edges = (cx - 1, 0)
    bands = (pl.ds(cx - 3, 3), pl.ds(0, 3))

    def at(d):
        return (lax.rem(me_x + d[0] + nx, nx), lax.rem(me_y + d[1] + ny, ny))

    def wait_rows(count, sem):
        whole = ready.at[pl.ds(0, count), :]
        pltpu.make_async_copy(whole, whole, sem).wait()

    def count_rows(ref):
        total = 1
        for n in ref.shape:
            total *= n
        return total // cy

    brought = [0, 0, 0]

    def bring(source, target, group):
        pltpu.make_async_copy(source, target, in_sem.at[group]).start()
        brought[group] += count_rows(target)

    bring(moist_in, state.at[0], 0)
    bring(warm_in, state.at[1], 0)
    cells = (size_cells, dry_cells, east_cells, north_cells, mult_cells)
    for s in range(2):
        for l in range(levels):
            stretch = pl.ds(l * sd, sd)
            for n, source in enumerate(cells):
                bring(source.at[:, l, edges[s], :], row_pack.at[s, n, stretch, :], 1)
            bring(perm_cells.at[:, l, edges[s], :], turn_pack.at[s, stretch, :], 1)
        bring(lx_in.at[0, pl.ds(s, 1), :], list_pack.at[s], 1)

    friends = [(dx, 0) for dx in MOVES] + [(dx, dy) for dx in MOVES for dy in ys] + [(0, dy) for dy in ys]
    barrier = pltpu.get_barrier_semaphore()
    for d in friends:
        pl.semaphore_signal(barrier, inc=1, device_id=at(d), device_id_type=MESH)

    for n, source in enumerate((size_in, mult_in, dry_in, east_in, north_in)):
        bring(source, drops.at[n], 2)
    bring(perm_in, perm, 2)
    lists = [
        pltpu.make_async_copy(source.at[0], target, in_sem.at[3 + n])
        for n, (source, target) in enumerate(((lx_in, lx), (ly_in, ly), (lc_in, lc)))
    ]
    for copy in lists:
        copy.start()

    sent = [0]
    due = [0, 0, 0, 0]

    def send(source, target, group, d):
        pltpu.make_async_remote_copy(
            src_ref=source, dst_ref=target, send_sem=send_sem.at[0], recv_sem=recv_sem.at[group],
            device_id=at(d), device_id_type=MESH,
        ).start()
        sent[0] += count_rows(source)
        due[group] += count_rows(source)

    line = iota((cx, cy), 0)
    lane = iota((cx, cy), 1)
    low_half = line < half

    def send_fields(s):
        own, far = state.at[:, :, bands[s], :], MOVES[s]
        group = (1, 0)[s]
        send(own, state_x.at[s, :, :, bands[s], :], group, (far, 0))
        for t, dy in enumerate(ys):
            send(own, diag_in.at[s, t, :, :, bands[s], :], group, (far, dy))

    def send_rows(s):
        first, second = ((2, 3), (0, 0))[s]
        send(row_pack.at[s, 0:4], row_x.at[s, 0:4], first, (MOVES[s], 0))
        send(list_pack.at[s], list_x.at[s], first, (MOVES[s], 0))
        send(row_pack.at[s, 4], row_x.at[s, 4], second, (MOVES[s], 0))
        send(turn_pack.at[s], turn_x.at[s], second, (MOVES[s], 0))

    def send_corner(s):
        tile = None
        for n in range(6):
            for l in range(levels):
                stretch = pl.ds(l * sd, sd)
                value = row_pack[s, n, stretch, :] if n < 5 else turn_pack[s, stretch, :].astype(jnp.float32)
                spot = 8 * n + 4 * s + 2 * l
                moved = turn(value, spot + 1, 1)
                tile = moved if tile is None else jnp.where(lane >= spot, moved, tile)
        corner_pack[s] = tile
        corner_pack[s, 0:4, note : note + kc] = lc[...].astype(jnp.float32)
        for t, dy in enumerate(ys):
            send(corner_pack.at[s], corner_in.at[s, t], (2, 0)[s], (MOVES[s], dy))

    wait_rows(brought[0], in_sem.at[0])
    pl.semaphore_wait(barrier, len(friends))
    send_fields(0)
    wait_rows(brought[1], in_sem.at[1])
    send_rows(0)
    for t, dy in enumerate(ys):
        send(state, state_y.at[t], 0, (0, dy))
    for copy in lists:
        copy.wait()
    send_corner(0)
    send_fields(1)
    send_rows(1)
    send_corner(1)
    wait_rows(brought[2], in_sem.at[2])
    attributes = (0, 2, 3, 4, 1)
    for n in range(6):
        tile = None
        for i in range(cx):
            for l in range(levels):
                picked = pl.ds(l * cx + i, sd, stride=tall)
                value = drops[attributes[n], picked, :] if n < 5 else perm[picked, :].astype(jnp.float32)
                spot = 4 * i + 2 * l
                moved = turn(value, spot + 1, 1)
                tile = moved if tile is None else jnp.where(lane >= spot, moved, tile)
        col_pack[n] = tile
    col_pack[5, 0:2, note : note + ky] = ly[...].astype(jnp.float32)
    for t, dy in enumerate(ys):
        send(col_pack, col_in.at[t], 2, (0, dy))

    def span(n, k):
        return pl.ds(n * slots_all + k * tall, tall)

    order = [perm[k * tall : (k + 1) * tall, :] for k in range(sd)]
    for m in range(sd):
        part = pl.ds(m * tall, tall)
        weight = drops[1, part, :]
        partner = jnp.zeros((tall, cy), jnp.int32)
        first = jnp.zeros((tall, cy), jnp.int32)
        for p in range(sd):
            mine = order[p] == m
            partner = jnp.where(mine, order[p ^ 1], partner)
            if p % 2 == 0:
                first = jnp.where(mine, 1, first)
        other = drops[1, pl.ds(0, tall), :]
        for k in range(1, sd):
            other = jnp.where(partner == k, drops[1, pl.ds(k * tall, tall), :], other)
        rate, eaten = match(weight, other, first > 0)
        for n in range(3):
            bits[n, part, :] = mod(lax.shift_right_logical(partner, jnp.int32(n)), 2)
        for n, value in enumerate(prepare(drops[0, part, :], drops[2, part, :])):
            ready[span(n, m), :] = value
        east, north = drops[3, part, :], drops[4, part, :]
        ready[span(6, m), :] = jnp.abs(east - 0.5)
        ready[span(7, m), :] = jnp.abs(north - 0.5)
        ready[span(8, m), :] = rate
        ready[span(9, m), :] = eaten
        wx, wy = kernel_weights(east), kernel_weights(north)
        for a in SHIFTS:
            along = wx[a] * weight
            for b in SHIFTS:
                share[3 * a + b + 4, part, :] = wy[b] * along

    mask[...] = jnp.ones_like(mask)
    for r, side in enumerate(edges):
        slots = lx[r : r + 1, :]
        hot_row = iota((rows, kx), 0) == div(slots, block)
        hot_lane = jnp.where(iota((cy, kx), 0) == mod(slots, cy), 1.0, 0.0).astype(jnp.bfloat16)
        named = lax.dot_general(
            jnp.where(hot_row, 1.0, 0.0).astype(jnp.bfloat16), hot_lane,
            (((1,), (1,)), ((), ())), preferred_element_type=jnp.float32,
        )
        mask[pl.ds(side, rows, stride=cx), :] = 1.0 - named

    width = 2 * ky + 4 * kc
    lane_e = iota((1, width), 1)
    high = (lane_e < ky) | ((lane_e >= 2 * ky) & (lane_e < 2 * ky + 2 * kc))
    high_all = jnp.broadcast_to(high, (slots_all, width))
    slots = jnp.concatenate(
        [ly[0:1, :], ly[1:2, :], lc[0:1, :], lc[2:3, :], lc[1:2, :], lc[3:4, :]], 1
    )
    hot_e = jnp.where(iota((slots_all, width), 0) == div(slots, cy), 1.0, 0.0)
    left_high = jnp.max(jnp.where(high_all, hot_e, 0.0), 1, keepdims=True)
    left_low = jnp.max(jnp.where(high_all, 0.0, hot_e), 1, keepdims=True)
    lane_all = iota((slots_all, cy), 1)
    mask[...] = mask[...] * (
        1.0 - jnp.where(lane_all == cy - 1, left_high, jnp.where(lane_all == 0, left_low, 0.0))
    )

    def land(slots, move_x, move_y):
        level = mod(div(slots, block), levels)
        i = mod(mod(div(slots, cy), cx) + move_x, cx)
        target = (level * cx + i) * cy + mod(mod(slots, cy) + move_y, cy)
        return jnp.where(slots >= 0, target, -1)

    def blend(parts, pick_second):
        return parts[0] if len(parts) == 1 else jnp.where(pick_second, parts[1], parts[0])

    left_lanes = lane < cy // 2
    odd_lane = mod(lane, 2) == 1
    second_level = mod(div(lane, 2), 2) == 1
    ends = jnp.where(odd_lane, 0, cy - 1)
    step = mod(div(lane, 4), cx)
    keys = [(a, b) for a in SHIFTS for b in SHIFTS]

    def climate(fields):
        mixed = []
        for f in range(2):
            mixed.append([])
            for l in range(levels):
                centre = fields[f][l]
                around = turn(centre, -1, 0) + turn(centre, 1, 0) + turn(centre, -1, 1) + turn(centre, 1, 1)
                stacked = fields[f][min(l + 1, levels - 1)] + fields[f][max(l - 1, 0)]
                mixed[f].append(
                    (1.0 - 4.0 * MIX_HORIZONTAL - 2.0 * MIX_VERTICAL) * centre
                    + MIX_HORIZONTAL * around + MIX_VERTICAL * stacked
                )
        shifted = []
        terms = []
        for l in range(levels):
            vapour, warmth = mixed[0][l], mixed[1][l]
            decay = jnp.exp2((-17.27 * LOG2E) * (warmth - 273.15) / (warmth - 35.86))
            humid = (GROWTH_STEP / EXCESS_FACTOR) * (vapour * decay) - GROWTH_STEP
            shifted.append({b: turn(humid, -b, 1) for b in SHIFTS})
            terms.append(differences({(a, b): turn(shifted[l][b][:, :cy], -a, 0) for a, b in keys}))
        return mixed, shifted, terms

    def columns(shifted, b, piece):
        pair = [take(shifted[l][b][piece, cy:], ends, 1) for l in range(levels)]
        return take(jnp.where(second_level, pair[1], pair[0]), step, 0)

    def mate(weight, turns):
        seat = iota((sd, cy), 0)
        rank = jnp.zeros((sd, cy), jnp.int32)
        for p in range(1, sd):
            rank = jnp.where(jnp.broadcast_to(turns[p : p + 1], (sd, cy)) == seat, p, rank)
        partner = take(turns, rank ^ 1, 0)
        return partner, match(weight, take(weight, partner, 0), mod(rank, 2) == 0)

    def expand(prepared, east, north, around):
        base, top, inverse_slope, strength, lowest, cube = prepared
        level = base + interpolate(around, east, north, jnp.abs(east - 0.5), jnp.abs(north - 0.5))
        root, volume = settle(level, top, inverse_slope, strength, lowest)
        return root, volume, volume - cube

    def merge(root, volume, weight, mated):
        partner, (rate, eaten) = mated
        after, lost = collide(root, volume, take(root, partner, 0), rate, eaten)
        return after, weight - lost

    def surround(l, r):
        return {key: jnp.broadcast_to(near[l, n, r : r + 1, :], (sd, cy)) for n, key in enumerate(keys)}

    def side_growth(s):
        found = []
        for l in range(levels):
            radius, dry, east, north = (row_x[s, n, pl.ds(l * sd, sd), :] for n in range(4))
            found.append(expand(prepare(radius, dry), east, north, surround(l, edges[s])))
        return found

    def side_rows(s, found):
        fallen = []
        for l in range(levels):
            stretch = pl.ds(l * sd, sd)
            root, volume, gain = found[l]
            weight = row_x[s, 4, stretch, :]
            radius, weight_left = merge(root, volume, weight, mate(weight, turn_x[s, stretch, :]))
            late_x[s, 0, stretch, :] = radius
            late_x[s, 1, stretch, :] = weight_left
            wx, wy = kernel_weights(row_x[s, 2, stretch, :]), kernel_weights(row_x[s, 3, stretch, :])
            along = wx[MOVES[s]] * (weight * gain)
            fallen.append(jnp.sum(spread({b: wy[b] * along for b in SHIFTS}, 1, lane), 0, keepdims=True))
        return fallen

    def side_records(s, fields):
        slots = list_x[s].reshape(deep, cy)
        level = mod(div(slots, block), levels)
        row = jnp.where(slots >= 0, level * sd + div(slots, block * levels), -1)
        column = mod(slots, cy)
        for n, source, from_n in fields:
            got = jnp.zeros((deep, cy), jnp.float32)
            for r in range(rows):
                value = jnp.broadcast_to(source[s, from_n, r : r + 1, :], (deep, cy))
                got = jnp.where(row == r, take(value, column, 1), got)
            rec_out[n, :, pl.ds(s * kx, kx)] = got.reshape(1, kx)
        return slots

    still = [(2, row_x, 1), (3, row_x, 2), (4, row_x, 3)]
    moving = [(0, late_x, 0), (1, late_x, 1)]

    wait_rows(due[0], recv_sem.at[0])
    fields = []
    for f in range(2):
        fields.append([])
        for l in range(levels):
            own_half = jnp.concatenate([state[f, l], state_x[1, f, l]], 0)
            side_y = blend([state_y[t, f, l] for t in range(len(ys))], left_lanes)
            far = blend([diag_in[1, t, f, l] for t in range(len(ys))], left_lanes)
            fields[f].append(jnp.concatenate([own_half, jnp.concatenate([side_y, far], 0)], 1))
    mixed, shifted, terms = climate(fields)
    window = {key: jnp.concatenate([t[key][:cx] for t in terms], 0) for key in keys}
    for l in range(levels):
        for n, key in enumerate(keys):
            near[l, n] = terms[l][key][cx:]
        moist_out[l] = mixed[0][l][:cx, :cy]
        warm_out[l] = mixed[1][l][:cx, :cy]
    inside = {
        b: jnp.where(
            lane < 4 * cx, columns(shifted, b, slice(0, cx)), columns(shifted, b, slice(cx, 2 * cx))
        )
        for b in SHIFTS
    }
    fallen = [None, side_rows(1, side_growth(1))]
    slots = side_records(1, still + moving)
    box_out[:, pl.ds(kx, kx)] = land(slots, -1, 0).reshape(1, kx)

    grown = []
    cubes = []
    deposit = {}
    for k in range(sd):
        part = pl.ds(k * tall, tall)
        base, top, inverse_slope, strength, lowest, cube, reach_x, reach_y = (
            ready[span(n, k), :] for n in range(8)
        )
        level = base + interpolate(window, drops[3, part, :], drops[4, part, :], reach_x, reach_y)
        root, volume = settle(level, top, inverse_slope, strength, lowest)
        gain = volume - cube
        for a, b in keys:
            term = share[3 * a + b + 4, part, :] * gain
            deposit[a, b] = term if k == 0 else deposit[a, b] + term
        grown.append(root)
        cubes.append(volume)

    own = []
    for l in range(levels):
        inner = {}
        for b in SHIFTS:
            parts = {a: jnp.where(line < 2, 0.0, deposit[a, b][l * cx : (l + 1) * cx]) for a in SHIFTS}
            inner[b] = spread(parts, 0, line)
        own.append(spread(inner, 1, lane) + jnp.where(line == cx - 1, fallen[1][l], 0.0))

    for m in range(sd):
        part = pl.ds(m * tall, tall)
        found = grown
        for n in range(3):
            odd = bits[n, part, :] > 0
            found = [jnp.where(odd, found[2 * i + 1], found[2 * i]) for i in range(len(found) // 2)]
        radius, lost = collide(grown[m], cubes[m], found[0], ready[span(8, m), :], ready[span(9, m), :])
        size_out[part, :] = radius
        mult_out[part, :] = mask[part, :] * (drops[1, part, :] - lost)

    redo = [(l, i) for l in range(levels) for i in range(2)]
    waiting = {}
    for l, i in redo:
        picked = pl.ds(l * cx + i, sd, stride=tall)
        radius, weight, dry, east, north = (drops[n, picked, :] for n in range(5))
        waiting[l, i] = (
            prepare(radius, dry), weight, east, north, mate(weight, perm[picked, :]), mask[picked, :]
        )

    wait_rows(due[1], recv_sem.at[1])
    fields = []
    for f in range(2):
        fields.append([])
        for l in range(levels):
            side_y = blend([state_y[t, f, l] for t in range(len(ys))], left_lanes)
            far = blend([diag_in[0, t, f, l] for t in range(len(ys))], left_lanes)
            fields[f].append(
                jnp.concatenate(
                    [jnp.where(low_half, state[f, l], state_x[0, f, l]), jnp.where(low_half, side_y, far)], 1
                )
            )
    mixed, shifted, terms = climate(fields)
    fresh = (lane < 8) | (lane >= cy - 8)
    column = {b: jnp.where(fresh, columns(shifted, b, slice(0, cx)), inside[b]) for b in SHIFTS}
    col_terms = differences({(a, b): turn(column[b], -4 * a, 1) for a, b in keys})
    for l in range(levels):
        for n, key in enumerate(keys):
            near[l, n] = terms[l][key]
        moist_out[l, 0:1, :] = mixed[0][l][0:1, :cy]
        warm_out[l, 0:1, :] = mixed[1][l][0:1, :cy]
    for l in range(levels):
        landing = [None] * 3
        for i in range(2):
            picked = pl.ds(l * cx + i, sd, stride=tall)
            prepared, weight, east, north, mated, keep = waiting[l, i]
            root, volume, gain = expand(prepared, east, north, surround(l, i))
            radius, weight_left = merge(root, volume, weight, mated)
            size_out[picked, :] = radius
            mult_out[picked, :] = keep * weight_left
            wx, wy = kernel_weights(east), kernel_weights(north)
            for a in SHIFTS:
                if i + a < 0:
                    continue
                along = wx[a] * (weight * gain)
                parts = {b: wy[b] * along for b in SHIFTS}
                if landing[i + a] is not None:
                    parts = {b: parts[b] + landing[i + a][b] for b in SHIFTS}
                landing[i + a] = parts
        for r in range(3):
            added = jnp.sum(spread(landing[r], 1, lane), 0, keepdims=True)
            own[l] = own[l] + jnp.where(line == r, added, 0.0)

    wait_rows(due[2], recv_sem.at[2])
    side = side_growth(0)
    corner = [blend([corner_in[s, t] for t in range(len(ys))], odd_lane) for s in range(2)]
    values = []
    for n in range(6):
        beside = blend([col_in[t, n] for t in range(len(ys))], odd_lane)
        below = jnp.where(lane < 4 * cx, beside, turn(corner[1], 4 * (cx - 1) - 8 * n, 1))
        values.append(jnp.where(lane >= cy - 4, turn(corner[0], cy - 4 - 8 * n, 1), below))
    radius, dry, east, north, weight, turns = values
    root, volume, gain = expand(prepare(radius, dry), east, north, col_terms)
    radius, weight_left = merge(root, volume, weight, mate(weight, turns.astype(jnp.int32)))
    wx, wy = kernel_weights(east), kernel_weights(north)
    across = jnp.where(odd_lane, wy[-1], wy[1]) * (weight * gain)
    rain = sum(turn(jnp.sum(wx[a] * across, 0, keepdims=True), 4 * a, 1) for a in SHIFTS)
    outer = jnp.where(lane == cy - 1, 1, 0)
    for l in range(levels):
        sent_in = take(jnp.broadcast_to(rain, (cx, cy)), 4 * line + 2 * l + outer, 1)
        own[l] = own[l] + jnp.where((lane == 0) | (lane == cy - 1), sent_in, 0.0)

    slots = jnp.concatenate(
        [col_in[d if len(ys) == 2 else 0, 5, d : d + 1, note : note + ky] for d in range(2)]
        + [
            corner_in[s, d if len(ys) == 2 else 0, 2 * s + d : 2 * s + d + 1, note : note + kc]
            for d in range(2) for s in range(2)
        ],
        1,
    ).astype(jnp.int32)
    face = lane_e < 2 * ky
    which = div(lane_e - 2 * ky, kc)
    minus_x = mod(which, 2)
    minus_y = jnp.where(face, jnp.where(lane_e < ky, 0, 1), div(which, 2))
    move_x = jnp.where(face, 0, 1 - 2 * minus_x)
    live = slots >= 0
    level = mod(div(slots, block), levels)
    place = jnp.where(face, mod(div(slots, cy), cx), jnp.where(minus_x == 0, cy // 4 - 1, cx))
    spot = jnp.broadcast_to(jnp.where(live, 4 * place + 2 * level + minus_y, 0), (sd, width))
    seat = iota((sd, width), 0) == jnp.where(live, div(slots, block * levels), -1)
    for n, value in enumerate((radius, weight_left, dry, east, north)):
        rec_out[n, :, pl.ds(2 * kx, width)] = jnp.sum(jnp.where(seat, take(value, spot, 1), 0.0), 0, keepdims=True)
    box_out[:, pl.ds(2 * kx, width)] = land(slots, move_x, 1 - 2 * minus_y)
    slots = side_records(0, still)
    box_out[:, pl.ds(0, kx)] = land(slots, 1, 0).reshape(1, kx)

    wait_rows(due[3], recv_sem.at[3])
    fallen = side_rows(0, side)
    for l in range(levels):
        total = own[l] + jnp.where(line == 0, fallen[l], 0.0)
        moist_out[l] = moist_out[l] - VAPOUR_PER_SOURCE * total
        warm_out[l] = warm_out[l] + WARMING_FACTOR * total
    side_records(0, moving)

    wait_rows(sent[0], send_sem.at[0])


def publish(*refs):
    count = len(refs) // 2
    sems = refs[-1]
    copies = [
        pltpu.make_async_copy(refs[n], refs[count + n], sems.at[n]) for n in range(count)
    ]
    for copy in copies:
        copy.start()
    for copy in copies:
        copy.wait()


def per_device(nx, ny, moist, warm, size, mult, dry, east, north, perm, lx, ly, lc):
    levels, cx, cy = moist.shape
    sd = size.shape[0]
    kx, ky, kc = lx.shape[2], ly.shape[2], lc.shape[2]
    narr = 2 * kx + 2 * ky + 4 * kc
    slots = sd * levels * cx
    flat = [x.reshape(slots, cy) for x in (size, mult, dry, east, north, perm)]
    f32, i32 = jnp.float32, jnp.int32
    any_space = pl.BlockSpec(memory_space=pl.ANY)
    vmem_space = pl.BlockSpec(memory_space=pltpu.VMEM)
    dma = pltpu.SemaphoreType.DMA
    shapes = (
        ((levels, cx, cy), f32),
        ((levels, cx, cy), f32),
        ((slots, cy), f32),
        ((slots, cy), f32),
        ((5, 1, narr), f32),
        ((1, narr), i32),
    )
    n_y = 1 if ny == 2 else 2
    outs = pl.pallas_call(
        functools.partial(body, (levels, cx, cy, sd, kx, ky, kc, nx, ny)),
        out_shape=tuple(pltpu.VMEM(*s) for s in shapes),
        in_specs=[any_space] * 17,
        out_specs=[vmem_space] * 6,
        scratch_shapes=[
            pltpu.VMEM((2, levels, cx, cy), f32),
            pltpu.VMEM((5, slots, cy), f32),
            pltpu.VMEM((slots, cy), i32),
            pltpu.VMEM((2, kx), i32),
            pltpu.VMEM((2, ky), i32),
            pltpu.VMEM((4, kc), i32),
            pltpu.VMEM((2, 2, levels, cx, cy), f32),
            pltpu.VMEM((n_y, 2, levels, cx, cy), f32),
            pltpu.VMEM((2, n_y, 2, levels, cx, cy), f32),
            pltpu.VMEM((2, 1, kx), i32),
            pltpu.VMEM((2, 1, kx), i32),
            pltpu.VMEM((2, 5, sd * levels, cy), f32),
            pltpu.VMEM((2, 5, sd * levels, cy), f32),
            pltpu.VMEM((2, sd * levels, cy), i32),
            pltpu.VMEM((2, sd * levels, cy), i32),
            pltpu.VMEM((2, sd, cy), f32),
            pltpu.VMEM((2, n_y, sd, cy), f32),
            pltpu.VMEM((6, sd, cy), f32),
            pltpu.VMEM((n_y, 6, sd, cy), f32),
            pltpu.VMEM((slots, cy), f32),
            pltpu.VMEM((10 * slots, cy), f32),
            pltpu.VMEM((9, slots, cy), f32),
            pltpu.VMEM((3, slots, cy), i32),
            pltpu.VMEM((levels, 9, cx, cy), f32),
            pltpu.VMEM((2, 2, sd * levels, cy), f32),
            dma((6,)), dma((1,)), dma((4,)),
        ],
        compiler_params=pltpu.CompilerParams(collective_id=0, has_side_effects=True),
    )(moist, warm, *flat, size, mult, dry, east, north, perm, lx, ly, lc)
    outs = pl.pallas_call(
        publish,
        out_shape=tuple(jax.ShapeDtypeStruct(*s) for s in shapes),
        in_specs=[vmem_space] * 6,
        out_specs=[any_space] * 6,
        scratch_shapes=[dma((6,))],
    )(*[pltpu.with_memory_space_constraint(x, pltpu.VMEM) for x in outs])
    return (
        outs[0], outs[1], outs[2].reshape(size.shape), outs[3].reshape(size.shape), outs[4], outs[5],
    )


def solution(mesh):
    cell, drop, lists = P(None, "gx", "gy"), P(None, None, "gx", "gy"), P("gx", None, "gy")
    return jax.shard_map(
        functools.partial(per_device, mesh.shape["gx"], mesh.shape["gy"]),
        mesh=mesh,
        in_specs=(cell,) * 2 + (drop,) * 6 + (lists,) * 3,
        out_specs=(cell, cell, drop, drop, cell, P("gx", "gy")),
        check_vma=False,
    )
```

```python
import functools
import math

import jax
import jax.numpy as jnp
from jax import lax
from jax.experimental import pallas as pl
from jax.experimental.pallas import tpu as pltpu
from jax.sharding import PartitionSpec as P

NEWTON = 4
MIX_HORIZONTAL = 0.2
MIX_VERTICAL = 0.05
EXCESS_FACTOR = 4.2222
CURVATURE = 0.0012
KAPPA_SOLUTE = 0.6
GROWTH_STEP = 200.0
COLLIDE_RATE = 4e-07
VAPOUR_PER_SOURCE = 0.001
WARMING_FACTOR = 0.00249
LOG2E = math.log2(math.e)

MESH = pl.DeviceIdType.MESH
SHIFTS = (-1, 0, 1)
SIDES = (1, -1)
MOVES = (1, -1)


def div(x, n):
    return lax.shift_right_arithmetic(x, jnp.int32(n.bit_length() - 1))


def mod(x, n):
    return lax.bitwise_and(x, jnp.int32(n - 1))


def iota(shape, dim):
    return lax.broadcasted_iota(jnp.int32, shape, dim)


def turn(x, shift, dim):
    shift %= x.shape[dim]
    return pltpu.roll(x, shift, dim) if shift else x


def take(x, index, dim):
    return jnp.take_along_axis(x, index, axis=dim)


def kernel_weights(offset):
    return {
        -1: jnp.maximum(0.5 - offset, 0.0),
        0: 1.0 - jnp.abs(offset - 0.5),
        1: jnp.maximum(offset - 0.5, 0.0),
    }


def prepare(radius, dry):
    inverse = 1.0 / radius
    square = inverse * inverse
    lowest = dry * dry
    strength = (1.5 * GROWTH_STEP * KAPPA_SOLUTE) * (lowest * dry)
    pull = strength * (square * inverse)
    area = radius * radius
    return (
        area - (GROWTH_STEP * CURVATURE) * inverse,
        (5.0 / 3.0) * pull,
        1.0 + pull * square,
        strength,
        lowest,
        area * radius,
    )


def settle(level, top, bottom, strength, lowest):
    above = jnp.maximum(level + top, lowest * bottom)
    flat = lax.rsqrt(above * bottom)
    for sweep in range(NEWTON - 1):
        inverse_root = bottom * flat
        square = inverse_root * inverse_root
        pull = strength * (square * inverse_root)
        bottom = 1.0 + pull * square
        above = jnp.maximum(level + (5.0 / 3.0) * pull, lowest * bottom)
        flat = lax.rsqrt(above * bottom)
    root = above * flat
    return root, (root * root) * root


def differences(near):
    centre = near[0, 0]
    terms = {(0, 0): centre}
    for s in SIDES:
        terms[s, 0] = near[s, 0] - centre
        terms[0, s] = near[0, s] - centre
    for a in SIDES:
        for b in SIDES:
            terms[a, b] = near[a, b] - near[a, 0] - terms[0, b]
    return terms


def interpolate(terms, east, north, reach_x, reach_y):
    right, up = east > 0.5, north > 0.5
    slope_x = jnp.where(right, terms[1, 0], terms[-1, 0])
    slope_y = jnp.where(up, terms[0, 1], terms[0, -1])
    twist = jnp.where(
        right, jnp.where(up, terms[1, 1], terms[1, -1]), jnp.where(up, terms[-1, 1], terms[-1, -1])
    )
    return terms[0, 0] + reach_x * slope_x + reach_y * (slope_y + reach_x * twist)


def match(weight, other, first):
    big = (weight > other) | ((weight == other) & first)
    rate = (-COLLIDE_RATE * LOG2E) * jnp.where(big, weight, other)
    return rate, jnp.where(big, other, 0.0)


def collide(radius, cube, other, rate, eaten):
    total = radius + other
    chance = 1.0 - jnp.exp2(rate * (total * total) * (total * jnp.abs(radius - other)))
    volume = cube + chance * (other * other * other)
    merged = jnp.exp2(jnp.log(volume) * (LOG2E / 3.0))
    return jnp.where(eaten > 0.0, radius, merged), chance * eaten


def spread(parts, dim, index):
    size = parts[0].shape[dim]
    back, ahead = turn(parts[-1], -1, dim), turn(parts[1], 1, dim)
    return parts[0] + jnp.where(index == size - 1, 0.0, back) + jnp.where(index == 0, 0.0, ahead)


def body(
    sizes,
    moist_in, warm_in, size_in, mult_in, dry_in, east_in, north_in, perm_in,
    size_cells, mult_cells, dry_cells, east_cells, north_cells, perm_cells,
    lx_in, ly_in, lc_in,
    moist_out, warm_out, size_out, mult_out, rec_out, box_out,
    state, drops, perm, ly, lc,
    state_x, state_y, diag_in, list_pack, list_x,
    row_pack, row_x, turn_pack, turn_x, corner_pack, corner_in, col_pack, col_in,
    mask, ready, share, bits, near, near_up, late_x, fall,
    in_sem, send_sem, recv_sem,
):
    levels, cx, cy, sd, kx, ky, kc, nx, ny = sizes
    me_x = lax.axis_index("gx")
    me_y = lax.axis_index("gy")
    ys = (1,) if ny == 2 else (1, -1)
    half = cx // 2
    rows = sd * levels
    slots_all = rows * cx
    block = cx * cy
    tall = levels * cx
    deep = kx // cy
    edges = (cx - 1, 0)
    bands = (pl.ds(cx - 3, 3), pl.ds(0, 3))

    def at(d):
        return (lax.rem(me_x + d[0] + nx, nx), lax.rem(me_y + d[1] + ny, ny))

    def wait_rows(count, sem):
        whole = ready.at[pl.ds(0, count), :]
        pltpu.make_async_copy(whole, whole, sem).wait()

    def count_rows(ref):
        total = 1
        for n in ref.shape:
            total *= n
        return total // cy

    brought = [0, 0, 0, 0]

    def bring(source, target, group):
        pltpu.make_async_copy(source, target, in_sem.at[group]).start()
        brought[group] += count_rows(target)

    bring(moist_in, state.at[0], 0)
    bring(warm_in, state.at[1], 0)
    cells = (size_cells, dry_cells, east_cells, north_cells, mult_cells)

    def bring_rows(s, chosen, group):
        for n in chosen:
            for l in range(levels):
                stretch = pl.ds(l * sd, sd)
                if n < 5:
                    bring(cells[n].at[:, l, edges[s], :], row_pack.at[s, n, stretch, :], group)
                else:
                    bring(perm_cells.at[:, l, edges[s], :], turn_pack.at[s, stretch, :], group)

    bring_rows(0, range(4), 1)

    friends = [(dx, 0) for dx in MOVES] + [(dx, dy) for dx in MOVES for dy in ys] + [(0, dy) for dy in ys]
    barrier = pltpu.get_barrier_semaphore()
    for d in friends:
        pl.semaphore_signal(barrier, inc=1, device_id=at(d), device_id_type=MESH)

    bring_rows(0, (4, 5), 2)
    for s in range(2):
        bring(lx_in.at[0, pl.ds(s, 1), :], list_pack.at[s], 2)
    bring_rows(1, range(6), 2)
    lists = [
        pltpu.make_async_copy(source.at[0], target, in_sem.at[4 + n])
        for n, (source, target) in enumerate(((ly_in, ly), (lc_in, lc)))
    ]
    for copy in lists:
        copy.start()
    for n, source in enumerate((size_in, mult_in, dry_in, east_in, north_in)):
        bring(source, drops.at[n], 3)
    bring(perm_in, perm, 3)

    sent = [0]
    due = [0] * 6

    def send(source, target, group, d):
        pltpu.make_async_remote_copy(
            src_ref=source, dst_ref=target, send_sem=send_sem.at[0], recv_sem=recv_sem.at[group],
            device_id=at(d), device_id_type=MESH,
        ).start()
        sent[0] += count_rows(source)
        due[group] += count_rows(source)

    line = iota((cx, cy), 0)
    lane = iota((cx, cy), 1)
    low_half = line < half

    def send_fields(s):
        own, far = state.at[:, :, bands[s], :], MOVES[s]
        group = (1, 0)[s]
        send(own, state_x.at[s, :, :, bands[s], :], group, (far, 0))
        for t, dy in enumerate(ys):
            send(own, diag_in.at[s, t, :, :, bands[s], :], group, (far, dy))

    def send_growth(s):
        send(row_pack.at[s, 0:4], row_x.at[s, 0:4], (4, 3)[s], (MOVES[s], 0))

    def send_rest(s):
        send(row_pack.at[s, 4], row_x.at[s, 4], (5, 3)[s], (MOVES[s], 0))
        send(turn_pack.at[s], turn_x.at[s], (5, 3)[s], (MOVES[s], 0))
        send(list_pack.at[s], list_x.at[s], (5, 3)[s], (MOVES[s], 0))

    def send_corner(s):
        tile = None
        for n in range(6):
            for l in range(levels):
                stretch = pl.ds(l * sd, sd)
                value = row_pack[s, n, stretch, :] if n < 5 else turn_pack[s, stretch, :].astype(jnp.float32)
                spot = 8 * n + 4 * s + 2 * l
                moved = turn(value, spot + 1, 1)
                tile = moved if tile is None else jnp.where(lane >= spot, moved, tile)
        corner_pack[s] = tile
        for d in range(2):
            spot = 2 * ky + kc * (2 * d + s)
            corner_pack[s, 2 * s + d : 2 * s + d + 1, spot : spot + kc] = lc[
                2 * s + d : 2 * s + d + 1, :
            ].astype(jnp.float32)
        for t, dy in enumerate(ys):
            send(corner_pack.at[s], corner_in.at[s, t], 2, (MOVES[s], dy))

    wait_rows(brought[0], in_sem.at[0])
    pl.semaphore_wait(barrier, len(friends))
    send_fields(0)
    wait_rows(brought[1], in_sem.at[1])
    send_growth(0)
    for t, dy in enumerate(ys):
        send(state, state_y.at[t], 0, (0, dy))
    wait_rows(brought[2], in_sem.at[2])
    send_rest(0)
    for copy in lists:
        copy.wait()
    send_fields(1)
    send_corner(0)
    send_growth(1)
    send_rest(1)
    send_corner(1)
    wait_rows(brought[3], in_sem.at[3])
    attributes = (0, 2, 3, 4, 1)
    for n in range(6):
        tile = None
        for i in range(cx):
            for l in range(levels):
                picked = pl.ds(l * cx + i, sd, stride=tall)
                value = drops[attributes[n], picked, :] if n < 5 else perm[picked, :].astype(jnp.float32)
                spot = 4 * i + 2 * l
                moved = turn(value, spot + 1, 1)
                tile = moved if tile is None else jnp.where(lane >= spot, moved, tile)
        col_pack[n] = tile
    for d in range(2):
        col_pack[6, d : d + 1, d * ky : (d + 1) * ky] = ly[d : d + 1, :].astype(jnp.float32)
    for t, dy in enumerate(ys):
        send(col_pack, col_in.at[t], 2, (0, dy))

    def span(n, k):
        return pl.ds(n * slots_all + k * tall, tall)

    order = [perm[k * tall : (k + 1) * tall, :] for k in range(sd)]
    for m in range(sd):
        part = pl.ds(m * tall, tall)
        weight = drops[1, part, :]
        partner = jnp.zeros((tall, cy), jnp.int32)
        first = jnp.zeros((tall, cy), jnp.int32)
        for p in range(sd):
            mine = order[p] == m
            partner = jnp.where(mine, order[p ^ 1], partner)
            if p % 2 == 0:
                first = jnp.where(mine, 1, first)
        other = drops[1, pl.ds(0, tall), :]
        for k in range(1, sd):
            other = jnp.where(partner == k, drops[1, pl.ds(k * tall, tall), :], other)
        rate, eaten = match(weight, other, first > 0)
        for n in range(3):
            bits[n, part, :] = mod(lax.shift_right_logical(partner, jnp.int32(n)), 2)
        for n, value in enumerate(prepare(drops[0, part, :], drops[2, part, :])):
            ready[span(n, m), :] = value
        east, north = drops[3, part, :], drops[4, part, :]
        ready[span(6, m), :] = jnp.abs(east - 0.5)
        ready[span(7, m), :] = jnp.abs(north - 0.5)
        ready[span(8, m), :] = rate
        ready[span(9, m), :] = eaten
        wx, wy = kernel_weights(east), kernel_weights(north)
        for a in SHIFTS:
            along = wx[a] * weight
            for b in SHIFTS:
                share[3 * a + b + 4, part, :] = wy[b] * along

    mask[...] = jnp.ones_like(mask)
    for r, side in enumerate(edges):
        slots = list_pack[r]
        hot_row = iota((rows, kx), 0) == div(slots, block)
        hot_lane = jnp.where(iota((cy, kx), 0) == mod(slots, cy), 1.0, 0.0).astype(jnp.bfloat16)
        named = lax.dot_general(
            jnp.where(hot_row, 1.0, 0.0).astype(jnp.bfloat16), hot_lane,
            (((1,), (1,)), ((), ())), preferred_element_type=jnp.float32,
        )
        mask[pl.ds(side, rows, stride=cx), :] = 1.0 - named

    width = 2 * ky + 4 * kc
    lane_e = iota((1, width), 1)
    high = (lane_e < ky) | ((lane_e >= 2 * ky) & (lane_e < 2 * ky + 2 * kc))
    high_all = jnp.broadcast_to(high, (slots_all, width))
    slots = jnp.concatenate(
        [ly[0:1, :], ly[1:2, :], lc[0:1, :], lc[2:3, :], lc[1:2, :], lc[3:4, :]], 1
    )
    hot_e = jnp.where(iota((slots_all, width), 0) == div(slots, cy), 1.0, 0.0)
    left_high = jnp.max(jnp.where(high_all, hot_e, 0.0), 1, keepdims=True)
    left_low = jnp.max(jnp.where(high_all, 0.0, hot_e), 1, keepdims=True)
    lane_all = iota((slots_all, cy), 1)
    mask[...] = mask[...] * (
        1.0 - jnp.where(lane_all == cy - 1, left_high, jnp.where(lane_all == 0, left_low, 0.0))
    )

    def land(slots, move_x, move_y):
        level = mod(div(slots, block), levels)
        i = mod(mod(div(slots, cy), cx) + move_x, cx)
        target = (level * cx + i) * cy + mod(mod(slots, cy) + move_y, cy)
        return jnp.where(slots >= 0, target, -1)

    def blend(parts, pick_second):
        return parts[0] if len(parts) == 1 else jnp.where(pick_second, parts[1], parts[0])

    left_lanes = lane < cy // 2
    odd_lane = mod(lane, 2) == 1
    group = div(lane, 4)
    keys = [(a, b) for a in SHIFTS for b in SHIFTS]

    def climate(fields):
        deep_lane = iota(fields[0][0][0].shape, 1)
        odd = mod(deep_lane, 2) == 1

        def fixed(value, spot):
            return take(value, jnp.full(value.shape, spot, jnp.int32), 1)

        def reach(own, other, s):
            if s == 0:
                return own
            inside = deep_lane < cy - s if s > 0 else deep_lane >= -s
            return jnp.where(inside, turn(own, -s, 1), turn(other, -s, 1))

        def brink(own, other, s):
            if s == 0:
                return take(other, jnp.where(odd, 0, cy - 1), 1)
            if s > 0:
                return jnp.where(odd, fixed(other, s), fixed(own, s - 1))
            return jnp.where(odd, fixed(own, cy + s), fixed(other, cy - 1 + s))

        def humidity(cut):
            raw = [[{s: cut(*fields[f][l], s) for s in range(-2, 3)} for l in range(levels)] for f in range(2)]
            mixed = []
            for f in range(2):
                mixed.append([])
                for l in range(levels):
                    at_shift = {}
                    for b in SHIFTS:
                        centre = raw[f][l][b]
                        around = raw[f][l][b - 1] + raw[f][l][b + 1] + (turn(centre, -1, 0) + turn(centre, 1, 0))
                        stacked = raw[f][min(l + 1, levels - 1)][b] + raw[f][max(l - 1, 0)][b]
                        at_shift[b] = (
                            (1.0 - 4.0 * MIX_HORIZONTAL - 2.0 * MIX_VERTICAL) * centre
                            + MIX_HORIZONTAL * around + MIX_VERTICAL * stacked
                        )
                    mixed[f].append(at_shift)
            humid = []
            for l in range(levels):
                humid.append({})
                for b in SHIFTS:
                    warmth = mixed[1][l][b]
                    decay = jnp.exp2((-17.27 * LOG2E) * (warmth - 273.15) / (warmth - 35.86))
                    humid[l][b] = (GROWTH_STEP / EXCESS_FACTOR) * (mixed[0][l][b] * decay) - GROWTH_STEP
            return mixed, humid

        mixed, humid = humidity(reach)
        terms = [differences({(a, b): turn(humid[l][b], -a, 0) for a, b in keys}) for l in range(levels)]
        _, column = humidity(brink)
        wide_level = mod(div(deep_lane, 2), 2) == 1
        column = {b: jnp.where(wide_level, column[1][b], column[0][b]) for b in SHIFTS}
        return mixed, terms, column

    def from_row(value, a):
        return take(value, mod(group + a, cx), 0)

    def mate(weight, turns):
        seat = iota((sd, cy), 0)
        rank = jnp.zeros((sd, cy), jnp.int32)
        for p in range(1, sd):
            rank = jnp.where(jnp.broadcast_to(turns[p : p + 1], (sd, cy)) == seat, p, rank)
        partner = take(turns, rank ^ 1, 0)
        return partner, match(weight, take(weight, partner, 0), mod(rank, 2) == 0)

    def expand(prepared, east, north, around):
        base, top, bottom, strength, lowest, cube = prepared
        level = base + interpolate(around, east, north, jnp.abs(east - 0.5), jnp.abs(north - 0.5))
        root, volume = settle(level, top, bottom, strength, lowest)
        return root, volume, volume - cube

    def merge(root, volume, weight, mated):
        partner, (rate, eaten) = mated
        after, lost = collide(root, volume, take(root, partner, 0), rate, eaten)
        return after, weight - lost

    def surround(ref, l, r):
        return {key: jnp.broadcast_to(ref[l, n, r : r + 1, :], (sd, cy)) for n, key in enumerate(keys)}

    def side_growth(s):
        ref, r = ((near, cx - 1), (near_up, 0))[s]
        found = []
        for l in range(levels):
            radius, dry, east, north = (row_x[s, n, pl.ds(l * sd, sd), :] for n in range(4))
            found.append(expand(prepare(radius, dry), east, north, surround(ref, l, r)))
        return found

    def side_rows(s, found):
        home = (0, cx - 1)[s]
        for l in range(levels):
            stretch = pl.ds(l * sd, sd)
            root, volume, gain = found[l]
            weight = row_x[s, 4, stretch, :]
            radius, weight_left = merge(root, volume, weight, mate(weight, turn_x[s, stretch, :]))
            late_x[s, 0, stretch, :] = radius
            late_x[s, 1, stretch, :] = weight_left
            wx, wy = kernel_weights(row_x[s, 2, stretch, :]), kernel_weights(row_x[s, 3, stretch, :])
            along = wx[MOVES[s]] * (weight * gain)
            for b in SHIFTS:
                fall[b + 1, l, home : home + 1, :] += jnp.sum(wy[b] * along, 0, keepdims=True)

    def side_records(s):
        slots = list_x[s].reshape(deep, cy)
        level = mod(div(slots, block), levels)
        row = jnp.where(slots >= 0, level * sd + div(slots, block * levels), -1)
        column = mod(slots, cy)
        fields = [(2, row_x, 1), (3, row_x, 2), (4, row_x, 3), (0, late_x, 0), (1, late_x, 1)]
        for n, source, from_n in fields:
            got = jnp.zeros((deep, cy), jnp.float32)
            for r in range(rows):
                value = jnp.broadcast_to(source[s, from_n, r : r + 1, :], (deep, cy))
                got = jnp.where(row == r, take(value, column, 1), got)
            rec_out[n, :, pl.ds(s * kx, kx)] = got.reshape(1, kx)
        box_out[:, pl.ds(s * kx, kx)] = land(slots, MOVES[s], 0).reshape(1, kx)

    wait_rows(due[0], recv_sem.at[0])
    fields = []
    for f in range(2):
        fields.append([])
        for l in range(levels):
            side_y = blend([state_y[t, f, l] for t in range(len(ys))], left_lanes)
            far = blend([diag_in[1, t, f, l] for t in range(len(ys))], left_lanes)
            fields[f].append(
                (jnp.concatenate([state[f, l], state_x[1, f, l]], 0), jnp.concatenate([side_y, far], 0))
            )
    mixed, terms, column = climate(fields)
    window = {key: jnp.concatenate([t[key][:cx] for t in terms], 0) for key in keys}
    for l in range(levels):
        for n, key in enumerate(keys):
            near_up[l, n] = terms[l][key][cx:]
        moist_out[l] = mixed[0][l][0][:cx]
        warm_out[l] = mixed[1][l][0][:cx]
    inside = {
        (a, b): jnp.where(
            mod(group + a, cy // 4) < cx, from_row(column[b][:cx], a), from_row(column[b][cx:], a)
        )
        for a, b in keys
    }

    grown = []
    cubes = []
    deposit = {}
    for k in range(sd):
        part = pl.ds(k * tall, tall)
        base, top, bottom, strength, lowest, cube, reach_x, reach_y = (ready[span(n, k), :] for n in range(8))
        level = base + interpolate(window, drops[3, part, :], drops[4, part, :], reach_x, reach_y)
        root, volume = settle(level, top, bottom, strength, lowest)
        gain = volume - cube
        for a, b in keys:
            term = share[3 * a + b + 4, part, :] * gain
            deposit[a, b] = term if k == 0 else deposit[a, b] + term
        grown.append(root)
        cubes.append(volume)

    for l in range(levels):
        for b in SHIFTS:
            parts = {a: jnp.where(line < 2, 0.0, deposit[a, b][l * cx : (l + 1) * cx]) for a in SHIFTS}
            fall[b + 1, l] = spread(parts, 0, line)

    for m in range(sd):
        part = pl.ds(m * tall, tall)
        found = grown
        for n in range(3):
            odd = bits[n, part, :] > 0
            found = [jnp.where(odd, found[2 * i + 1], found[2 * i]) for i in range(len(found) // 2)]
        radius, lost = collide(grown[m], cubes[m], found[0], ready[span(8, m), :], ready[span(9, m), :])
        size_out[part, :] = radius
        mult_out[part, :] = mask[part, :] * (drops[1, part, :] - lost)

    def upper_side():
        wait_rows(due[3], recv_sem.at[3])
        side_rows(1, side_growth(1))
        side_records(1)

    pl.when(me_x != nx - 1)(upper_side)

    redo = [(l, i) for l in range(levels) for i in range(2)]
    waiting = {}
    for l, i in redo:
        picked = pl.ds(l * cx + i, sd, stride=tall)
        radius, weight, dry, east, north = (drops[n, picked, :] for n in range(5))
        waiting[l, i] = (
            prepare(radius, dry), weight, east, north, mate(weight, perm[picked, :]), mask[picked, :]
        )

    wait_rows(due[1], recv_sem.at[1])
    fields = []
    for f in range(2):
        fields.append([])
        for l in range(levels):
            side_y = blend([state_y[t, f, l] for t in range(len(ys))], left_lanes)
            far = blend([diag_in[0, t, f, l] for t in range(len(ys))], left_lanes)
            fields[f].append(
                (jnp.where(low_half, state[f, l], state_x[0, f, l]), jnp.where(low_half, side_y, far))
            )
    mixed, terms, column = climate(fields)
    for l in range(levels):
        for n, key in enumerate(keys):
            near[l, n] = terms[l][key]
        moist_out[l, 0:1, :] = mixed[0][l][0][0:1]
        warm_out[l, 0:1, :] = mixed[1][l][0][0:1]
    col_terms = differences(
        {
            (a, b): jnp.where(mod(group + a + 2, cy // 4) < 4, from_row(column[b], a), inside[a, b])
            for a, b in keys
        }
    )
    for l in range(levels):
        landing = [None] * 3
        for i in range(2):
            picked = pl.ds(l * cx + i, sd, stride=tall)
            prepared, weight, east, north, mated, keep = waiting[l, i]
            root, volume, gain = expand(prepared, east, north, surround(near, l, i))
            radius, weight_left = merge(root, volume, weight, mated)
            size_out[picked, :] = radius
            mult_out[picked, :] = keep * weight_left
            wx, wy = kernel_weights(east), kernel_weights(north)
            for a in SHIFTS:
                if i + a < 0:
                    continue
                along = wx[a] * (weight * gain)
                parts = {b: wy[b] * along for b in SHIFTS}
                if landing[i + a] is not None:
                    parts = {b: parts[b] + landing[i + a][b] for b in SHIFTS}
                landing[i + a] = parts
        for r in range(3):
            for b in SHIFTS:
                fall[b + 1, l, r : r + 1, :] += jnp.sum(landing[r][b], 0, keepdims=True)

    wait_rows(due[2], recv_sem.at[2])
    corner = [blend([corner_in[s, t] for t in range(len(ys))], odd_lane) for s in range(2)]
    values = []
    for n in range(6):
        beside = blend([col_in[t, n] for t in range(len(ys))], odd_lane)
        below = jnp.where(lane < 4 * cx, beside, turn(corner[1], 4 * (cx - 1) - 8 * n, 1))
        values.append(jnp.where(lane >= cy - 4, turn(corner[0], cy - 4 - 8 * n, 1), below))
    radius, dry, east, north, weight, turns = values
    root, volume, gain = expand(prepare(radius, dry), east, north, col_terms)
    radius, weight_left = merge(root, volume, weight, mate(weight, turns.astype(jnp.int32)))
    wx, wy = kernel_weights(east), kernel_weights(north)
    across = jnp.where(odd_lane, wy[-1], wy[1]) * (weight * gain)
    rain = {a: jnp.broadcast_to(jnp.sum(wx[a] * across, 0, keepdims=True), (cx, cy)) for a in SHIFTS}
    outer = jnp.where(lane == cy - 1, 1, 0)
    edge_fall = []
    for l in range(levels):
        sent_in = sum(take(rain[a], mod(4 * (line - a) + 2 * l + outer, cy), 1) for a in SHIFTS)
        edge_fall.append(jnp.where((lane == 0) | (lane == cy - 1), sent_in, 0.0))

    which = div(lane_e - 2 * ky, kc)
    minus_x = mod(which, 2)
    face = lane_e < 2 * ky
    minus_y = jnp.where(face, jnp.where(lane_e < ky, 0, 1), div(which, 2))
    slots = None
    for d in range(2):
        t = d if len(ys) == 2 else 0
        faces = col_in[t, 6, d : d + 1, :]
        corners = [corner_in[s, t, 2 * s + d : 2 * s + d + 1, :] for s in range(2)]
        found = jnp.where(face, faces, jnp.where(minus_x == 0, corners[0], corners[1]))
        slots = found if d == 0 else jnp.where(minus_y == 0, slots, found)
    slots = slots.astype(jnp.int32)
    move_x = jnp.where(face, 0, 1 - 2 * minus_x)
    live = slots >= 0
    level = mod(div(slots, block), levels)
    place = jnp.where(face, mod(div(slots, cy), cx), jnp.where(minus_x == 0, cy // 4 - 1, cx))
    spot = jnp.broadcast_to(jnp.where(live, 4 * place + 2 * level + minus_y, 0), (sd, width))
    seat = iota((sd, width), 0) == jnp.where(live, div(slots, block * levels), -1)
    for n, value in enumerate((radius, weight_left, dry, east, north)):
        rec_out[n, :, pl.ds(2 * kx, width)] = jnp.sum(jnp.where(seat, take(value, spot, 1), 0.0), 0, keepdims=True)
    box_out[:, pl.ds(2 * kx, width)] = land(slots, move_x, 1 - 2 * minus_y)

    wait_rows(due[4], recv_sem.at[4])
    side = side_growth(0)
    wait_rows(due[5], recv_sem.at[5])
    side_rows(0, side)
    side_records(0)

    pl.when(me_x == nx - 1)(upper_side)

    for l in range(levels):
        total = spread({b: fall[b + 1, l] for b in SHIFTS}, 1, lane) + edge_fall[l]
        moist_out[l] = moist_out[l] - VAPOUR_PER_SOURCE * total
        warm_out[l] = warm_out[l] + WARMING_FACTOR * total

    wait_rows(sent[0], send_sem.at[0])


def publish(*refs):
    count = len(refs) // 2
    sems = refs[-1]
    copies = [
        pltpu.make_async_copy(refs[n], refs[count + n], sems.at[n]) for n in range(count)
    ]
    for copy in copies:
        copy.start()
    for copy in copies:
        copy.wait()


def per_device(nx, ny, moist, warm, size, mult, dry, east, north, perm, lx, ly, lc):
    levels, cx, cy = moist.shape
    sd = size.shape[0]
    kx, ky, kc = lx.shape[2], ly.shape[2], lc.shape[2]
    narr = 2 * kx + 2 * ky + 4 * kc
    slots = sd * levels * cx
    flat = [x.reshape(slots, cy) for x in (size, mult, dry, east, north, perm)]
    f32, i32 = jnp.float32, jnp.int32
    any_space = pl.BlockSpec(memory_space=pl.ANY)
    vmem_space = pl.BlockSpec(memory_space=pltpu.VMEM)
    dma = pltpu.SemaphoreType.DMA
    shapes = (
        ((levels, cx, cy), f32),
        ((levels, cx, cy), f32),
        ((slots, cy), f32),
        ((slots, cy), f32),
        ((5, 1, narr), f32),
        ((1, narr), i32),
    )
    n_y = 1 if ny == 2 else 2
    outs = pl.pallas_call(
        functools.partial(body, (levels, cx, cy, sd, kx, ky, kc, nx, ny)),
        out_shape=tuple(pltpu.VMEM(*s) for s in shapes),
        in_specs=[any_space] * 17,
        out_specs=[vmem_space] * 6,
        scratch_shapes=[
            pltpu.VMEM((2, levels, cx, cy), f32),
            pltpu.VMEM((5, slots, cy), f32),
            pltpu.VMEM((slots, cy), i32),
            pltpu.VMEM((2, ky), i32),
            pltpu.VMEM((4, kc), i32),
            pltpu.VMEM((2, 2, levels, cx, cy), f32),
            pltpu.VMEM((n_y, 2, levels, cx, cy), f32),
            pltpu.VMEM((2, n_y, 2, levels, cx, cy), f32),
            pltpu.VMEM((2, 1, kx), i32),
            pltpu.VMEM((2, 1, kx), i32),
            pltpu.VMEM((2, 5, sd * levels, cy), f32),
            pltpu.VMEM((2, 5, sd * levels, cy), f32),
            pltpu.VMEM((2, sd * levels, cy), i32),
            pltpu.VMEM((2, sd * levels, cy), i32),
            pltpu.VMEM((2, sd, cy), f32),
            pltpu.VMEM((2, n_y, sd, cy), f32),
            pltpu.VMEM((7, sd, cy), f32),
            pltpu.VMEM((n_y, 7, sd, cy), f32),
            pltpu.VMEM((slots, cy), f32),
            pltpu.VMEM((10 * slots, cy), f32),
            pltpu.VMEM((9, slots, cy), f32),
            pltpu.VMEM((3, slots, cy), i32),
            pltpu.VMEM((levels, 9, cx, cy), f32),
            pltpu.VMEM((levels, 9, cx, cy), f32),
            pltpu.VMEM((2, 2, sd * levels, cy), f32),
            pltpu.VMEM((3, levels, cx, cy), f32),
            dma((6,)), dma((1,)), dma((6,)),
        ],
        compiler_params=pltpu.CompilerParams(collective_id=0, has_side_effects=True),
    )(moist, warm, *flat, size, mult, dry, east, north, perm, lx, ly, lc)
    outs = pl.pallas_call(
        publish,
        out_shape=tuple(jax.ShapeDtypeStruct(*s) for s in shapes),
        in_specs=[vmem_space] * 6,
        out_specs=[any_space] * 6,
        scratch_shapes=[dma((6,))],
    )(*[pltpu.with_memory_space_constraint(x, pltpu.VMEM) for x in outs])
    return (
        outs[0], outs[1], outs[2].reshape(size.shape), outs[3].reshape(size.shape), outs[4], outs[5],
    )


def solution(mesh):
    cell, drop, lists = P(None, "gx", "gy"), P(None, None, "gx", "gy"), P("gx", None, "gy")
    return jax.shard_map(
        functools.partial(per_device, mesh.shape["gx"], mesh.shape["gy"]),
        mesh=mesh,
        in_specs=(cell,) * 2 + (drop,) * 6 + (lists,) * 3,
        out_specs=(cell, cell, drop, drop, cell, P("gx", "gy")),
        check_vma=False,
    )
```

```python
import functools
import math

import jax
import jax.numpy as jnp
from jax import lax
from jax.experimental import pallas as pl
from jax.experimental.pallas import tpu as pltpu
from jax.sharding import PartitionSpec as P

NEWTON = 4
MIX_HORIZONTAL = 0.2
MIX_VERTICAL = 0.05
EXCESS_FACTOR = 4.2222
CURVATURE = 0.0012
KAPPA_SOLUTE = 0.6
GROWTH_STEP = 200.0
COLLIDE_RATE = 4e-07
VAPOUR_PER_SOURCE = 0.001
WARMING_FACTOR = 0.00249
LOG2E = math.log2(math.e)

MESH = pl.DeviceIdType.MESH
SHIFTS = (-1, 0, 1)
SIDES = (1, -1)
MOVES = (1, -1)


def div(x, n):
    return lax.shift_right_arithmetic(x, jnp.int32(n.bit_length() - 1))


def mod(x, n):
    return lax.bitwise_and(x, jnp.int32(n - 1))


def iota(shape, dim):
    return lax.broadcasted_iota(jnp.int32, shape, dim)


def turn(x, shift, dim):
    shift %= x.shape[dim]
    return pltpu.roll(x, shift, dim) if shift else x


def take(x, index, dim):
    return jnp.take_along_axis(x, index, axis=dim)


def kernel_weights(offset):
    return {
        -1: jnp.maximum(0.5 - offset, 0.0),
        0: 1.0 - jnp.abs(offset - 0.5),
        1: jnp.maximum(offset - 0.5, 0.0),
    }


def prepare(radius, dry):
    inverse = 1.0 / radius
    square = inverse * inverse
    lowest = dry * dry
    strength = (1.5 * GROWTH_STEP * KAPPA_SOLUTE) * (lowest * dry)
    pull = strength * (square * inverse)
    area = radius * radius
    return (
        area - (GROWTH_STEP * CURVATURE) * inverse,
        (5.0 / 3.0) * pull,
        1.0 + pull * square,
        strength,
        lowest,
        area * radius,
    )


def settle(level, top, bottom, strength, lowest):
    above = jnp.maximum(level + top, lowest * bottom)
    flat = lax.rsqrt(above * bottom)
    for sweep in range(NEWTON - 1):
        inverse_root = bottom * flat
        square = inverse_root * inverse_root
        pull = strength * (square * inverse_root)
        bottom = 1.0 + pull * square
        above = jnp.maximum(level + (5.0 / 3.0) * pull, lowest * bottom)
        flat = lax.rsqrt(above * bottom)
    root = above * flat
    return root, (root * root) * root


def differences(near):
    centre = near[0, 0]
    terms = {(0, 0): centre}
    for s in SIDES:
        terms[s, 0] = near[s, 0] - centre
        terms[0, s] = near[0, s] - centre
    for a in SIDES:
        for b in SIDES:
            terms[a, b] = near[a, b] - near[a, 0] - terms[0, b]
    return terms


def interpolate(terms, east, north, reach_x, reach_y):
    right, up = east > 0.5, north > 0.5
    slope_x = jnp.where(right, terms[1, 0], terms[-1, 0])
    slope_y = jnp.where(up, terms[0, 1], terms[0, -1])
    twist = jnp.where(
        right, jnp.where(up, terms[1, 1], terms[1, -1]), jnp.where(up, terms[-1, 1], terms[-1, -1])
    )
    return terms[0, 0] + reach_x * slope_x + reach_y * (slope_y + reach_x * twist)


def match(weight, other, first):
    big = (weight > other) | ((weight == other) & first)
    rate = (-COLLIDE_RATE * LOG2E) * jnp.where(big, weight, other)
    return rate, jnp.where(big, other, 0.0)


def collide(radius, cube, other, rate, eaten):
    total = radius + other
    chance = 1.0 - jnp.exp2(rate * (total * total) * (total * jnp.abs(radius - other)))
    volume = cube + chance * (other * other * other)
    merged = jnp.exp2(jnp.log(volume) * (LOG2E / 3.0))
    return jnp.where(eaten > 0.0, radius, merged), chance * eaten


def spread(parts, dim, index):
    size = parts[0].shape[dim]
    back, ahead = turn(parts[-1], -1, dim), turn(parts[1], 1, dim)
    return parts[0] + jnp.where(index == size - 1, 0.0, back) + jnp.where(index == 0, 0.0, ahead)


def body(
    sizes,
    moist_in, warm_in, size_in, mult_in, dry_in, east_in, north_in, perm_in,
    size_cells, mult_cells, dry_cells, east_cells, north_cells, perm_cells,
    lx_in, ly_in, lc_in,
    moist_out, warm_out, size_out, mult_out, rec_out, box_out,
    state, drops, perm, ly, lc,
    state_x, state_y, diag_in, list_pack, list_sort, list_x,
    row_pack, row_sort, row_x, turn_pack, rank_of, corner_pack, corner_in, col_pack, col_in,
    mask, ready, share, bits, near, near_up, late_x, fall,
    in_sem, send_sem, recv_sem, lower_in,
):
    levels, cx, cy, sd, kx, ky, kc, nx, ny = sizes
    me_x = lax.axis_index("gx")
    me_y = lax.axis_index("gy")
    ys = (1,) if ny == 2 else (1, -1)
    half = cx // 2
    rows = sd * levels
    slots_all = rows * cx
    block = cx * cy
    tall = levels * cx
    deep = kx // cy
    edges = (cx - 1, 0)
    bands = (pl.ds(cx - 3, 3), pl.ds(0, 3))

    def at(d):
        return (lax.rem(me_x + d[0] + nx, nx), lax.rem(me_y + d[1] + ny, ny))

    def wait_rows(count, sem):
        whole = ready.at[pl.ds(0, count), :]
        pltpu.make_async_copy(whole, whole, sem).wait()

    def count_rows(ref):
        total = 1
        for n in ref.shape:
            total *= n
        return total // cy

    brought = [0, 0, 0, 0]

    def bring(source, target, group):
        pltpu.make_async_copy(source, target, in_sem.at[group]).start()
        brought[group] += count_rows(target)

    cells = (size_cells, dry_cells, east_cells, north_cells, mult_cells)

    def bring_rows(s, chosen, group):
        for n in chosen:
            for l in range(levels):
                stretch = pl.ds(l * sd, sd)
                if n < 5:
                    bring(cells[n].at[:, l, edges[s], :], row_pack.at[s, n, stretch, :], group)
                else:
                    bring(perm_cells.at[:, l, edges[s], :], turn_pack.at[s, stretch, :], group)

    bring_rows(0, (5, 0, 1, 2, 3, 4), 1)
    bring(lx_in.at[0, pl.ds(0, 1), :], list_pack.at[0], 1)
    bring(moist_in, state.at[0], 0)
    bring(warm_in, state.at[1], 0)

    beside = [0] + list(ys)
    barrier = pltpu.get_barrier_semaphore()
    for d in [(-1, dy) for dy in beside] + [(0, dy) for dy in ys]:
        pl.semaphore_signal(barrier, inc=1, device_id=at(d), device_id_type=MESH)

    bring_rows(1, range(6), 2)
    bring(lx_in.at[0, pl.ds(1, 1), :], list_pack.at[1], 2)
    lists = [
        pltpu.make_async_copy(source.at[0], target, in_sem.at[4 + n])
        for n, (source, target) in enumerate(((ly_in, ly), (lc_in, lc)))
    ]
    for copy in lists:
        copy.start()
    for n, source in enumerate((size_in, mult_in, dry_in, east_in, north_in)):
        bring(source, drops.at[n], 3)
    bring(perm_in, perm, 3)

    sent = [0]
    due = [0] * 7

    def send(source, target, group, d):
        pltpu.make_async_remote_copy(
            src_ref=source, dst_ref=target, send_sem=send_sem.at[0], recv_sem=recv_sem.at[group],
            device_id=at(d), device_id_type=MESH,
        ).start()
        sent[0] += count_rows(source)
        due[group] += count_rows(source)

    line = iota((cx, cy), 0)
    lane = iota((cx, cy), 1)
    low_half = line < half

    def send_fields(s):
        own, far = state.at[:, :, bands[s], :], MOVES[s]
        group = (1, 0)[s]
        send(own, state_x.at[s, :, :, bands[s], :], group, (far, 0))
        for t, dy in enumerate(ys):
            send(own, diag_in.at[s, t, :, :, bands[s], :], group, (far, dy))

    seat = iota((sd, cy), 0)

    def send_rows(s):
        for l in range(levels):
            stretch = pl.ds(l * sd, sd)
            turns = turn_pack[s, stretch, :]
            for n in range(5):
                row_sort[s, n, stretch, :] = take(row_pack[s, n, stretch, :], turns, 0)
        send(row_sort.at[s, 0:4], row_x.at[s, 0:4], (4, 3)[s], (MOVES[s], 0))
        send(row_sort.at[s, 4], row_x.at[s, 4], (5, 3)[s], (MOVES[s], 0))
        for l in range(levels):
            rank = jnp.zeros((sd, cy), jnp.int32)
            for p in range(1, sd):
                here = jnp.broadcast_to(turn_pack[s, l * sd + p : l * sd + p + 1, :], (sd, cy)) == seat
                rank = jnp.where(here, p, rank)
            rank_of[s, pl.ds(l * sd, sd), :] = rank
        slots = list_pack[s].reshape(deep, cy)
        k = div(slots, block * levels)
        row = mod(div(slots, block), levels) * sd + k
        place = jnp.zeros((deep, cy), jnp.int32)
        for r in range(rows):
            value = take(jnp.broadcast_to(rank_of[s, r : r + 1, :], (deep, cy)), mod(slots, cy), 1)
            place = jnp.where(row == r, value, place)
        moved = jnp.where(slots >= 0, slots + (place - k) * (block * levels), -1)
        list_sort[s] = moved.reshape(1, kx)
        send(list_sort.at[s], list_x.at[s], (6, 3)[s], (MOVES[s], 0))

    def send_corner(s):
        tile = None
        for n in range(6):
            for l in range(levels):
                stretch = pl.ds(l * sd, sd)
                value = row_pack[s, n, stretch, :] if n < 5 else turn_pack[s, stretch, :].astype(jnp.float32)
                spot = 8 * n + 4 * s + 2 * l
                moved = turn(value, spot + 1, 1)
                tile = moved if tile is None else jnp.where(lane >= spot, moved, tile)
        corner_pack[s] = tile
        for d in range(2):
            spot = 2 * ky + kc * (2 * d + s)
            corner_pack[s, 2 * s + d : 2 * s + d + 1, spot : spot + kc] = lc[
                2 * s + d : 2 * s + d + 1, :
            ].astype(jnp.float32)
        for t, dy in enumerate(ys):
            send(corner_pack.at[s], corner_in.at[s, t], 2, (MOVES[s], dy))

    pl.semaphore_wait(barrier, len(beside) + len(ys))
    for dy in beside:
        for f, source in enumerate((moist_in, warm_in)):
            target = state_x.at[0] if dy == 0 else diag_in.at[0, ys.index(dy)]
            send(source.at[:, bands[0], :], target.at[f, :, bands[0], :], 1, (1, dy))
    for dy in beside:
        pl.semaphore_signal(lower_in, inc=1, device_id=at((1, dy)), device_id_type=MESH)
    wait_rows(brought[1], in_sem.at[1])
    send_rows(0)
    for copy in lists:
        copy.wait()
    send_corner(0)
    wait_rows(brought[0], in_sem.at[0])
    for t, dy in enumerate(ys):
        send(state, state_y.at[t], 0, (0, dy))
    wait_rows(brought[2], in_sem.at[2])
    wait_rows(brought[3], in_sem.at[3])
    attributes = (0, 2, 3, 4, 1)
    for n in range(6):
        tile = None
        for i in range(cx):
            for l in range(levels):
                picked = pl.ds(l * cx + i, sd, stride=tall)
                value = drops[attributes[n], picked, :] if n < 5 else perm[picked, :].astype(jnp.float32)
                spot = 4 * i + 2 * l
                moved = turn(value, spot + 1, 1)
                tile = moved if tile is None else jnp.where(lane >= spot, moved, tile)
        col_pack[n] = tile
    for d in range(2):
        col_pack[6, d : d + 1, d * ky : (d + 1) * ky] = ly[d : d + 1, :].astype(jnp.float32)
    for t, dy in enumerate(ys):
        send(col_pack, col_in.at[t], 2, (0, dy))

    def span(n, k):
        return pl.ds(n * slots_all + k * tall, tall)

    order = [perm[k * tall : (k + 1) * tall, :] for k in range(sd)]
    for m in range(sd):
        part = pl.ds(m * tall, tall)
        weight = drops[1, part, :]
        partner = jnp.zeros((tall, cy), jnp.int32)
        first = jnp.zeros((tall, cy), jnp.int32)
        for p in range(sd):
            mine = order[p] == m
            partner = jnp.where(mine, order[p ^ 1], partner)
            if p % 2 == 0:
                first = jnp.where(mine, 1, first)
        other = drops[1, pl.ds(0, tall), :]
        for k in range(1, sd):
            other = jnp.where(partner == k, drops[1, pl.ds(k * tall, tall), :], other)
        rate, eaten = match(weight, other, first > 0)
        for n in range(3):
            bits[n, part, :] = mod(lax.shift_right_logical(partner, jnp.int32(n)), 2)
        for n, value in enumerate(prepare(drops[0, part, :], drops[2, part, :])):
            ready[span(n, m), :] = value
        east, north = drops[3, part, :], drops[4, part, :]
        ready[span(6, m), :] = jnp.abs(east - 0.5)
        ready[span(7, m), :] = jnp.abs(north - 0.5)
        ready[span(8, m), :] = rate
        ready[span(9, m), :] = eaten
        wx, wy = kernel_weights(east), kernel_weights(north)
        for a in SHIFTS:
            along = wx[a] * weight
            for b in SHIFTS:
                share[3 * a + b + 4, part, :] = wy[b] * along

    mask[...] = jnp.ones_like(mask)
    for r, side in enumerate(edges):
        slots = list_pack[r]
        hot_row = iota((rows, kx), 0) == div(slots, block)
        hot_lane = jnp.where(iota((cy, kx), 0) == mod(slots, cy), 1.0, 0.0).astype(jnp.bfloat16)
        named = lax.dot_general(
            jnp.where(hot_row, 1.0, 0.0).astype(jnp.bfloat16), hot_lane,
            (((1,), (1,)), ((), ())), preferred_element_type=jnp.float32,
        )
        mask[pl.ds(side, rows, stride=cx), :] = 1.0 - named

    width = 2 * ky + 4 * kc
    lane_e = iota((1, width), 1)
    high = (lane_e < ky) | ((lane_e >= 2 * ky) & (lane_e < 2 * ky + 2 * kc))
    high_all = jnp.broadcast_to(high, (slots_all, width))
    slots = jnp.concatenate(
        [ly[0:1, :], ly[1:2, :], lc[0:1, :], lc[2:3, :], lc[1:2, :], lc[3:4, :]], 1
    )
    hot_e = jnp.where(iota((slots_all, width), 0) == div(slots, cy), 1.0, 0.0)
    left_high = jnp.max(jnp.where(high_all, hot_e, 0.0), 1, keepdims=True)
    left_low = jnp.max(jnp.where(high_all, 0.0, hot_e), 1, keepdims=True)
    lane_all = iota((slots_all, cy), 1)
    mask[...] = mask[...] * (
        1.0 - jnp.where(lane_all == cy - 1, left_high, jnp.where(lane_all == 0, left_low, 0.0))
    )

    def land(slots, move_x, move_y):
        level = mod(div(slots, block), levels)
        i = mod(mod(div(slots, cy), cx) + move_x, cx)
        target = (level * cx + i) * cy + mod(mod(slots, cy) + move_y, cy)
        return jnp.where(slots >= 0, target, -1)

    def blend(parts, pick_second):
        return parts[0] if len(parts) == 1 else jnp.where(pick_second, parts[1], parts[0])

    left_lanes = lane < cy // 2
    odd_lane = mod(lane, 2) == 1
    group = div(lane, 4)
    keys = [(a, b) for a in SHIFTS for b in SHIFTS]

    def climate(fields):
        deep_lane = iota(fields[0][0][0].shape, 1)
        odd = mod(deep_lane, 2) == 1

        def fixed(value, spot):
            return take(value, jnp.full(value.shape, spot, jnp.int32), 1)

        def reach(own, other, s):
            if s == 0:
                return own
            inside = deep_lane < cy - s if s > 0 else deep_lane >= -s
            return jnp.where(inside, turn(own, -s, 1), turn(other, -s, 1))

        def brink(own, other, s):
            if s == 0:
                return take(other, jnp.where(odd, 0, cy - 1), 1)
            if s > 0:
                return jnp.where(odd, fixed(other, s), fixed(own, s - 1))
            return jnp.where(odd, fixed(own, cy + s), fixed(other, cy - 1 + s))

        def humidity(cut):
            raw = [[{s: cut(*fields[f][l], s) for s in range(-2, 3)} for l in range(levels)] for f in range(2)]
            mixed = []
            for f in range(2):
                mixed.append([])
                for l in range(levels):
                    at_shift = {}
                    for b in SHIFTS:
                        centre = raw[f][l][b]
                        around = raw[f][l][b - 1] + raw[f][l][b + 1] + (turn(centre, -1, 0) + turn(centre, 1, 0))
                        stacked = raw[f][min(l + 1, levels - 1)][b] + raw[f][max(l - 1, 0)][b]
                        at_shift[b] = (
                            (1.0 - 4.0 * MIX_HORIZONTAL - 2.0 * MIX_VERTICAL) * centre
                            + MIX_HORIZONTAL * around + MIX_VERTICAL * stacked
                        )
                    mixed[f].append(at_shift)
            humid = []
            for l in range(levels):
                humid.append({})
                for b in SHIFTS:
                    warmth = mixed[1][l][b]
                    decay = jnp.exp2((-17.27 * LOG2E) * (warmth - 273.15) / (warmth - 35.86))
                    humid[l][b] = (GROWTH_STEP / EXCESS_FACTOR) * (mixed[0][l][b] * decay) - GROWTH_STEP
            return mixed, humid

        mixed, humid = humidity(reach)
        terms = [differences({(a, b): turn(humid[l][b], -a, 0) for a, b in keys}) for l in range(levels)]
        _, column = humidity(brink)
        wide_level = mod(div(deep_lane, 2), 2) == 1
        column = {b: jnp.where(wide_level, column[1][b], column[0][b]) for b in SHIFTS}
        return mixed, terms, column

    def from_row(value, a):
        return take(value, mod(group + a, cx), 0)

    def mate(weight, turns):
        rank = jnp.zeros((sd, cy), jnp.int32)
        for p in range(1, sd):
            rank = jnp.where(jnp.broadcast_to(turns[p : p + 1], (sd, cy)) == seat, p, rank)
        partner = take(turns, rank ^ 1, 0)
        return partner, match(weight, take(weight, partner, 0), mod(rank, 2) == 0)

    def expand(prepared, east, north, around):
        base, top, bottom, strength, lowest, cube = prepared
        level = base + interpolate(around, east, north, jnp.abs(east - 0.5), jnp.abs(north - 0.5))
        root, volume = settle(level, top, bottom, strength, lowest)
        return root, volume, volume - cube

    across_pair = seat ^ 1

    def pair(weight):
        return across_pair, match(weight, take(weight, across_pair, 0), mod(seat, 2) == 0)

    def merge(root, volume, weight, mated):
        partner, (rate, eaten) = mated
        after, lost = collide(root, volume, take(root, partner, 0), rate, eaten)
        return after, weight - lost

    def surround(ref, l, r):
        return {key: jnp.broadcast_to(ref[l, n, r : r + 1, :], (sd, cy)) for n, key in enumerate(keys)}

    def side_growth(s):
        ref, r = ((near, cx - 1), (near_up, 0))[s]
        found = []
        for l in range(levels):
            radius, dry, east, north = (row_x[s, n, pl.ds(l * sd, sd), :] for n in range(4))
            found.append(expand(prepare(radius, dry), east, north, surround(ref, l, r)))
        return found

    def side_rows(s, found):
        home = (0, cx - 1)[s]
        for l in range(levels):
            stretch = pl.ds(l * sd, sd)
            root, volume, gain = found[l]
            weight = row_x[s, 4, stretch, :]
            radius, weight_left = merge(root, volume, weight, pair(weight))
            late_x[s, 0, stretch, :] = radius
            late_x[s, 1, stretch, :] = weight_left
            wx, wy = kernel_weights(row_x[s, 2, stretch, :]), kernel_weights(row_x[s, 3, stretch, :])
            along = wx[MOVES[s]] * (weight * gain)
            for b in SHIFTS:
                fall[b + 1, l, home : home + 1, :] += jnp.sum(wy[b] * along, 0, keepdims=True)

    def side_records(s):
        slots = list_x[s].reshape(deep, cy)
        level = mod(div(slots, block), levels)
        row = jnp.where(slots >= 0, level * sd + div(slots, block * levels), -1)
        column = mod(slots, cy)
        fields = [(2, row_x, 1), (3, row_x, 2), (4, row_x, 3), (0, late_x, 0), (1, late_x, 1)]
        for n, source, from_n in fields:
            got = jnp.zeros((deep, cy), jnp.float32)
            for r in range(rows):
                value = jnp.broadcast_to(source[s, from_n, r : r + 1, :], (deep, cy))
                got = jnp.where(row == r, take(value, column, 1), got)
            rec_out[n, :, pl.ds(s * kx, kx)] = got.reshape(1, kx)
        box_out[:, pl.ds(s * kx, kx)] = land(slots, MOVES[s], 0).reshape(1, kx)

    pl.semaphore_wait(lower_in, len(beside))
    send_fields(1)
    send_rows(1)
    send_corner(1)

    wait_rows(due[0], recv_sem.at[0])
    fields = []
    for f in range(2):
        fields.append([])
        for l in range(levels):
            side_y = blend([state_y[t, f, l] for t in range(len(ys))], left_lanes)
            far = blend([diag_in[1, t, f, l] for t in range(len(ys))], left_lanes)
            fields[f].append(
                (jnp.concatenate([state[f, l], state_x[1, f, l]], 0), jnp.concatenate([side_y, far], 0))
            )
    mixed, terms, column = climate(fields)
    window = {key: jnp.concatenate([t[key][:cx] for t in terms], 0) for key in keys}
    for l in range(levels):
        for n, key in enumerate(keys):
            near_up[l, n] = terms[l][key][cx:]
        moist_out[l] = mixed[0][l][0][:cx]
        warm_out[l] = mixed[1][l][0][:cx]
    inside = {
        (a, b): jnp.where(
            mod(group + a, cy // 4) < cx, from_row(column[b][:cx], a), from_row(column[b][cx:], a)
        )
        for a, b in keys
    }

    grown = []
    cubes = []
    deposit = {}
    for k in range(sd):
        part = pl.ds(k * tall, tall)
        base, top, bottom, strength, lowest, cube, reach_x, reach_y = (ready[span(n, k), :] for n in range(8))
        level = base + interpolate(window, drops[3, part, :], drops[4, part, :], reach_x, reach_y)
        root, volume = settle(level, top, bottom, strength, lowest)
        gain = volume - cube
        for a, b in keys:
            term = share[3 * a + b + 4, part, :] * gain
            deposit[a, b] = term if k == 0 else deposit[a, b] + term
        grown.append(root)
        cubes.append(volume)

    for l in range(levels):
        for b in SHIFTS:
            parts = {a: jnp.where(line < 2, 0.0, deposit[a, b][l * cx : (l + 1) * cx]) for a in SHIFTS}
            fall[b + 1, l] = spread(parts, 0, line)

    for m in range(sd):
        part = pl.ds(m * tall, tall)
        found = grown
        for n in range(3):
            odd = bits[n, part, :] > 0
            found = [jnp.where(odd, found[2 * i + 1], found[2 * i]) for i in range(len(found) // 2)]
        radius, lost = collide(grown[m], cubes[m], found[0], ready[span(8, m), :], ready[span(9, m), :])
        size_out[part, :] = radius
        mult_out[part, :] = mask[part, :] * (drops[1, part, :] - lost)

    def upper_side():
        wait_rows(due[3], recv_sem.at[3])
        side_rows(1, side_growth(1))
        side_records(1)

    pl.when(me_x != nx - 1)(upper_side)

    redo = [(l, i) for l in range(levels) for i in range(2)]
    waiting = {}
    for l, i in redo:
        picked = pl.ds(l * cx + i, sd, stride=tall)
        radius, weight, dry, east, north = (drops[n, picked, :] for n in range(5))
        waiting[l, i] = (
            prepare(radius, dry), weight, east, north, mate(weight, perm[picked, :]), mask[picked, :]
        )

    wait_rows(due[1], recv_sem.at[1])
    fields = []
    for f in range(2):
        fields.append([])
        for l in range(levels):
            side_y = blend([state_y[t, f, l] for t in range(len(ys))], left_lanes)
            far = blend([diag_in[0, t, f, l] for t in range(len(ys))], left_lanes)
            fields[f].append(
                (jnp.where(low_half, state[f, l], state_x[0, f, l]), jnp.where(low_half, side_y, far))
            )
    mixed, terms, column = climate(fields)
    for l in range(levels):
        for n, key in enumerate(keys):
            near[l, n] = terms[l][key]
        moist_out[l, 0:1, :] = mixed[0][l][0][0:1]
        warm_out[l, 0:1, :] = mixed[1][l][0][0:1]
    col_terms = differences(
        {
            (a, b): jnp.where(mod(group + a + 2, cy // 4) < 4, from_row(column[b], a), inside[a, b])
            for a, b in keys
        }
    )
    for l in range(levels):
        landing = [None] * 3
        for i in range(2):
            picked = pl.ds(l * cx + i, sd, stride=tall)
            prepared, weight, east, north, mated, keep = waiting[l, i]
            root, volume, gain = expand(prepared, east, north, surround(near, l, i))
            radius, weight_left = merge(root, volume, weight, mated)
            size_out[picked, :] = radius
            mult_out[picked, :] = keep * weight_left
            wx, wy = kernel_weights(east), kernel_weights(north)
            for a in SHIFTS:
                if i + a < 0:
                    continue
                along = wx[a] * (weight * gain)
                parts = {b: wy[b] * along for b in SHIFTS}
                if landing[i + a] is not None:
                    parts = {b: parts[b] + landing[i + a][b] for b in SHIFTS}
                landing[i + a] = parts
        for r in range(3):
            for b in SHIFTS:
                fall[b + 1, l, r : r + 1, :] += jnp.sum(landing[r][b], 0, keepdims=True)

    wait_rows(due[2], recv_sem.at[2])
    corner = [blend([corner_in[s, t] for t in range(len(ys))], odd_lane) for s in range(2)]
    values = []
    for n in range(6):
        beside = blend([col_in[t, n] for t in range(len(ys))], odd_lane)
        below = jnp.where(lane < 4 * cx, beside, turn(corner[1], 4 * (cx - 1) - 8 * n, 1))
        values.append(jnp.where(lane >= cy - 4, turn(corner[0], cy - 4 - 8 * n, 1), below))
    radius, dry, east, north, weight, turns = values
    root, volume, gain = expand(prepare(radius, dry), east, north, col_terms)
    radius, weight_left = merge(root, volume, weight, mate(weight, turns.astype(jnp.int32)))
    wx, wy = kernel_weights(east), kernel_weights(north)
    across = jnp.where(odd_lane, wy[-1], wy[1]) * (weight * gain)
    rain = {a: jnp.broadcast_to(jnp.sum(wx[a] * across, 0, keepdims=True), (cx, cy)) for a in SHIFTS}
    outer = jnp.where(lane == cy - 1, 1, 0)
    edge_fall = []
    for l in range(levels):
        sent_in = sum(take(rain[a], mod(4 * (line - a) + 2 * l + outer, cy), 1) for a in SHIFTS)
        edge_fall.append(jnp.where((lane == 0) | (lane == cy - 1), sent_in, 0.0))

    which = div(lane_e - 2 * ky, kc)
    minus_x = mod(which, 2)
    face = lane_e < 2 * ky
    minus_y = jnp.where(face, jnp.where(lane_e < ky, 0, 1), div(which, 2))
    slots = None
    for d in range(2):
        t = d if len(ys) == 2 else 0
        faces = col_in[t, 6, d : d + 1, :]
        corners = [corner_in[s, t, 2 * s + d : 2 * s + d + 1, :] for s in range(2)]
        found = jnp.where(face, faces, jnp.where(minus_x == 0, corners[0], corners[1]))
        slots = found if d == 0 else jnp.where(minus_y == 0, slots, found)
    slots = slots.astype(jnp.int32)
    move_x = jnp.where(face, 0, 1 - 2 * minus_x)
    live = slots >= 0
    level = mod(div(slots, block), levels)
    place = jnp.where(face, mod(div(slots, cy), cx), jnp.where(minus_x == 0, cy // 4 - 1, cx))
    spot = jnp.broadcast_to(jnp.where(live, 4 * place + 2 * level + minus_y, 0), (sd, width))
    chosen = iota((sd, width), 0) == jnp.where(live, div(slots, block * levels), -1)
    for n, value in enumerate((radius, weight_left, dry, east, north)):
        rec_out[n, :, pl.ds(2 * kx, width)] = jnp.sum(jnp.where(chosen, take(value, spot, 1), 0.0), 0, keepdims=True)
    box_out[:, pl.ds(2 * kx, width)] = land(slots, move_x, 1 - 2 * minus_y)

    wait_rows(due[4], recv_sem.at[4])
    side = side_growth(0)
    pl.when(me_x == nx - 1)(upper_side)
    wait_rows(due[5], recv_sem.at[5])
    side_rows(0, side)
    wait_rows(due[6], recv_sem.at[6])
    side_records(0)
    for l in range(levels):
        total = spread({b: fall[b + 1, l] for b in SHIFTS}, 1, lane) + edge_fall[l]
        moist_out[l] = moist_out[l] - VAPOUR_PER_SOURCE * total
        warm_out[l] = warm_out[l] + WARMING_FACTOR * total

    wait_rows(sent[0], send_sem.at[0])


def publish(*refs):
    count = len(refs) // 2
    sems = refs[-1]
    copies = [
        pltpu.make_async_copy(refs[n], refs[count + n], sems.at[n]) for n in range(count)
    ]
    for copy in copies:
        copy.start()
    for copy in copies:
        copy.wait()


def per_device(nx, ny, moist, warm, size, mult, dry, east, north, perm, lx, ly, lc):
    levels, cx, cy = moist.shape
    sd = size.shape[0]
    kx, ky, kc = lx.shape[2], ly.shape[2], lc.shape[2]
    narr = 2 * kx + 2 * ky + 4 * kc
    slots = sd * levels * cx
    flat = [x.reshape(slots, cy) for x in (size, mult, dry, east, north, perm)]
    f32, i32 = jnp.float32, jnp.int32
    any_space = pl.BlockSpec(memory_space=pl.ANY)
    vmem_space = pl.BlockSpec(memory_space=pltpu.VMEM)
    dma = pltpu.SemaphoreType.DMA
    shapes = (
        ((levels, cx, cy), f32),
        ((levels, cx, cy), f32),
        ((slots, cy), f32),
        ((slots, cy), f32),
        ((5, 1, narr), f32),
        ((1, narr), i32),
    )
    n_y = 1 if ny == 2 else 2
    outs = pl.pallas_call(
        functools.partial(body, (levels, cx, cy, sd, kx, ky, kc, nx, ny)),
        out_shape=tuple(pltpu.VMEM(*s) for s in shapes),
        in_specs=[any_space] * 17,
        out_specs=[vmem_space] * 6,
        scratch_shapes=[
            pltpu.VMEM((2, levels, cx, cy), f32),
            pltpu.VMEM((5, slots, cy), f32),
            pltpu.VMEM((slots, cy), i32),
            pltpu.VMEM((2, ky), i32),
            pltpu.VMEM((4, kc), i32),
            pltpu.VMEM((2, 2, levels, cx, cy), f32),
            pltpu.VMEM((n_y, 2, levels, cx, cy), f32),
            pltpu.VMEM((2, n_y, 2, levels, cx, cy), f32),
            pltpu.VMEM((2, 1, kx), i32),
            pltpu.VMEM((2, 1, kx), i32),
            pltpu.VMEM((2, 1, kx), i32),
            pltpu.VMEM((2, 5, sd * levels, cy), f32),
            pltpu.VMEM((2, 5, sd * levels, cy), f32),
            pltpu.VMEM((2, 5, sd * levels, cy), f32),
            pltpu.VMEM((2, sd * levels, cy), i32),
            pltpu.VMEM((2, sd * levels, cy), i32),
            pltpu.VMEM((2, sd, cy), f32),
            pltpu.VMEM((2, n_y, sd, cy), f32),
            pltpu.VMEM((7, sd, cy), f32),
            pltpu.VMEM((n_y, 7, sd, cy), f32),
            pltpu.VMEM((slots, cy), f32),
            pltpu.VMEM((10 * slots, cy), f32),
            pltpu.VMEM((9, slots, cy), f32),
            pltpu.VMEM((3, slots, cy), i32),
            pltpu.VMEM((levels, 9, cx, cy), f32),
            pltpu.VMEM((levels, 9, cx, cy), f32),
            pltpu.VMEM((2, 2, sd * levels, cy), f32),
            pltpu.VMEM((3, levels, cx, cy), f32),
            dma((6,)), dma((1,)), dma((7,)), pltpu.SemaphoreType.REGULAR,
        ],
        compiler_params=pltpu.CompilerParams(collective_id=0, has_side_effects=True),
    )(moist, warm, *flat, size, mult, dry, east, north, perm, lx, ly, lc)
    outs = pl.pallas_call(
        publish,
        out_shape=tuple(jax.ShapeDtypeStruct(*s) for s in shapes),
        in_specs=[vmem_space] * 6,
        out_specs=[any_space] * 6,
        scratch_shapes=[dma((6,))],
    )(*[pltpu.with_memory_space_constraint(x, pltpu.VMEM) for x in outs])
    return (
        outs[0], outs[1], outs[2].reshape(size.shape), outs[3].reshape(size.shape), outs[4], outs[5],
    )


def solution(mesh):
    cell, drop, lists = P(None, "gx", "gy"), P(None, None, "gx", "gy"), P("gx", None, "gy")
    return jax.shard_map(
        functools.partial(per_device, mesh.shape["gx"], mesh.shape["gy"]),
        mesh=mesh,
        in_specs=(cell,) * 2 + (drop,) * 6 + (lists,) * 3,
        out_specs=(cell, cell, drop, drop, cell, P("gx", "gy")),
        check_vma=False,
    )
```

```python
import functools
import math

import jax
import jax.numpy as jnp
from jax import lax
from jax.experimental import pallas as pl
from jax.experimental.pallas import tpu as pltpu
from jax.sharding import PartitionSpec as P

NEWTON = 4
MIX_HORIZONTAL = 0.2
MIX_VERTICAL = 0.05
EXCESS_FACTOR = 4.2222
CURVATURE = 0.0012
KAPPA_SOLUTE = 0.6
GROWTH_STEP = 200.0
COLLIDE_RATE = 4e-07
VAPOUR_PER_SOURCE = 0.001
WARMING_FACTOR = 0.00249
LOG2E = math.log2(math.e)

MESH = pl.DeviceIdType.MESH
SHIFTS = (-1, 0, 1)
SIDES = (1, -1)
MOVES = (1, -1)


def div(x, n):
    return lax.shift_right_arithmetic(x, jnp.int32(n.bit_length() - 1))


def mod(x, n):
    return lax.bitwise_and(x, jnp.int32(n - 1))


def iota(shape, dim):
    return lax.broadcasted_iota(jnp.int32, shape, dim)


def turn(x, shift, dim):
    shift %= x.shape[dim]
    return pltpu.roll(x, shift, dim) if shift else x


def take(x, index, dim):
    return jnp.take_along_axis(x, index, axis=dim)


def kernel_weights(offset):
    return {
        -1: jnp.maximum(0.5 - offset, 0.0),
        0: 1.0 - jnp.abs(offset - 0.5),
        1: jnp.maximum(offset - 0.5, 0.0),
    }


def prepare(radius, dry):
    inverse = 1.0 / radius
    square = inverse * inverse
    lowest = dry * dry
    strength = (1.5 * GROWTH_STEP * KAPPA_SOLUTE) * (lowest * dry)
    pull = strength * (square * inverse)
    area = radius * radius
    return (
        area - (GROWTH_STEP * CURVATURE) * inverse,
        (5.0 / 3.0) * pull,
        1.0 + pull * square,
        strength,
        lowest,
        area * radius,
    )


def settle(level, top, bottom, strength, lowest):
    above = jnp.maximum(level + top, lowest * bottom)
    flat = lax.rsqrt(above * bottom)
    for sweep in range(NEWTON - 1):
        inverse_root = bottom * flat
        square = inverse_root * inverse_root
        pull = strength * (square * inverse_root)
        bottom = 1.0 + pull * square
        above = jnp.maximum(level + (5.0 / 3.0) * pull, lowest * bottom)
        flat = lax.rsqrt(above * bottom)
    root = above * flat
    return root, (root * root) * root


def differences(near):
    centre = near[0, 0]
    terms = {(0, 0): centre}
    for s in SIDES:
        terms[s, 0] = near[s, 0] - centre
        terms[0, s] = near[0, s] - centre
    for a in SIDES:
        for b in SIDES:
            terms[a, b] = near[a, b] - near[a, 0] - terms[0, b]
    return terms


def interpolate(terms, east, north, reach_x, reach_y):
    right, up = east > 0.5, north > 0.5
    slope_x = jnp.where(right, terms[1, 0], terms[-1, 0])
    slope_y = jnp.where(up, terms[0, 1], terms[0, -1])
    twist = jnp.where(
        right, jnp.where(up, terms[1, 1], terms[1, -1]), jnp.where(up, terms[-1, 1], terms[-1, -1])
    )
    return terms[0, 0] + reach_x * slope_x + reach_y * (slope_y + reach_x * twist)


def match(weight, other, first):
    big = (weight > other) | ((weight == other) & first)
    rate = (-COLLIDE_RATE * LOG2E) * jnp.where(big, weight, other)
    return rate, jnp.where(big, other, 0.0)


def collide(radius, cube, other, rate, eaten):
    total = radius + other
    chance = 1.0 - jnp.exp2(rate * (total * total) * (total * jnp.abs(radius - other)))
    volume = cube + chance * (other * other * other)
    merged = jnp.exp2(jnp.log(volume) * (LOG2E / 3.0))
    return jnp.where(eaten > 0.0, radius, merged), chance * eaten


def spread(parts, dim, index):
    size = parts[0].shape[dim]
    back, ahead = turn(parts[-1], -1, dim), turn(parts[1], 1, dim)
    return parts[0] + jnp.where(index == size - 1, 0.0, back) + jnp.where(index == 0, 0.0, ahead)


def body(
    sizes,
    moist_in, warm_in, size_in, mult_in, dry_in, east_in, north_in, perm_in,
    size_cells, mult_cells, dry_cells, east_cells, north_cells, perm_cells,
    lx_in, ly_in, lc_in,
    moist_out, warm_out, size_out, mult_out, rec_out, box_out,
    state, drops, perm, ly, lc,
    state_x, state_y, diag_in, list_pack, list_sort, list_x,
    row_pack, row_sort, row_x, turn_pack, rank_of, corner_pack, corner_in, col_pack, col_in,
    mask, ready, share, bits, near, near_up, late_x, fall, brink_fall,
    in_sem, send_sem, recv_sem, lower_in,
):
    levels, cx, cy, sd, kx, ky, kc, nx, ny = sizes
    me_x = lax.axis_index("gx")
    me_y = lax.axis_index("gy")
    ys = (1,) if ny == 2 else (1, -1)
    half = cx // 2
    rows = sd * levels
    slots_all = rows * cx
    block = cx * cy
    tall = levels * cx
    deep = kx // cy
    edges = (cx - 1, 0)
    bands = (pl.ds(cx - 3, 3), pl.ds(0, 3))

    def at(d):
        return (lax.rem(me_x + d[0] + nx, nx), lax.rem(me_y + d[1] + ny, ny))

    def wait_rows(count, sem):
        whole = ready.at[pl.ds(0, count), :]
        pltpu.make_async_copy(whole, whole, sem).wait()

    def count_rows(ref):
        total = 1
        for n in ref.shape:
            total *= n
        return total // cy

    brought = [0, 0, 0]

    def bring(source, target, group):
        pltpu.make_async_copy(source, target, in_sem.at[group]).start()
        brought[group] += count_rows(target)

    cells = (size_cells, dry_cells, east_cells, north_cells, mult_cells)

    def bring_rows(s, chosen, group):
        for n in chosen:
            for l in range(levels):
                stretch = pl.ds(l * sd, sd)
                if n < 5:
                    bring(cells[n].at[:, l, edges[s], :], row_pack.at[s, n, stretch, :], group)
                else:
                    bring(perm_cells.at[:, l, edges[s], :], turn_pack.at[s, stretch, :], group)

    bring_rows(0, (5, 0, 1), 1)
    bring_rows(0, (2, 3, 4), 2)
    bring(lx_in.at[0, pl.ds(0, 1), :], list_pack.at[0], 2)
    bring(moist_in, state.at[0], 0)
    bring(warm_in, state.at[1], 0)

    beside = [0] + list(ys)
    barrier = pltpu.get_barrier_semaphore()
    for d in [(-1, dy) for dy in beside] + [(0, dy) for dy in ys]:
        pl.semaphore_signal(barrier, inc=1, device_id=at(d), device_id_type=MESH)

    bring_rows(1, range(6), 0)
    bring(lx_in.at[0, pl.ds(1, 1), :], list_pack.at[1], 0)
    lists = [
        pltpu.make_async_copy(source.at[0], target, in_sem.at[3 + n])
        for n, (source, target) in enumerate(((ly_in, ly), (lc_in, lc)))
    ]
    for copy in lists:
        copy.start()
    for n, source in enumerate((size_in, mult_in, dry_in, east_in, north_in)):
        bring(source, drops.at[n], 0)
    bring(perm_in, perm, 0)

    sent = [0]
    due = [0] * 7

    def send(source, target, group, d):
        pltpu.make_async_remote_copy(
            src_ref=source, dst_ref=target, send_sem=send_sem.at[0], recv_sem=recv_sem.at[group],
            device_id=at(d), device_id_type=MESH,
        ).start()
        sent[0] += count_rows(source)
        due[group] += count_rows(source)

    line = iota((cx, cy), 0)
    lane = iota((cx, cy), 1)
    low_half = line < half

    def send_fields(s):
        own, far = state.at[:, :, bands[s], :], MOVES[s]
        group = (1, 0)[s]
        send(own, state_x.at[s, :, :, bands[s], :], group, (far, 0))
        for t, dy in enumerate(ys):
            send(own, diag_in.at[s, t, :, :, bands[s], :], group, (far, dy))

    seat = iota((sd, cy), 0)

    def sort_rows(s, chosen):
        for l in range(levels):
            stretch = pl.ds(l * sd, sd)
            turns = turn_pack[s, stretch, :]
            for n in chosen:
                row_sort[s, n, stretch, :] = take(row_pack[s, n, stretch, :], turns, 0)

    def send_first(s):
        sort_rows(s, (0, 1))
        send(row_sort.at[s, 0:2], row_x.at[s, 0:2], (4, 3)[s], (MOVES[s], 0))

    def send_rows(s):
        sort_rows(s, (2, 3, 4))
        send(row_sort.at[s, 2:4], row_x.at[s, 2:4], (4, 3)[s], (MOVES[s], 0))
        send(row_sort.at[s, 4], row_x.at[s, 4], (5, 3)[s], (MOVES[s], 0))
        for l in range(levels):
            rank = jnp.zeros((sd, cy), jnp.int32)
            for p in range(1, sd):
                here = jnp.broadcast_to(turn_pack[s, l * sd + p : l * sd + p + 1, :], (sd, cy)) == seat
                rank = jnp.where(here, p, rank)
            rank_of[s, pl.ds(l * sd, sd), :] = rank
        slots = list_pack[s].reshape(deep, cy)
        k = div(slots, block * levels)
        row = mod(div(slots, block), levels) * sd + k
        place = jnp.zeros((deep, cy), jnp.int32)
        for r in range(rows):
            value = take(jnp.broadcast_to(rank_of[s, r : r + 1, :], (deep, cy)), mod(slots, cy), 1)
            place = jnp.where(row == r, value, place)
        moved = jnp.where(slots >= 0, slots + (place - k) * (block * levels), -1)
        list_sort[s] = moved.reshape(1, kx)
        send(list_sort.at[s], list_x.at[s], (6, 3)[s], (MOVES[s], 0))

    def send_corner(s):
        tile = None
        for n in range(6):
            for l in range(levels):
                stretch = pl.ds(l * sd, sd)
                value = row_pack[s, n, stretch, :] if n < 5 else turn_pack[s, stretch, :].astype(jnp.float32)
                spot = 8 * n + 4 * s + 2 * l
                moved = turn(value, spot + 1, 1)
                tile = moved if tile is None else jnp.where(lane >= spot, moved, tile)
        corner_pack[s] = tile
        for d in range(2):
            spot = 2 * ky + kc * (2 * d + s)
            corner_pack[s, 2 * s + d : 2 * s + d + 1, spot : spot + kc] = lc[
                2 * s + d : 2 * s + d + 1, :
            ].astype(jnp.float32)
        for t, dy in enumerate(ys):
            send(corner_pack.at[s], corner_in.at[s, t], 2, (MOVES[s], dy))

    pl.semaphore_wait(barrier, len(beside) + len(ys))
    for dy in beside:
        for f, source in enumerate((moist_in, warm_in)):
            target = state_x.at[0] if dy == 0 else diag_in.at[0, ys.index(dy)]
            send(source.at[:, bands[0], :], target.at[f, :, bands[0], :], 1, (1, dy))
    for dy in beside:
        pl.semaphore_signal(lower_in, inc=1, device_id=at((1, dy)), device_id_type=MESH)
    wait_rows(brought[1], in_sem.at[1])
    send_first(0)
    wait_rows(brought[2], in_sem.at[2])
    send_rows(0)
    for copy in lists:
        copy.wait()
    send_corner(0)
    wait_rows(brought[0], in_sem.at[0])
    for t, dy in enumerate(ys):
        send(state, state_y.at[t], 0, (0, dy))
    attributes = (0, 2, 3, 4, 1)
    for n in range(6):
        tile = None
        for i in range(cx):
            for l in range(levels):
                picked = pl.ds(l * cx + i, sd, stride=tall)
                value = drops[attributes[n], picked, :] if n < 5 else perm[picked, :].astype(jnp.float32)
                spot = 4 * i + 2 * l
                moved = turn(value, spot + 1, 1)
                tile = moved if tile is None else jnp.where(lane >= spot, moved, tile)
        col_pack[n] = tile
    for d in range(2):
        col_pack[6, d : d + 1, d * ky : (d + 1) * ky] = ly[d : d + 1, :].astype(jnp.float32)
    for t, dy in enumerate(ys):
        send(col_pack, col_in.at[t], 2, (0, dy))

    def span(n, k):
        return pl.ds(n * slots_all + k * tall, tall)

    order = [perm[k * tall : (k + 1) * tall, :] for k in range(sd)]
    for m in range(sd):
        part = pl.ds(m * tall, tall)
        weight = drops[1, part, :]
        partner = jnp.zeros((tall, cy), jnp.int32)
        first = jnp.zeros((tall, cy), jnp.int32)
        for p in range(sd):
            mine = order[p] == m
            partner = jnp.where(mine, order[p ^ 1], partner)
            if p % 2 == 0:
                first = jnp.where(mine, 1, first)
        other = drops[1, pl.ds(0, tall), :]
        for k in range(1, sd):
            other = jnp.where(partner == k, drops[1, pl.ds(k * tall, tall), :], other)
        rate, eaten = match(weight, other, first > 0)
        for n in range(3):
            bits[n, part, :] = mod(lax.shift_right_logical(partner, jnp.int32(n)), 2)
        for n, value in enumerate(prepare(drops[0, part, :], drops[2, part, :])):
            ready[span(n, m), :] = value
        east, north = drops[3, part, :], drops[4, part, :]
        ready[span(6, m), :] = jnp.abs(east - 0.5)
        ready[span(7, m), :] = jnp.abs(north - 0.5)
        ready[span(8, m), :] = rate
        ready[span(9, m), :] = eaten
        wx, wy = kernel_weights(east), kernel_weights(north)
        for a in SHIFTS:
            along = wx[a] * weight
            for b in SHIFTS:
                share[3 * a + b + 4, part, :] = wy[b] * along

    mask[...] = jnp.ones_like(mask)
    for r, side in enumerate(edges):
        slots = list_pack[r]
        hot_row = iota((rows, kx), 0) == div(slots, block)
        hot_lane = jnp.where(iota((cy, kx), 0) == mod(slots, cy), 1.0, 0.0).astype(jnp.bfloat16)
        named = lax.dot_general(
            jnp.where(hot_row, 1.0, 0.0).astype(jnp.bfloat16), hot_lane,
            (((1,), (1,)), ((), ())), preferred_element_type=jnp.float32,
        )
        mask[pl.ds(side, rows, stride=cx), :] = 1.0 - named

    width = 2 * ky + 4 * kc
    lane_e = iota((1, width), 1)
    high = (lane_e < ky) | ((lane_e >= 2 * ky) & (lane_e < 2 * ky + 2 * kc))
    high_all = jnp.broadcast_to(high, (slots_all, width))
    slots = jnp.concatenate(
        [ly[0:1, :], ly[1:2, :], lc[0:1, :], lc[2:3, :], lc[1:2, :], lc[3:4, :]], 1
    )
    hot_e = jnp.where(iota((slots_all, width), 0) == div(slots, cy), 1.0, 0.0)
    left_high = jnp.max(jnp.where(high_all, hot_e, 0.0), 1, keepdims=True)
    left_low = jnp.max(jnp.where(high_all, 0.0, hot_e), 1, keepdims=True)
    lane_all = iota((slots_all, cy), 1)
    mask[...] = mask[...] * (
        1.0 - jnp.where(lane_all == cy - 1, left_high, jnp.where(lane_all == 0, left_low, 0.0))
    )

    def land(slots, move_x, move_y):
        level = mod(div(slots, block), levels)
        i = mod(mod(div(slots, cy), cx) + move_x, cx)
        target = (level * cx + i) * cy + mod(mod(slots, cy) + move_y, cy)
        return jnp.where(slots >= 0, target, -1)

    def blend(parts, pick_second):
        return parts[0] if len(parts) == 1 else jnp.where(pick_second, parts[1], parts[0])

    left_lanes = lane < cy // 2
    odd_lane = mod(lane, 2) == 1
    group = div(lane, 4)
    keys = [(a, b) for a in SHIFTS for b in SHIFTS]

    def climate(fields):
        deep_lane = iota(fields[0][0][0].shape, 1)
        odd = mod(deep_lane, 2) == 1

        def fixed(value, spot):
            return take(value, jnp.full(value.shape, spot, jnp.int32), 1)

        def reach(own, other, s):
            if s == 0:
                return own
            inside = deep_lane < cy - s if s > 0 else deep_lane >= -s
            return jnp.where(inside, turn(own, -s, 1), turn(other, -s, 1))

        def brink(own, other, s):
            if s == 0:
                return take(other, jnp.where(odd, 0, cy - 1), 1)
            if s > 0:
                return jnp.where(odd, fixed(other, s), fixed(own, s - 1))
            return jnp.where(odd, fixed(own, cy + s), fixed(other, cy - 1 + s))

        def humidity(cut):
            raw = [[{s: cut(*fields[f][l], s) for s in range(-2, 3)} for l in range(levels)] for f in range(2)]
            mixed = []
            for f in range(2):
                mixed.append([])
                for l in range(levels):
                    at_shift = {}
                    for b in SHIFTS:
                        centre = raw[f][l][b]
                        around = raw[f][l][b - 1] + raw[f][l][b + 1] + (turn(centre, -1, 0) + turn(centre, 1, 0))
                        stacked = raw[f][min(l + 1, levels - 1)][b] + raw[f][max(l - 1, 0)][b]
                        at_shift[b] = (
                            (1.0 - 4.0 * MIX_HORIZONTAL - 2.0 * MIX_VERTICAL) * centre
                            + MIX_HORIZONTAL * around + MIX_VERTICAL * stacked
                        )
                    mixed[f].append(at_shift)
            humid = []
            for l in range(levels):
                humid.append({})
                for b in SHIFTS:
                    warmth = mixed[1][l][b]
                    decay = jnp.exp2((-17.27 * LOG2E) * (warmth - 273.15) / (warmth - 35.86))
                    humid[l][b] = (GROWTH_STEP / EXCESS_FACTOR) * (mixed[0][l][b] * decay) - GROWTH_STEP
            return mixed, humid

        mixed, humid = humidity(reach)
        terms = [differences({(a, b): turn(humid[l][b], -a, 0) for a, b in keys}) for l in range(levels)]
        _, column = humidity(brink)
        wide_level = mod(div(deep_lane, 2), 2) == 1
        column = {b: jnp.where(wide_level, column[1][b], column[0][b]) for b in SHIFTS}
        return mixed, terms, column

    def from_row(value, a):
        return take(value, mod(group + a, cx), 0)

    def mate(weight, turns):
        rank = jnp.zeros((sd, cy), jnp.int32)
        for p in range(1, sd):
            rank = jnp.where(jnp.broadcast_to(turns[p : p + 1], (sd, cy)) == seat, p, rank)
        partner = take(turns, rank ^ 1, 0)
        return partner, match(weight, take(weight, partner, 0), mod(rank, 2) == 0)

    def expand(prepared, east, north, around):
        base, top, bottom, strength, lowest, cube = prepared
        level = base + interpolate(around, east, north, jnp.abs(east - 0.5), jnp.abs(north - 0.5))
        root, volume = settle(level, top, bottom, strength, lowest)
        return root, volume, volume - cube

    across_pair = seat ^ 1

    def pair(weight):
        return across_pair, match(weight, take(weight, across_pair, 0), mod(seat, 2) == 0)

    def merge(root, volume, weight, mated):
        partner, (rate, eaten) = mated
        after, lost = collide(root, volume, take(root, partner, 0), rate, eaten)
        return after, weight - lost

    def surround(ref, l, r):
        return {key: jnp.broadcast_to(ref[l, n, r : r + 1, :], (sd, cy)) for n, key in enumerate(keys)}

    def side_growth(s):
        ref, r = ((near, cx - 1), (near_up, 0))[s]
        found = []
        for l in range(levels):
            radius, dry, east, north = (row_x[s, n, pl.ds(l * sd, sd), :] for n in range(4))
            found.append(expand(prepare(radius, dry), east, north, surround(ref, l, r)))
        return found

    def side_rows(s, found):
        home = (0, cx - 1)[s]
        for l in range(levels):
            stretch = pl.ds(l * sd, sd)
            root, volume, gain = found[l]
            weight = row_x[s, 4, stretch, :]
            radius, weight_left = merge(root, volume, weight, pair(weight))
            late_x[s, 0, stretch, :] = radius
            late_x[s, 1, stretch, :] = weight_left
            wx, wy = kernel_weights(row_x[s, 2, stretch, :]), kernel_weights(row_x[s, 3, stretch, :])
            along = wx[MOVES[s]] * (weight * gain)
            for b in SHIFTS:
                fall[b + 1, l, home : home + 1, :] += jnp.sum(wy[b] * along, 0, keepdims=True)

    def side_records(s):
        slots = list_x[s].reshape(deep, cy)
        level = mod(div(slots, block), levels)
        row = jnp.where(slots >= 0, level * sd + div(slots, block * levels), -1)
        column = mod(slots, cy)
        fields = [(2, row_x, 1), (3, row_x, 2), (4, row_x, 3), (0, late_x, 0), (1, late_x, 1)]
        for n, source, from_n in fields:
            got = jnp.zeros((deep, cy), jnp.float32)
            for r in range(rows):
                value = jnp.broadcast_to(source[s, from_n, r : r + 1, :], (deep, cy))
                got = jnp.where(row == r, take(value, column, 1), got)
            rec_out[n, :, pl.ds(s * kx, kx)] = got.reshape(1, kx)
        box_out[:, pl.ds(s * kx, kx)] = land(slots, MOVES[s], 0).reshape(1, kx)

    pl.semaphore_wait(lower_in, len(beside))
    send_fields(1)
    send_first(1)
    send_rows(1)
    send_corner(1)

    wait_rows(due[0], recv_sem.at[0])
    fields = []
    for f in range(2):
        fields.append([])
        for l in range(levels):
            side_y = blend([state_y[t, f, l] for t in range(len(ys))], left_lanes)
            far = blend([diag_in[1, t, f, l] for t in range(len(ys))], left_lanes)
            fields[f].append(
                (jnp.concatenate([state[f, l], state_x[1, f, l]], 0), jnp.concatenate([side_y, far], 0))
            )
    mixed, terms, column = climate(fields)
    window = {key: jnp.concatenate([t[key][:cx] for t in terms], 0) for key in keys}
    for l in range(levels):
        for n, key in enumerate(keys):
            near_up[l, n] = terms[l][key][cx:]
        moist_out[l] = mixed[0][l][0][:cx]
        warm_out[l] = mixed[1][l][0][:cx]
    inside = {
        (a, b): jnp.where(
            mod(group + a, cy // 4) < cx, from_row(column[b][:cx], a), from_row(column[b][cx:], a)
        )
        for a, b in keys
    }

    grown = []
    cubes = []
    deposit = {}
    for k in range(sd):
        part = pl.ds(k * tall, tall)
        base, top, bottom, strength, lowest, cube, reach_x, reach_y = (ready[span(n, k), :] for n in range(8))
        level = base + interpolate(window, drops[3, part, :], drops[4, part, :], reach_x, reach_y)
        root, volume = settle(level, top, bottom, strength, lowest)
        gain = volume - cube
        for a, b in keys:
            term = share[3 * a + b + 4, part, :] * gain
            deposit[a, b] = term if k == 0 else deposit[a, b] + term
        grown.append(root)
        cubes.append(volume)

    for l in range(levels):
        for b in SHIFTS:
            parts = {a: jnp.where(line < 2, 0.0, deposit[a, b][l * cx : (l + 1) * cx]) for a in SHIFTS}
            fall[b + 1, l] = spread(parts, 0, line)

    for m in range(sd):
        part = pl.ds(m * tall, tall)
        found = grown
        for n in range(3):
            odd = bits[n, part, :] > 0
            found = [jnp.where(odd, found[2 * i + 1], found[2 * i]) for i in range(len(found) // 2)]
        radius, lost = collide(grown[m], cubes[m], found[0], ready[span(8, m), :], ready[span(9, m), :])
        size_out[part, :] = radius
        mult_out[part, :] = mask[part, :] * (drops[1, part, :] - lost)

    def upper_side():
        wait_rows(due[3], recv_sem.at[3])
        side_rows(1, side_growth(1))
        side_records(1)

    pl.when(me_x != nx - 1)(upper_side)

    redo = [(l, i) for l in range(levels) for i in range(2)]
    waiting = {}
    for l, i in redo:
        picked = pl.ds(l * cx + i, sd, stride=tall)
        radius, weight, dry, east, north = (drops[n, picked, :] for n in range(5))
        waiting[l, i] = (
            prepare(radius, dry), weight, east, north, mate(weight, perm[picked, :]), mask[picked, :]
        )

    wait_rows(due[1], recv_sem.at[1])
    fields = []
    for f in range(2):
        fields.append([])
        for l in range(levels):
            side_y = blend([state_y[t, f, l] for t in range(len(ys))], left_lanes)
            far = blend([diag_in[0, t, f, l] for t in range(len(ys))], left_lanes)
            fields[f].append(
                (jnp.where(low_half, state[f, l], state_x[0, f, l]), jnp.where(low_half, side_y, far))
            )
    mixed, terms, column = climate(fields)
    for l in range(levels):
        for n, key in enumerate(keys):
            near[l, n] = terms[l][key]
        moist_out[l, 0:1, :] = mixed[0][l][0][0:1]
        warm_out[l, 0:1, :] = mixed[1][l][0][0:1]
    col_terms = differences(
        {
            (a, b): jnp.where(mod(group + a + 2, cy // 4) < 4, from_row(column[b], a), inside[a, b])
            for a, b in keys
        }
    )
    for l in range(levels):
        landing = [None] * 3
        for i in range(2):
            picked = pl.ds(l * cx + i, sd, stride=tall)
            prepared, weight, east, north, mated, keep = waiting[l, i]
            root, volume, gain = expand(prepared, east, north, surround(near, l, i))
            radius, weight_left = merge(root, volume, weight, mated)
            size_out[picked, :] = radius
            mult_out[picked, :] = keep * weight_left
            wx, wy = kernel_weights(east), kernel_weights(north)
            for a in SHIFTS:
                if i + a < 0:
                    continue
                along = wx[a] * (weight * gain)
                parts = {b: wy[b] * along for b in SHIFTS}
                if landing[i + a] is not None:
                    parts = {b: parts[b] + landing[i + a][b] for b in SHIFTS}
                landing[i + a] = parts
        for r in range(3):
            for b in SHIFTS:
                fall[b + 1, l, r : r + 1, :] += jnp.sum(landing[r][b], 0, keepdims=True)

    pl.when(me_x == nx - 1)(upper_side)

    def columns():
        wait_rows(due[2], recv_sem.at[2])
        corner = [blend([corner_in[s, t] for t in range(len(ys))], odd_lane) for s in range(2)]
        values = []
        for n in range(6):
            beside = blend([col_in[t, n] for t in range(len(ys))], odd_lane)
            below = jnp.where(lane < 4 * cx, beside, turn(corner[1], 4 * (cx - 1) - 8 * n, 1))
            values.append(jnp.where(lane >= cy - 4, turn(corner[0], cy - 4 - 8 * n, 1), below))
        radius, dry, east, north, weight, turns = values
        root, volume, gain = expand(prepare(radius, dry), east, north, col_terms)
        radius, weight_left = merge(root, volume, weight, mate(weight, turns.astype(jnp.int32)))
        wx, wy = kernel_weights(east), kernel_weights(north)
        across = jnp.where(odd_lane, wy[-1], wy[1]) * (weight * gain)
        rain = {a: jnp.broadcast_to(jnp.sum(wx[a] * across, 0, keepdims=True), (cx, cy)) for a in SHIFTS}
        outer = jnp.where(lane == cy - 1, 1, 0)
        for l in range(levels):
            sent_in = sum(take(rain[a], mod(4 * (line - a) + 2 * l + outer, cy), 1) for a in SHIFTS)
            brink_fall[l] = jnp.where((lane == 0) | (lane == cy - 1), sent_in, 0.0)

        which = div(lane_e - 2 * ky, kc)
        minus_x = mod(which, 2)
        face = lane_e < 2 * ky
        minus_y = jnp.where(face, jnp.where(lane_e < ky, 0, 1), div(which, 2))
        slots = None
        for d in range(2):
            t = d if len(ys) == 2 else 0
            faces = col_in[t, 6, d : d + 1, :]
            corners = [corner_in[s, t, 2 * s + d : 2 * s + d + 1, :] for s in range(2)]
            found = jnp.where(face, faces, jnp.where(minus_x == 0, corners[0], corners[1]))
            slots = found if d == 0 else jnp.where(minus_y == 0, slots, found)
        slots = slots.astype(jnp.int32)
        move_x = jnp.where(face, 0, 1 - 2 * minus_x)
        live = slots >= 0
        level = mod(div(slots, block), levels)
        place = jnp.where(face, mod(div(slots, cy), cx), jnp.where(minus_x == 0, cy // 4 - 1, cx))
        spot = jnp.broadcast_to(jnp.where(live, 4 * place + 2 * level + minus_y, 0), (sd, width))
        chosen = iota((sd, width), 0) == jnp.where(live, div(slots, block * levels), -1)
        for n, value in enumerate((radius, weight_left, dry, east, north)):
            rec_out[n, :, pl.ds(2 * kx, width)] = jnp.sum(jnp.where(chosen, take(value, spot, 1), 0.0), 0, keepdims=True)
        box_out[:, pl.ds(2 * kx, width)] = land(slots, move_x, 1 - 2 * minus_y)

    def rows_below():
        wait_rows(due[4], recv_sem.at[4])
        side = side_growth(0)
        wait_rows(due[5], recv_sem.at[5])
        side_rows(0, side)
        wait_rows(due[6], recv_sem.at[6])
        side_records(0)

    def total_up():
        for l in range(levels):
            total = spread({b: fall[b + 1, l] for b in SHIFTS}, 1, lane) + brink_fall[l]
            moist_out[l] = moist_out[l] - VAPOUR_PER_SOURCE * total
            warm_out[l] = warm_out[l] + WARMING_FACTOR * total

    @pl.when(me_y == 0)
    def _():
        columns()
        rows_below()
        total_up()

    @pl.when(me_y != 0)
    def _():
        rows_below()
        columns()
        total_up()

    wait_rows(sent[0], send_sem.at[0])


def publish(*refs):
    whole, sem = refs[-2:]
    count = len(refs) // 2 - 1
    for n in range(count):
        pltpu.make_async_copy(refs[n], refs[count + n], sem).start()
    pltpu.make_async_copy(whole, whole, sem).wait()


def per_device(nx, ny, moist, warm, size, mult, dry, east, north, perm, lx, ly, lc):
    levels, cx, cy = moist.shape
    sd = size.shape[0]
    kx, ky, kc = lx.shape[2], ly.shape[2], lc.shape[2]
    narr = 2 * kx + 2 * ky + 4 * kc
    slots = sd * levels * cx
    flat = [x.reshape(slots, cy) for x in (size, mult, dry, east, north, perm)]
    f32, i32 = jnp.float32, jnp.int32
    any_space = pl.BlockSpec(memory_space=pl.ANY)
    vmem_space = pl.BlockSpec(memory_space=pltpu.VMEM)
    dma = pltpu.SemaphoreType.DMA
    shapes = (
        ((levels, cx, cy), f32),
        ((levels, cx, cy), f32),
        ((slots, cy), f32),
        ((slots, cy), f32),
        ((5, 1, narr), f32),
        ((1, narr), i32),
    )
    n_y = 1 if ny == 2 else 2
    total = 2 * levels * cx + 2 * slots + 6 * narr // cy
    outs = pl.pallas_call(
        functools.partial(body, (levels, cx, cy, sd, kx, ky, kc, nx, ny)),
        out_shape=tuple(pltpu.VMEM(*s) for s in shapes),
        in_specs=[any_space] * 17,
        out_specs=[vmem_space] * 6,
        scratch_shapes=[
            pltpu.VMEM((2, levels, cx, cy), f32),
            pltpu.VMEM((5, slots, cy), f32),
            pltpu.VMEM((slots, cy), i32),
            pltpu.VMEM((2, ky), i32),
            pltpu.VMEM((4, kc), i32),
            pltpu.VMEM((2, 2, levels, cx, cy), f32),
            pltpu.VMEM((n_y, 2, levels, cx, cy), f32),
            pltpu.VMEM((2, n_y, 2, levels, cx, cy), f32),
            pltpu.VMEM((2, 1, kx), i32),
            pltpu.VMEM((2, 1, kx), i32),
            pltpu.VMEM((2, 1, kx), i32),
            pltpu.VMEM((2, 5, sd * levels, cy), f32),
            pltpu.VMEM((2, 5, sd * levels, cy), f32),
            pltpu.VMEM((2, 5, sd * levels, cy), f32),
            pltpu.VMEM((2, sd * levels, cy), i32),
            pltpu.VMEM((2, sd * levels, cy), i32),
            pltpu.VMEM((2, sd, cy), f32),
            pltpu.VMEM((2, n_y, sd, cy), f32),
            pltpu.VMEM((7, sd, cy), f32),
            pltpu.VMEM((n_y, 7, sd, cy), f32),
            pltpu.VMEM((slots, cy), f32),
            pltpu.VMEM((10 * slots, cy), f32),
            pltpu.VMEM((9, slots, cy), f32),
            pltpu.VMEM((3, slots, cy), i32),
            pltpu.VMEM((levels, 9, cx, cy), f32),
            pltpu.VMEM((levels, 9, cx, cy), f32),
            pltpu.VMEM((2, 2, sd * levels, cy), f32),
            pltpu.VMEM((3, levels, cx, cy), f32),
            pltpu.VMEM((levels, cx, cy), f32),
            dma((5,)), dma((1,)), dma((7,)), pltpu.SemaphoreType.REGULAR,
        ],
        compiler_params=pltpu.CompilerParams(collective_id=0, has_side_effects=True),
    )(moist, warm, *flat, size, mult, dry, east, north, perm, lx, ly, lc)
    outs = pl.pallas_call(
        publish,
        out_shape=tuple(jax.ShapeDtypeStruct(*s) for s in shapes),
        in_specs=[vmem_space] * 6,
        out_specs=[any_space] * 6,
        scratch_shapes=[pltpu.VMEM((total, cy), f32), dma],
    )(*[pltpu.with_memory_space_constraint(x, pltpu.VMEM) for x in outs])
    return (
        outs[0], outs[1], outs[2].reshape(size.shape), outs[3].reshape(size.shape), outs[4], outs[5],
    )


def solution(mesh):
    cell, drop, lists = P(None, "gx", "gy"), P(None, None, "gx", "gy"), P("gx", None, "gy")
    return jax.shard_map(
        functools.partial(per_device, mesh.shape["gx"], mesh.shape["gy"]),
        mesh=mesh,
        in_specs=(cell,) * 2 + (drop,) * 6 + (lists,) * 3,
        out_specs=(cell, cell, drop, drop, cell, P("gx", "gy")),
        check_vma=False,
    )
```

```python
import functools
import math

import jax
import jax.numpy as jnp
from jax import lax
from jax.experimental import pallas as pl
from jax.experimental.pallas import tpu as pltpu
from jax.sharding import PartitionSpec as P

NEWTON = 4
MIX_HORIZONTAL = 0.2
MIX_VERTICAL = 0.05
EXCESS_FACTOR = 4.2222
CURVATURE = 0.0012
KAPPA_SOLUTE = 0.6
GROWTH_STEP = 200.0
COLLIDE_RATE = 4e-07
VAPOUR_PER_SOURCE = 0.001
WARMING_FACTOR = 0.00249
LOG2E = math.log2(math.e)

MESH = pl.DeviceIdType.MESH
SHIFTS = (-1, 0, 1)
SIDES = (1, -1)
MOVES = (1, -1)


def div(x, n):
    return lax.shift_right_arithmetic(x, jnp.int32(n.bit_length() - 1))


def mod(x, n):
    return lax.bitwise_and(x, jnp.int32(n - 1))


def iota(shape, dim):
    return lax.broadcasted_iota(jnp.int32, shape, dim)


def turn(x, shift, dim):
    shift %= x.shape[dim]
    return pltpu.roll(x, shift, dim) if shift else x


def take(x, index, dim):
    return jnp.take_along_axis(x, index, axis=dim)


def kernel_weights(offset):
    return {
        -1: jnp.maximum(0.5 - offset, 0.0),
        0: 1.0 - jnp.abs(offset - 0.5),
        1: jnp.maximum(offset - 0.5, 0.0),
    }


def prepare(radius, dry):
    inverse = 1.0 / radius
    square = inverse * inverse
    lowest = dry * dry
    strength = (1.5 * GROWTH_STEP * KAPPA_SOLUTE) * (lowest * dry)
    pull = strength * (square * inverse)
    area = radius * radius
    return (
        area - (GROWTH_STEP * CURVATURE) * inverse,
        (5.0 / 3.0) * pull,
        1.0 + pull * square,
        strength,
        lowest,
        area * radius,
    )


def settle(level, top, bottom, strength, lowest):
    above = jnp.maximum(level + top, lowest * bottom)
    flat = lax.rsqrt(above * bottom)
    for sweep in range(NEWTON - 1):
        inverse_root = bottom * flat
        square = inverse_root * inverse_root
        pull = strength * (square * inverse_root)
        bottom = 1.0 + pull * square
        above = jnp.maximum(level + (5.0 / 3.0) * pull, lowest * bottom)
        flat = lax.rsqrt(above * bottom)
    root = above * flat
    return root, (root * root) * root


def differences(near):
    centre = near[0, 0]
    terms = {(0, 0): centre}
    for s in SIDES:
        terms[s, 0] = near[s, 0] - centre
        terms[0, s] = near[0, s] - centre
    for a in SIDES:
        for b in SIDES:
            terms[a, b] = near[a, b] - near[a, 0] - terms[0, b]
    return terms


def interpolate(terms, east, north, reach_x, reach_y):
    right, up = east > 0.5, north > 0.5
    slope_x = jnp.where(right, terms[1, 0], terms[-1, 0])
    slope_y = jnp.where(up, terms[0, 1], terms[0, -1])
    twist = jnp.where(
        right, jnp.where(up, terms[1, 1], terms[1, -1]), jnp.where(up, terms[-1, 1], terms[-1, -1])
    )
    return terms[0, 0] + reach_x * slope_x + reach_y * (slope_y + reach_x * twist)


def match(weight, other, first):
    big = (weight > other) | ((weight == other) & first)
    rate = (-COLLIDE_RATE * LOG2E) * jnp.where(big, weight, other)
    return rate, jnp.where(big, other, 0.0)


def collide(radius, cube, other, rate, eaten):
    total = radius + other
    chance = 1.0 - jnp.exp2(rate * (total * total) * (total * jnp.abs(radius - other)))
    volume = cube + chance * (other * other * other)
    merged = jnp.exp2(jnp.log(volume) * (LOG2E / 3.0))
    return jnp.where(eaten > 0.0, radius, merged), chance * eaten


def spread(parts, dim, index):
    size = parts[0].shape[dim]
    back, ahead = turn(parts[-1], -1, dim), turn(parts[1], 1, dim)
    return parts[0] + jnp.where(index == size - 1, 0.0, back) + jnp.where(index == 0, 0.0, ahead)


def body(
    sizes,
    moist_in, warm_in, size_in, mult_in, dry_in, east_in, north_in, perm_in,
    size_cells, mult_cells, dry_cells, east_cells, north_cells, perm_cells,
    lx_in, ly_in, lc_in,
    moist_out, warm_out, size_out, mult_out, rec_out, box_out,
    state, drops, perm, ly, lc,
    state_x, state_y, diag_in, list_pack, list_sort, list_x,
    row_pack, row_sort, row_x, turn_pack, rank_of, corner_pack, corner_in, col_pack, col_in,
    mask, ready, share, bits, near, near_up, late_x, fall, brink_fall,
    in_sem, send_sem, recv_sem, lower_in,
):
    levels, cx, cy, sd, kx, ky, kc, nx, ny = sizes
    me_x = lax.axis_index("gx")
    me_y = lax.axis_index("gy")
    ys = (1,) if ny == 2 else (1, -1)
    half = cx // 2
    rows = sd * levels
    slots_all = rows * cx
    block = cx * cy
    tall = levels * cx
    deep = kx // cy
    edges = (cx - 1, 0)
    bands = (pl.ds(cx - 3, 3), pl.ds(0, 3))

    def at(d):
        return (lax.rem(me_x + d[0] + nx, nx), lax.rem(me_y + d[1] + ny, ny))

    def wait_rows(count, sem):
        whole = ready.at[pl.ds(0, count), :]
        pltpu.make_async_copy(whole, whole, sem).wait()

    def count_rows(ref):
        total = 1
        for n in ref.shape:
            total *= n
        return total // cy

    brought = [0, 0, 0]

    def bring(source, target, group):
        pltpu.make_async_copy(source, target, in_sem.at[group]).start()
        brought[group] += count_rows(target)

    cells = (size_cells, dry_cells, east_cells, north_cells, mult_cells)

    def bring_rows(s, chosen, group):
        for n in chosen:
            for l in range(levels):
                stretch = pl.ds(l * sd, sd)
                if n < 5:
                    bring(cells[n].at[:, l, edges[s], :], row_pack.at[s, n, stretch, :], group)
                else:
                    bring(perm_cells.at[:, l, edges[s], :], turn_pack.at[s, stretch, :], group)

    bring_rows(0, (5, 0, 1), 1)
    bring_rows(0, (2, 3, 4), 2)
    bring(lx_in.at[0, pl.ds(0, 1), :], list_pack.at[0], 2)
    bring(moist_in, state.at[0], 0)
    bring(warm_in, state.at[1], 0)

    beside = [0] + list(ys)
    barrier = pltpu.get_barrier_semaphore()
    for d in [(-1, dy) for dy in beside] + [(0, dy) for dy in ys]:
        pl.semaphore_signal(barrier, inc=1, device_id=at(d), device_id_type=MESH)

    bring_rows(1, range(6), 0)
    bring(lx_in.at[0, pl.ds(1, 1), :], list_pack.at[1], 0)
    lists = [
        pltpu.make_async_copy(source.at[0], target, in_sem.at[3 + n])
        for n, (source, target) in enumerate(((ly_in, ly), (lc_in, lc)))
    ]
    for copy in lists:
        copy.start()
    for n, source in enumerate((size_in, mult_in, dry_in, east_in, north_in)):
        bring(source, drops.at[n], 0)
    bring(perm_in, perm, 0)

    sent = [0]
    due = [0] * 7

    def send(source, target, group, d):
        pltpu.make_async_remote_copy(
            src_ref=source, dst_ref=target, send_sem=send_sem.at[0], recv_sem=recv_sem.at[group],
            device_id=at(d), device_id_type=MESH,
        ).start()
        sent[0] += count_rows(source)
        due[group] += count_rows(source)

    line = iota((cx, cy), 0)
    lane = iota((cx, cy), 1)
    low_half = line < half

    def send_fields(s):
        own, far = state.at[:, :, bands[s], :], MOVES[s]
        group = (1, 0)[s]
        send(own, state_x.at[s, :, :, bands[s], :], group, (far, 0))
        for t, dy in enumerate(ys):
            send(own, diag_in.at[s, t, :, :, bands[s], :], group, (far, dy))

    seat = iota((sd, cy), 0)

    def look_up(load_row, row, column):
        groups = 2
        found = [None] * groups
        for m in range(rows // groups):
            for n in range(groups):
                r = n * (rows // groups) + m
                value = take(jnp.broadcast_to(load_row(r), (deep, cy)), column, 1)
                found[n] = value if m == 0 else jnp.where(row == r, value, found[n])
        while len(found) > 1:
            size = rows // len(found)
            odd = mod(div(row, size), 2) == 1
            found = [jnp.where(odd, found[2 * m + 1], found[2 * m]) for m in range(len(found) // 2)]
        return found[0]

    def sort_rows(s, chosen):
        for l in range(levels):
            stretch = pl.ds(l * sd, sd)
            turns = turn_pack[s, stretch, :]
            for n in chosen:
                row_sort[s, n, stretch, :] = take(row_pack[s, n, stretch, :], turns, 0)

    def send_first(s):
        sort_rows(s, (0, 1))
        send(row_sort.at[s, 0:2], row_x.at[s, 0:2], (4, 3)[s], (MOVES[s], 0))

    def send_rows(s):
        sort_rows(s, (2, 3, 4))
        send(row_sort.at[s, 2:4], row_x.at[s, 2:4], (4, 3)[s], (MOVES[s], 0))
        send(row_sort.at[s, 4], row_x.at[s, 4], (5, 3)[s], (MOVES[s], 0))
        for l in range(levels):
            rank = jnp.zeros((sd, cy), jnp.int32)
            for p in range(1, sd):
                here = jnp.broadcast_to(turn_pack[s, l * sd + p : l * sd + p + 1, :], (sd, cy)) == seat
                rank = jnp.where(here, p, rank)
            rank_of[s, pl.ds(l * sd, sd), :] = rank
        slots = list_pack[s].reshape(deep, cy)
        k = div(slots, block * levels)
        row = mod(div(slots, block), levels) * sd + k
        place = look_up(lambda r: rank_of[s, r : r + 1, :], row, mod(slots, cy))
        moved = jnp.where(slots >= 0, slots + (place - k) * (block * levels), -1)
        list_sort[s] = moved.reshape(1, kx)
        send(list_sort.at[s], list_x.at[s], (6, 3)[s], (MOVES[s], 0))

    def send_corner(s):
        tile = None
        for n in range(6):
            for l in range(levels):
                stretch = pl.ds(l * sd, sd)
                value = row_pack[s, n, stretch, :] if n < 5 else turn_pack[s, stretch, :].astype(jnp.float32)
                spot = 8 * n + 4 * s + 2 * l
                moved = turn(value, spot + 1, 1)
                tile = moved if tile is None else jnp.where(lane >= spot, moved, tile)
        corner_pack[s] = tile
        for d in range(2):
            spot = 2 * ky + kc * (2 * d + s)
            corner_pack[s, 2 * s + d : 2 * s + d + 1, spot : spot + kc] = lc[
                2 * s + d : 2 * s + d + 1, :
            ].astype(jnp.float32)
        for t, dy in enumerate(ys):
            send(corner_pack.at[s], corner_in.at[s, t], 2, (MOVES[s], dy))

    pl.semaphore_wait(barrier, len(beside) + len(ys))
    for dy in beside:
        for f, source in enumerate((moist_in, warm_in)):
            target = state_x.at[0] if dy == 0 else diag_in.at[0, ys.index(dy)]
            send(source.at[:, bands[0], :], target.at[f, :, bands[0], :], 1, (1, dy))
    for dy in beside:
        pl.semaphore_signal(lower_in, inc=1, device_id=at((1, dy)), device_id_type=MESH)
    wait_rows(brought[1], in_sem.at[1])
    send_first(0)
    wait_rows(brought[2], in_sem.at[2])
    send_rows(0)
    for copy in lists:
        copy.wait()
    send_corner(0)
    wait_rows(brought[0], in_sem.at[0])
    for t, dy in enumerate(ys):
        send(state, state_y.at[t], 0, (0, dy))
    attributes = (0, 2, 3, 4, 1)
    for n in range(6):
        tile = None
        for i in range(cx):
            for l in range(levels):
                picked = pl.ds(l * cx + i, sd, stride=tall)
                value = drops[attributes[n], picked, :] if n < 5 else perm[picked, :].astype(jnp.float32)
                spot = 4 * i + 2 * l
                moved = turn(value, spot + 1, 1)
                tile = moved if tile is None else jnp.where(lane >= spot, moved, tile)
        col_pack[n] = tile
    for d in range(2):
        col_pack[6, d : d + 1, d * ky : (d + 1) * ky] = ly[d : d + 1, :].astype(jnp.float32)
    for t, dy in enumerate(ys):
        send(col_pack, col_in.at[t], 2, (0, dy))

    def span(n, k):
        return pl.ds(n * slots_all + k * tall, tall)

    order = [perm[k * tall : (k + 1) * tall, :] for k in range(sd)]
    for m in range(sd):
        part = pl.ds(m * tall, tall)
        weight = drops[1, part, :]
        partner = jnp.zeros((tall, cy), jnp.int32)
        first = jnp.zeros((tall, cy), jnp.int32)
        for p in range(sd):
            mine = order[p] == m
            partner = jnp.where(mine, order[p ^ 1], partner)
            if p % 2 == 0:
                first = jnp.where(mine, 1, first)
        other = drops[1, pl.ds(0, tall), :]
        for k in range(1, sd):
            other = jnp.where(partner == k, drops[1, pl.ds(k * tall, tall), :], other)
        rate, eaten = match(weight, other, first > 0)
        for n in range(3):
            bits[n, part, :] = mod(lax.shift_right_logical(partner, jnp.int32(n)), 2)
        for n, value in enumerate(prepare(drops[0, part, :], drops[2, part, :])):
            ready[span(n, m), :] = value
        east, north = drops[3, part, :], drops[4, part, :]
        ready[span(6, m), :] = jnp.abs(east - 0.5)
        ready[span(7, m), :] = jnp.abs(north - 0.5)
        ready[span(8, m), :] = rate
        ready[span(9, m), :] = eaten
        wx, wy = kernel_weights(east), kernel_weights(north)
        for a in SHIFTS:
            along = wx[a] * weight
            for b in SHIFTS:
                share[3 * a + b + 4, part, :] = wy[b] * along

    mask[...] = jnp.ones_like(mask)
    for r, side in enumerate(edges):
        slots = list_pack[r]
        hot_row = iota((rows, kx), 0) == div(slots, block)
        hot_lane = jnp.where(iota((cy, kx), 0) == mod(slots, cy), 1.0, 0.0).astype(jnp.bfloat16)
        named = lax.dot_general(
            jnp.where(hot_row, 1.0, 0.0).astype(jnp.bfloat16), hot_lane,
            (((1,), (1,)), ((), ())), preferred_element_type=jnp.float32,
        )
        mask[pl.ds(side, rows, stride=cx), :] = 1.0 - named

    width = 2 * ky + 4 * kc
    lane_e = iota((1, width), 1)
    high = (lane_e < ky) | ((lane_e >= 2 * ky) & (lane_e < 2 * ky + 2 * kc))
    high_all = jnp.broadcast_to(high, (slots_all, width))
    slots = jnp.concatenate(
        [ly[0:1, :], ly[1:2, :], lc[0:1, :], lc[2:3, :], lc[1:2, :], lc[3:4, :]], 1
    )
    hot_e = jnp.where(iota((slots_all, width), 0) == div(slots, cy), 1.0, 0.0)
    left_high = jnp.max(jnp.where(high_all, hot_e, 0.0), 1, keepdims=True)
    left_low = jnp.max(jnp.where(high_all, 0.0, hot_e), 1, keepdims=True)
    lane_all = iota((slots_all, cy), 1)
    mask[...] = mask[...] * (
        1.0 - jnp.where(lane_all == cy - 1, left_high, jnp.where(lane_all == 0, left_low, 0.0))
    )

    def land(slots, move_x, move_y):
        level = mod(div(slots, block), levels)
        i = mod(mod(div(slots, cy), cx) + move_x, cx)
        target = (level * cx + i) * cy + mod(mod(slots, cy) + move_y, cy)
        return jnp.where(slots >= 0, target, -1)

    def blend(parts, pick_second):
        return parts[0] if len(parts) == 1 else jnp.where(pick_second, parts[1], parts[0])

    left_lanes = lane < cy // 2
    odd_lane = mod(lane, 2) == 1
    group = div(lane, 4)
    keys = [(a, b) for a in SHIFTS for b in SHIFTS]

    def climate(fields):
        deep_lane = iota(fields[0][0][0].shape, 1)
        odd = mod(deep_lane, 2) == 1

        def fixed(value, spot):
            return take(value, jnp.full(value.shape, spot, jnp.int32), 1)

        def reach(own, other, s):
            if s == 0:
                return own
            inside = deep_lane < cy - s if s > 0 else deep_lane >= -s
            return jnp.where(inside, turn(own, -s, 1), turn(other, -s, 1))

        def brink(own, other, s):
            if s == 0:
                return take(other, jnp.where(odd, 0, cy - 1), 1)
            if s > 0:
                return jnp.where(odd, fixed(other, s), fixed(own, s - 1))
            return jnp.where(odd, fixed(own, cy + s), fixed(other, cy - 1 + s))

        def humidity(cut):
            raw = [[{s: cut(*fields[f][l], s) for s in range(-2, 3)} for l in range(levels)] for f in range(2)]
            mixed = []
            for f in range(2):
                mixed.append([])
                for l in range(levels):
                    at_shift = {}
                    for b in SHIFTS:
                        centre = raw[f][l][b]
                        around = raw[f][l][b - 1] + raw[f][l][b + 1] + (turn(centre, -1, 0) + turn(centre, 1, 0))
                        stacked = raw[f][min(l + 1, levels - 1)][b] + raw[f][max(l - 1, 0)][b]
                        at_shift[b] = (
                            (1.0 - 4.0 * MIX_HORIZONTAL - 2.0 * MIX_VERTICAL) * centre
                            + MIX_HORIZONTAL * around + MIX_VERTICAL * stacked
                        )
                    mixed[f].append(at_shift)
            humid = []
            for l in range(levels):
                humid.append({})
                for b in SHIFTS:
                    warmth = mixed[1][l][b]
                    decay = jnp.exp2((-17.27 * LOG2E) * (warmth - 273.15) / (warmth - 35.86))
                    humid[l][b] = (GROWTH_STEP / EXCESS_FACTOR) * (mixed[0][l][b] * decay) - GROWTH_STEP
            return mixed, humid

        mixed, humid = humidity(reach)
        terms = [differences({(a, b): turn(humid[l][b], -a, 0) for a, b in keys}) for l in range(levels)]
        _, column = humidity(brink)
        wide_level = mod(div(deep_lane, 2), 2) == 1
        column = {b: jnp.where(wide_level, column[1][b], column[0][b]) for b in SHIFTS}
        return mixed, terms, column

    def from_row(value, a):
        return take(value, mod(group + a, cx), 0)

    def mate(weight, turns):
        rank = jnp.zeros((sd, cy), jnp.int32)
        for p in range(1, sd):
            rank = jnp.where(jnp.broadcast_to(turns[p : p + 1], (sd, cy)) == seat, p, rank)
        partner = take(turns, rank ^ 1, 0)
        return partner, match(weight, take(weight, partner, 0), mod(rank, 2) == 0)

    def expand(prepared, east, north, around):
        base, top, bottom, strength, lowest, cube = prepared
        level = base + interpolate(around, east, north, jnp.abs(east - 0.5), jnp.abs(north - 0.5))
        root, volume = settle(level, top, bottom, strength, lowest)
        return root, volume, volume - cube

    across_pair = seat ^ 1

    def pair(weight):
        return across_pair, match(weight, take(weight, across_pair, 0), mod(seat, 2) == 0)

    def merge(root, volume, weight, mated):
        partner, (rate, eaten) = mated
        after, lost = collide(root, volume, take(root, partner, 0), rate, eaten)
        return after, weight - lost

    def surround(ref, l, r):
        return {key: jnp.broadcast_to(ref[l, n, r : r + 1, :], (sd, cy)) for n, key in enumerate(keys)}

    def side_growth(s):
        ref, r = ((near, cx - 1), (near_up, 0))[s]
        found = []
        for l in range(levels):
            radius, dry, east, north = (row_x[s, n, pl.ds(l * sd, sd), :] for n in range(4))
            found.append(expand(prepare(radius, dry), east, north, surround(ref, l, r)))
        return found

    def side_rows(s, found):
        home = (0, cx - 1)[s]
        for l in range(levels):
            stretch = pl.ds(l * sd, sd)
            root, volume, gain = found[l]
            weight = row_x[s, 4, stretch, :]
            radius, weight_left = merge(root, volume, weight, pair(weight))
            late_x[s, 0, stretch, :] = radius
            late_x[s, 1, stretch, :] = weight_left
            wx, wy = kernel_weights(row_x[s, 2, stretch, :]), kernel_weights(row_x[s, 3, stretch, :])
            along = wx[MOVES[s]] * (weight * gain)
            for b in SHIFTS:
                fall[b + 1, l, home : home + 1, :] += jnp.sum(wy[b] * along, 0, keepdims=True)

    def side_records(s):
        slots = list_x[s].reshape(deep, cy)
        level = mod(div(slots, block), levels)
        live = slots >= 0
        row = level * sd + div(slots, block * levels)
        column = mod(slots, cy)
        fields = [(2, row_x, 1), (3, row_x, 2), (4, row_x, 3), (0, late_x, 0), (1, late_x, 1)]
        for n, source, from_n in fields:
            got = look_up(lambda r: source[s, from_n, r : r + 1, :], row, column)
            rec_out[n, :, pl.ds(s * kx, kx)] = jnp.where(live, got, 0.0).reshape(1, kx)
        box_out[:, pl.ds(s * kx, kx)] = land(slots, MOVES[s], 0).reshape(1, kx)

    pl.semaphore_wait(lower_in, len(beside))
    send_fields(1)
    send_first(1)
    send_rows(1)
    send_corner(1)

    wait_rows(due[0], recv_sem.at[0])
    fields = []
    for f in range(2):
        fields.append([])
        for l in range(levels):
            side_y = blend([state_y[t, f, l] for t in range(len(ys))], left_lanes)
            far = blend([diag_in[1, t, f, l] for t in range(len(ys))], left_lanes)
            fields[f].append(
                (jnp.concatenate([state[f, l], state_x[1, f, l]], 0), jnp.concatenate([side_y, far], 0))
            )
    mixed, terms, column = climate(fields)
    window = {key: jnp.concatenate([t[key][:cx] for t in terms], 0) for key in keys}
    for l in range(levels):
        for n, key in enumerate(keys):
            near_up[l, n] = terms[l][key][cx:]
        moist_out[l] = mixed[0][l][0][:cx]
        warm_out[l] = mixed[1][l][0][:cx]
    inside = {
        (a, b): jnp.where(
            mod(group + a, cy // 4) < cx, from_row(column[b][:cx], a), from_row(column[b][cx:], a)
        )
        for a, b in keys
    }

    grown = []
    cubes = []
    deposit = {}
    for k in range(sd):
        part = pl.ds(k * tall, tall)
        base, top, bottom, strength, lowest, cube, reach_x, reach_y = (ready[span(n, k), :] for n in range(8))
        level = base + interpolate(window, drops[3, part, :], drops[4, part, :], reach_x, reach_y)
        root, volume = settle(level, top, bottom, strength, lowest)
        gain = volume - cube
        for a, b in keys:
            term = share[3 * a + b + 4, part, :] * gain
            deposit[a, b] = term if k == 0 else deposit[a, b] + term
        grown.append(root)
        cubes.append(volume)

    for l in range(levels):
        for b in SHIFTS:
            parts = {a: jnp.where(line < 2, 0.0, deposit[a, b][l * cx : (l + 1) * cx]) for a in SHIFTS}
            fall[b + 1, l] = spread(parts, 0, line)

    for m in range(sd):
        part = pl.ds(m * tall, tall)
        found = grown
        for n in range(3):
            odd = bits[n, part, :] > 0
            found = [jnp.where(odd, found[2 * i + 1], found[2 * i]) for i in range(len(found) // 2)]
        radius, lost = collide(grown[m], cubes[m], found[0], ready[span(8, m), :], ready[span(9, m), :])
        size_out[part, :] = radius
        mult_out[part, :] = mask[part, :] * (drops[1, part, :] - lost)

    def upper_side():
        wait_rows(due[3], recv_sem.at[3])
        side_rows(1, side_growth(1))
        side_records(1)

    pl.when(me_x != nx - 1)(upper_side)

    redo = [(l, i) for l in range(levels) for i in range(2)]
    waiting = {}
    for l, i in redo:
        picked = pl.ds(l * cx + i, sd, stride=tall)
        radius, weight, dry, east, north = (drops[n, picked, :] for n in range(5))
        waiting[l, i] = (
            prepare(radius, dry), weight, east, north, mate(weight, perm[picked, :]), mask[picked, :]
        )

    wait_rows(due[1], recv_sem.at[1])
    fields = []
    for f in range(2):
        fields.append([])
        for l in range(levels):
            side_y = blend([state_y[t, f, l] for t in range(len(ys))], left_lanes)
            far = blend([diag_in[0, t, f, l] for t in range(len(ys))], left_lanes)
            fields[f].append(
                (jnp.where(low_half, state[f, l], state_x[0, f, l]), jnp.where(low_half, side_y, far))
            )
    mixed, terms, column = climate(fields)
    for l in range(levels):
        for n, key in enumerate(keys):
            near[l, n] = terms[l][key]
        moist_out[l, 0:1, :] = mixed[0][l][0][0:1]
        warm_out[l, 0:1, :] = mixed[1][l][0][0:1]
    col_terms = differences(
        {
            (a, b): jnp.where(mod(group + a + 2, cy // 4) < 4, from_row(column[b], a), inside[a, b])
            for a, b in keys
        }
    )
    for l in range(levels):
        landing = [None] * 3
        for i in range(2):
            picked = pl.ds(l * cx + i, sd, stride=tall)
            prepared, weight, east, north, mated, keep = waiting[l, i]
            root, volume, gain = expand(prepared, east, north, surround(near, l, i))
            radius, weight_left = merge(root, volume, weight, mated)
            size_out[picked, :] = radius
            mult_out[picked, :] = keep * weight_left
            wx, wy = kernel_weights(east), kernel_weights(north)
            for a in SHIFTS:
                if i + a < 0:
                    continue
                along = wx[a] * (weight * gain)
                parts = {b: wy[b] * along for b in SHIFTS}
                if landing[i + a] is not None:
                    parts = {b: parts[b] + landing[i + a][b] for b in SHIFTS}
                landing[i + a] = parts
        for r in range(3):
            for b in SHIFTS:
                fall[b + 1, l, r : r + 1, :] += jnp.sum(landing[r][b], 0, keepdims=True)

    pl.when(me_x == nx - 1)(upper_side)

    def columns():
        wait_rows(due[2], recv_sem.at[2])
        corner = [blend([corner_in[s, t] for t in range(len(ys))], odd_lane) for s in range(2)]
        values = []
        for n in range(6):
            beside = blend([col_in[t, n] for t in range(len(ys))], odd_lane)
            below = jnp.where(lane < 4 * cx, beside, turn(corner[1], 4 * (cx - 1) - 8 * n, 1))
            values.append(jnp.where(lane >= cy - 4, turn(corner[0], cy - 4 - 8 * n, 1), below))
        radius, dry, east, north, weight, turns = values
        root, volume, gain = expand(prepare(radius, dry), east, north, col_terms)
        radius, weight_left = merge(root, volume, weight, mate(weight, turns.astype(jnp.int32)))
        wx, wy = kernel_weights(east), kernel_weights(north)
        across = jnp.where(odd_lane, wy[-1], wy[1]) * (weight * gain)
        rain = {a: jnp.broadcast_to(jnp.sum(wx[a] * across, 0, keepdims=True), (cx, cy)) for a in SHIFTS}
        outer = jnp.where(lane == cy - 1, 1, 0)
        for l in range(levels):
            sent_in = sum(take(rain[a], mod(4 * (line - a) + 2 * l + outer, cy), 1) for a in SHIFTS)
            brink_fall[l] = jnp.where((lane == 0) | (lane == cy - 1), sent_in, 0.0)

        which = div(lane_e - 2 * ky, kc)
        minus_x = mod(which, 2)
        face = lane_e < 2 * ky
        minus_y = jnp.where(face, jnp.where(lane_e < ky, 0, 1), div(which, 2))
        slots = None
        for d in range(2):
            t = d if len(ys) == 2 else 0
            faces = col_in[t, 6, d : d + 1, :]
            corners = [corner_in[s, t, 2 * s + d : 2 * s + d + 1, :] for s in range(2)]
            found = jnp.where(face, faces, jnp.where(minus_x == 0, corners[0], corners[1]))
            slots = found if d == 0 else jnp.where(minus_y == 0, slots, found)
        slots = slots.astype(jnp.int32)
        move_x = jnp.where(face, 0, 1 - 2 * minus_x)
        live = slots >= 0
        level = mod(div(slots, block), levels)
        place = jnp.where(face, mod(div(slots, cy), cx), jnp.where(minus_x == 0, cy // 4 - 1, cx))
        spot = jnp.broadcast_to(jnp.where(live, 4 * place + 2 * level + minus_y, 0), (sd, width))
        chosen = iota((sd, width), 0) == jnp.where(live, div(slots, block * levels), -1)
        for n, value in enumerate((radius, weight_left, dry, east, north)):
            rec_out[n, :, pl.ds(2 * kx, width)] = jnp.sum(jnp.where(chosen, take(value, spot, 1), 0.0), 0, keepdims=True)
        box_out[:, pl.ds(2 * kx, width)] = land(slots, move_x, 1 - 2 * minus_y)

    def rows_below():
        wait_rows(due[4], recv_sem.at[4])
        side = side_growth(0)
        wait_rows(due[5], recv_sem.at[5])
        side_rows(0, side)
        wait_rows(due[6], recv_sem.at[6])
        side_records(0)

    def total_up():
        for l in range(levels):
            total = spread({b: fall[b + 1, l] for b in SHIFTS}, 1, lane) + brink_fall[l]
            moist_out[l] = moist_out[l] - VAPOUR_PER_SOURCE * total
            warm_out[l] = warm_out[l] + WARMING_FACTOR * total

    @pl.when(me_y == 0)
    def _():
        columns()
        rows_below()
        total_up()

    @pl.when(me_y != 0)
    def _():
        rows_below()
        columns()
        total_up()

    wait_rows(sent[0], send_sem.at[0])


def publish(*refs):
    whole, sem = refs[-2:]
    count = len(refs) // 2 - 1
    for n in range(count):
        pltpu.make_async_copy(refs[n], refs[count + n], sem).start()
    pltpu.make_async_copy(whole, whole, sem).wait()


def per_device(nx, ny, moist, warm, size, mult, dry, east, north, perm, lx, ly, lc):
    levels, cx, cy = moist.shape
    sd = size.shape[0]
    kx, ky, kc = lx.shape[2], ly.shape[2], lc.shape[2]
    narr = 2 * kx + 2 * ky + 4 * kc
    slots = sd * levels * cx
    flat = [x.reshape(slots, cy) for x in (size, mult, dry, east, north, perm)]
    f32, i32 = jnp.float32, jnp.int32
    any_space = pl.BlockSpec(memory_space=pl.ANY)
    vmem_space = pl.BlockSpec(memory_space=pltpu.VMEM)
    dma = pltpu.SemaphoreType.DMA
    shapes = (
        ((levels, cx, cy), f32),
        ((levels, cx, cy), f32),
        ((slots, cy), f32),
        ((slots, cy), f32),
        ((5, 1, narr), f32),
        ((1, narr), i32),
    )
    n_y = 1 if ny == 2 else 2
    total = 2 * levels * cx + 2 * slots + 6 * narr // cy
    outs = pl.pallas_call(
        functools.partial(body, (levels, cx, cy, sd, kx, ky, kc, nx, ny)),
        out_shape=tuple(pltpu.VMEM(*s) for s in shapes),
        in_specs=[any_space] * 17,
        out_specs=[vmem_space] * 6,
        scratch_shapes=[
            pltpu.VMEM((2, levels, cx, cy), f32),
            pltpu.VMEM((5, slots, cy), f32),
            pltpu.VMEM((slots, cy), i32),
            pltpu.VMEM((2, ky), i32),
            pltpu.VMEM((4, kc), i32),
            pltpu.VMEM((2, 2, levels, cx, cy), f32),
            pltpu.VMEM((n_y, 2, levels, cx, cy), f32),
            pltpu.VMEM((2, n_y, 2, levels, cx, cy), f32),
            pltpu.VMEM((2, 1, kx), i32),
            pltpu.VMEM((2, 1, kx), i32),
            pltpu.VMEM((2, 1, kx), i32),
            pltpu.VMEM((2, 5, sd * levels, cy), f32),
            pltpu.VMEM((2, 5, sd * levels, cy), f32),
            pltpu.VMEM((2, 5, sd * levels, cy), f32),
            pltpu.VMEM((2, sd * levels, cy), i32),
            pltpu.VMEM((2, sd * levels, cy), i32),
            pltpu.VMEM((2, sd, cy), f32),
            pltpu.VMEM((2, n_y, sd, cy), f32),
            pltpu.VMEM((7, sd, cy), f32),
            pltpu.VMEM((n_y, 7, sd, cy), f32),
            pltpu.VMEM((slots, cy), f32),
            pltpu.VMEM((10 * slots, cy), f32),
            pltpu.VMEM((9, slots, cy), f32),
            pltpu.VMEM((3, slots, cy), i32),
            pltpu.VMEM((levels, 9, cx, cy), f32),
            pltpu.VMEM((levels, 9, cx, cy), f32),
            pltpu.VMEM((2, 2, sd * levels, cy), f32),
            pltpu.VMEM((3, levels, cx, cy), f32),
            pltpu.VMEM((levels, cx, cy), f32),
            dma((5,)), dma((1,)), dma((7,)), pltpu.SemaphoreType.REGULAR,
        ],
        compiler_params=pltpu.CompilerParams(collective_id=0, has_side_effects=True),
    )(moist, warm, *flat, size, mult, dry, east, north, perm, lx, ly, lc)
    outs = pl.pallas_call(
        publish,
        out_shape=tuple(jax.ShapeDtypeStruct(*s) for s in shapes),
        in_specs=[vmem_space] * 6,
        out_specs=[any_space] * 6,
        scratch_shapes=[pltpu.VMEM((total, cy), f32), dma],
    )(*[pltpu.with_memory_space_constraint(x, pltpu.VMEM) for x in outs])
    return (
        outs[0], outs[1], outs[2].reshape(size.shape), outs[3].reshape(size.shape), outs[4], outs[5],
    )


def solution(mesh):
    cell, drop, lists = P(None, "gx", "gy"), P(None, None, "gx", "gy"), P("gx", None, "gy")
    return jax.shard_map(
        functools.partial(per_device, mesh.shape["gx"], mesh.shape["gy"]),
        mesh=mesh,
        in_specs=(cell,) * 2 + (drop,) * 6 + (lists,) * 3,
        out_specs=(cell, cell, drop, drop, cell, P("gx", "gy")),
        check_vma=False,
    )
```

```python
import functools
import math

import jax
import jax.numpy as jnp
from jax import lax
from jax.experimental import pallas as pl
from jax.experimental.pallas import tpu as pltpu
from jax.sharding import PartitionSpec as P

NEWTON = 4
MIX_HORIZONTAL = 0.2
MIX_VERTICAL = 0.05
EXCESS_FACTOR = 4.2222
CURVATURE = 0.0012
KAPPA_SOLUTE = 0.6
GROWTH_STEP = 200.0
COLLIDE_RATE = 4e-07
VAPOUR_PER_SOURCE = 0.001
WARMING_FACTOR = 0.00249
LOG2E = math.log2(math.e)

MESH = pl.DeviceIdType.MESH
SHIFTS = (-1, 0, 1)
SIDES = (1, -1)
MOVES = (1, -1)


def div(x, n):
    return lax.shift_right_arithmetic(x, jnp.int32(n.bit_length() - 1))


def mod(x, n):
    return lax.bitwise_and(x, jnp.int32(n - 1))


def iota(shape, dim):
    return lax.broadcasted_iota(jnp.int32, shape, dim)


def turn(x, shift, dim):
    shift %= x.shape[dim]
    return pltpu.roll(x, shift, dim) if shift else x


def take(x, index, dim):
    return jnp.take_along_axis(x, index, axis=dim)


def kernel_weights(offset):
    return {
        -1: jnp.maximum(0.5 - offset, 0.0),
        0: 1.0 - jnp.abs(offset - 0.5),
        1: jnp.maximum(offset - 0.5, 0.0),
    }


def prepare(radius, dry):
    inverse = 1.0 / radius
    square = inverse * inverse
    lowest = dry * dry
    strength = (1.5 * GROWTH_STEP * KAPPA_SOLUTE) * (lowest * dry)
    pull = strength * (square * inverse)
    area = radius * radius
    return (
        area - (GROWTH_STEP * CURVATURE) * inverse,
        (5.0 / 3.0) * pull,
        1.0 + pull * square,
        strength,
        lowest,
        area * radius,
    )


def settle(level, top, bottom, strength, lowest):
    above = jnp.maximum(level + top, lowest * bottom)
    flat = lax.rsqrt(above * bottom)
    for sweep in range(NEWTON - 1):
        inverse_root = bottom * flat
        square = inverse_root * inverse_root
        pull = strength * (square * inverse_root)
        bottom = 1.0 + pull * square
        above = jnp.maximum(level + (5.0 / 3.0) * pull, lowest * bottom)
        flat = lax.rsqrt(above * bottom)
    root = above * flat
    return root, (root * root) * root


def differences(near):
    centre = near[0, 0]
    terms = {(0, 0): centre}
    for s in SIDES:
        terms[s, 0] = near[s, 0] - centre
        terms[0, s] = near[0, s] - centre
    for a in SIDES:
        for b in SIDES:
            terms[a, b] = near[a, b] - near[a, 0] - terms[0, b]
    return terms


def interpolate(terms, east, north, reach_x, reach_y):
    right, up = east > 0.5, north > 0.5
    slope_x = jnp.where(right, terms[1, 0], terms[-1, 0])
    slope_y = jnp.where(up, terms[0, 1], terms[0, -1])
    twist = jnp.where(
        right, jnp.where(up, terms[1, 1], terms[1, -1]), jnp.where(up, terms[-1, 1], terms[-1, -1])
    )
    return terms[0, 0] + reach_x * slope_x + reach_y * (slope_y + reach_x * twist)


def match(weight, other, first):
    big = (weight > other) | ((weight == other) & first)
    rate = (-COLLIDE_RATE * LOG2E) * jnp.where(big, weight, other)
    return rate, jnp.where(big, other, 0.0)


def collide(radius, cube, other, rate, eaten):
    total = radius + other
    chance = 1.0 - jnp.exp2(rate * (total * total) * (total * jnp.abs(radius - other)))
    volume = cube + chance * (other * other * other)
    merged = jnp.exp2(jnp.log(volume) * (LOG2E / 3.0))
    return jnp.where(eaten > 0.0, radius, merged), chance * eaten


def spread(parts, dim, index):
    size = parts[0].shape[dim]
    back, ahead = turn(parts[-1], -1, dim), turn(parts[1], 1, dim)
    return parts[0] + jnp.where(index == size - 1, 0.0, back) + jnp.where(index == 0, 0.0, ahead)


def body(
    sizes,
    moist_in, warm_in, size_in, mult_in, dry_in, east_in, north_in, perm_in,
    size_cells, mult_cells, dry_cells, east_cells, north_cells, perm_cells,
    lx_in, ly_in, lc_in,
    moist_out, warm_out, size_out, mult_out, rec_out, box_out,
    state, drops, perm, ly, lc,
    state_x, state_y, diag_in, list_pack, list_sort, list_x,
    row_pack, row_sort, row_x, turn_pack, rank_of, corner_pack, corner_in, col_pack, col_in,
    mask, ready, share, bits, near, near_up, late_x, fall, brink_fall,
    in_sem, send_sem, recv_sem, lower_in,
):
    levels, cx, cy, sd, kx, ky, kc, nx, ny = sizes
    me_x = lax.axis_index("gx")
    me_y = lax.axis_index("gy")
    ys = (1,) if ny == 2 else (1, -1)
    half = cx // 2
    rows = sd * levels
    slots_all = rows * cx
    block = cx * cy
    tall = levels * cx
    deep = kx // cy
    edges = (cx - 1, 0)
    bands = (pl.ds(cx - 3, 3), pl.ds(0, 3))

    def at(d):
        return (lax.rem(me_x + d[0] + nx, nx), lax.rem(me_y + d[1] + ny, ny))

    def wait_rows(count, sem):
        whole = ready.at[pl.ds(0, count), :]
        pltpu.make_async_copy(whole, whole, sem).wait()

    def count_rows(ref):
        total = 1
        for n in ref.shape:
            total *= n
        return total // cy

    brought = [0, 0, 0]

    def bring(source, target, group):
        pltpu.make_async_copy(source, target, in_sem.at[group]).start()
        brought[group] += count_rows(target)

    cells = (size_cells, dry_cells, east_cells, north_cells, mult_cells)

    def bring_rows(s, chosen, group):
        for n in chosen:
            source = cells[n] if n < 5 else perm_cells
            bring(source.at[:, :, edges[s], :], row_pack.at[s, n] if n < 5 else turn_pack.at[s], group)

    bring_rows(0, (5, 0, 1), 1)
    bring_rows(0, (2, 3, 4), 2)
    bring(lx_in.at[0, pl.ds(0, 1), :], list_pack.at[0], 2)
    bring(moist_in, state.at[0], 0)
    bring(warm_in, state.at[1], 0)

    beside = [0] + list(ys)
    barrier = pltpu.get_barrier_semaphore()
    for d in [(-1, dy) for dy in beside] + [(0, dy) for dy in ys]:
        pl.semaphore_signal(barrier, inc=1, device_id=at(d), device_id_type=MESH)

    bring_rows(1, range(6), 0)
    bring(lx_in.at[0, pl.ds(1, 1), :], list_pack.at[1], 0)
    lists = [
        pltpu.make_async_copy(source.at[0], target, in_sem.at[3 + n])
        for n, (source, target) in enumerate(((ly_in, ly), (lc_in, lc)))
    ]
    for copy in lists:
        copy.start()
    for n, source in enumerate((size_in, mult_in, dry_in, east_in, north_in)):
        bring(source, drops.at[n], 0)
    bring(perm_in, perm, 0)

    sent = [0]
    due = [0] * 7

    def send(source, target, group, d):
        pltpu.make_async_remote_copy(
            src_ref=source, dst_ref=target, send_sem=send_sem.at[0], recv_sem=recv_sem.at[group],
            device_id=at(d), device_id_type=MESH,
        ).start()
        sent[0] += count_rows(source)
        due[group] += count_rows(source)

    line = iota((cx, cy), 0)
    lane = iota((cx, cy), 1)
    low_half = line < half

    def send_fields(s):
        own, far = state.at[:, :, bands[s], :], MOVES[s]
        group = (1, 0)[s]
        send(own, state_x.at[s, :, :, bands[s], :], group, (far, 0))
        for t, dy in enumerate(ys):
            send(own, diag_in.at[s, t, :, :, bands[s], :], group, (far, dy))

    seat = iota((sd, cy), 0)

    def look_up(load_row, row, column):
        groups = 2
        found = [None] * groups
        for m in range(rows // groups):
            for n in range(groups):
                r = n * (rows // groups) + m
                value = take(jnp.broadcast_to(load_row(r), (deep, cy)), column, 1)
                found[n] = value if m == 0 else jnp.where(row == r, value, found[n])
        while len(found) > 1:
            size = rows // len(found)
            odd = mod(div(row, size), 2) == 1
            found = [jnp.where(odd, found[2 * m + 1], found[2 * m]) for m in range(len(found) // 2)]
        return found[0]

    def sort_rows(s, chosen):
        for l in range(levels):
            stretch = pl.ds(l * sd, sd)
            turns = turn_pack[s, :, l, :]
            for n in chosen:
                row_sort[s, n, stretch, :] = take(row_pack[s, n, :, l, :], turns, 0)

    def send_first(s):
        sort_rows(s, (0, 1))
        send(row_sort.at[s, 0:2], row_x.at[s, 0:2], (4, 3)[s], (MOVES[s], 0))

    def send_rows(s):
        sort_rows(s, (2, 3, 4))
        send(row_sort.at[s, 2:4], row_x.at[s, 2:4], (4, 3)[s], (MOVES[s], 0))

    def send_rest(s):
        send(row_sort.at[s, 4], row_x.at[s, 4], (5, 3)[s], (MOVES[s], 0))
        for l in range(levels):
            rank = jnp.zeros((sd, cy), jnp.int32)
            for p in range(1, sd):
                here = jnp.broadcast_to(turn_pack[s, p : p + 1, l, :], (sd, cy)) == seat
                rank = jnp.where(here, p, rank)
            rank_of[s, pl.ds(l * sd, sd), :] = rank
        slots = list_pack[s].reshape(deep, cy)
        k = div(slots, block * levels)
        row = mod(div(slots, block), levels) * sd + k
        place = look_up(lambda r: rank_of[s, r : r + 1, :], row, mod(slots, cy))
        moved = jnp.where(slots >= 0, slots + (place - k) * (block * levels), -1)
        list_sort[s] = moved.reshape(1, kx)
        send(list_sort.at[s], list_x.at[s], (6, 3)[s], (MOVES[s], 0))

    def send_corner(s):
        tile = None
        for n in range(6):
            for l in range(levels):
                value = row_pack[s, n, :, l, :] if n < 5 else turn_pack[s, :, l, :].astype(jnp.float32)
                spot = 8 * n + 4 * s + 2 * l
                moved = turn(value, spot + 1, 1)
                tile = moved if tile is None else jnp.where(lane >= spot, moved, tile)
        corner_pack[s] = tile
        for d in range(2):
            spot = 2 * ky + kc * (2 * d + s)
            corner_pack[s, 2 * s + d : 2 * s + d + 1, spot : spot + kc] = lc[
                2 * s + d : 2 * s + d + 1, :
            ].astype(jnp.float32)
        for t, dy in enumerate(ys):
            send(corner_pack.at[s], corner_in.at[s, t], 2, (MOVES[s], dy))

    pl.semaphore_wait(barrier, len(beside) + len(ys))
    for dy in beside:
        for f, source in enumerate((moist_in, warm_in)):
            target = state_x.at[0] if dy == 0 else diag_in.at[0, ys.index(dy)]
            send(source.at[:, bands[0], :], target.at[f, :, bands[0], :], 1, (1, dy))
    for dy in beside:
        pl.semaphore_signal(lower_in, inc=1, device_id=at((1, dy)), device_id_type=MESH)
    wait_rows(brought[1], in_sem.at[1])
    send_first(0)
    wait_rows(brought[2], in_sem.at[2])
    send_rows(0)
    before = sent[0], list(due)

    @pl.when(me_y == 0)
    def _():
        send_rest(0)
        for copy in lists:
            copy.wait()
        send_corner(0)

    sent[0], due[:] = before

    @pl.when(me_y != 0)
    def _():
        for copy in lists:
            copy.wait()
        send_corner(0)
        send_rest(0)

    wait_rows(brought[0], in_sem.at[0])
    for t, dy in enumerate(ys):
        send(state, state_y.at[t], 0, (0, dy))
    attributes = (0, 2, 3, 4, 1)
    for n in range(6):
        tile = None
        for i in range(cx):
            for l in range(levels):
                picked = pl.ds(l * cx + i, sd, stride=tall)
                value = drops[attributes[n], picked, :] if n < 5 else perm[picked, :].astype(jnp.float32)
                spot = 4 * i + 2 * l
                moved = turn(value, spot + 1, 1)
                tile = moved if tile is None else jnp.where(lane >= spot, moved, tile)
        col_pack[n] = tile
    for d in range(2):
        col_pack[6, d : d + 1, d * ky : (d + 1) * ky] = ly[d : d + 1, :].astype(jnp.float32)
    for t, dy in enumerate(ys):
        send(col_pack, col_in.at[t], 2, (0, dy))

    def span(n, k):
        return pl.ds(n * slots_all + k * tall, tall)

    order = [perm[k * tall : (k + 1) * tall, :] for k in range(sd)]
    for m in range(sd):
        part = pl.ds(m * tall, tall)
        weight = drops[1, part, :]
        partner = jnp.zeros((tall, cy), jnp.int32)
        first = jnp.zeros((tall, cy), jnp.int32)
        for p in range(sd):
            mine = order[p] == m
            partner = jnp.where(mine, order[p ^ 1], partner)
            if p % 2 == 0:
                first = jnp.where(mine, 1, first)
        other = drops[1, pl.ds(0, tall), :]
        for k in range(1, sd):
            other = jnp.where(partner == k, drops[1, pl.ds(k * tall, tall), :], other)
        rate, eaten = match(weight, other, first > 0)
        for n in range(3):
            bits[n, part, :] = mod(lax.shift_right_logical(partner, jnp.int32(n)), 2)
        for n, value in enumerate(prepare(drops[0, part, :], drops[2, part, :])):
            ready[span(n, m), :] = value
        east, north = drops[3, part, :], drops[4, part, :]
        ready[span(6, m), :] = jnp.abs(east - 0.5)
        ready[span(7, m), :] = jnp.abs(north - 0.5)
        ready[span(8, m), :] = rate
        ready[span(9, m), :] = eaten
        wx, wy = kernel_weights(east), kernel_weights(north)
        for a in SHIFTS:
            along = wx[a] * weight
            for b in SHIFTS:
                share[3 * a + b + 4, part, :] = wy[b] * along

    mask[...] = jnp.ones_like(mask)
    for r, side in enumerate(edges):
        slots = list_pack[r]
        hot_row = iota((rows, kx), 0) == div(slots, block)
        hot_lane = jnp.where(iota((cy, kx), 0) == mod(slots, cy), 1.0, 0.0).astype(jnp.bfloat16)
        named = lax.dot_general(
            jnp.where(hot_row, 1.0, 0.0).astype(jnp.bfloat16), hot_lane,
            (((1,), (1,)), ((), ())), preferred_element_type=jnp.float32,
        )
        mask[pl.ds(side, rows, stride=cx), :] = 1.0 - named

    width = 2 * ky + 4 * kc
    lane_e = iota((1, width), 1)
    high = (lane_e < ky) | ((lane_e >= 2 * ky) & (lane_e < 2 * ky + 2 * kc))
    high_all = jnp.broadcast_to(high, (slots_all, width))
    slots = jnp.concatenate(
        [ly[0:1, :], ly[1:2, :], lc[0:1, :], lc[2:3, :], lc[1:2, :], lc[3:4, :]], 1
    )
    hot_e = jnp.where(iota((slots_all, width), 0) == div(slots, cy), 1.0, 0.0)
    left_high = jnp.max(jnp.where(high_all, hot_e, 0.0), 1, keepdims=True)
    left_low = jnp.max(jnp.where(high_all, 0.0, hot_e), 1, keepdims=True)
    lane_all = iota((slots_all, cy), 1)
    mask[...] = mask[...] * (
        1.0 - jnp.where(lane_all == cy - 1, left_high, jnp.where(lane_all == 0, left_low, 0.0))
    )

    def land(slots, move_x, move_y):
        level = mod(div(slots, block), levels)
        i = mod(mod(div(slots, cy), cx) + move_x, cx)
        target = (level * cx + i) * cy + mod(mod(slots, cy) + move_y, cy)
        return jnp.where(slots >= 0, target, -1)

    def blend(parts, pick_second):
        return parts[0] if len(parts) == 1 else jnp.where(pick_second, parts[1], parts[0])

    left_lanes = lane < cy // 2
    odd_lane = mod(lane, 2) == 1
    group = div(lane, 4)
    keys = [(a, b) for a in SHIFTS for b in SHIFTS]

    def climate(fields):
        deep_lane = iota(fields[0][0][0].shape, 1)
        odd = mod(deep_lane, 2) == 1

        def fixed(value, spot):
            return take(value, jnp.full(value.shape, spot, jnp.int32), 1)

        def reach(own, other, s):
            if s == 0:
                return own
            inside = deep_lane < cy - s if s > 0 else deep_lane >= -s
            return jnp.where(inside, turn(own, -s, 1), turn(other, -s, 1))

        def brink(own, other, s):
            if s == 0:
                return take(other, jnp.where(odd, 0, cy - 1), 1)
            if s > 0:
                return jnp.where(odd, fixed(other, s), fixed(own, s - 1))
            return jnp.where(odd, fixed(own, cy + s), fixed(other, cy - 1 + s))

        def humidity(cut):
            raw = [[{s: cut(*fields[f][l], s) for s in range(-2, 3)} for l in range(levels)] for f in range(2)]
            mixed = []
            for f in range(2):
                mixed.append([])
                for l in range(levels):
                    at_shift = {}
                    for b in SHIFTS:
                        centre = raw[f][l][b]
                        around = raw[f][l][b - 1] + raw[f][l][b + 1] + (turn(centre, -1, 0) + turn(centre, 1, 0))
                        stacked = raw[f][min(l + 1, levels - 1)][b] + raw[f][max(l - 1, 0)][b]
                        at_shift[b] = (
                            (1.0 - 4.0 * MIX_HORIZONTAL - 2.0 * MIX_VERTICAL) * centre
                            + MIX_HORIZONTAL * around + MIX_VERTICAL * stacked
                        )
                    mixed[f].append(at_shift)
            humid = []
            for l in range(levels):
                humid.append({})
                for b in SHIFTS:
                    warmth = mixed[1][l][b]
                    decay = jnp.exp2((-17.27 * LOG2E) * (warmth - 273.15) / (warmth - 35.86))
                    humid[l][b] = (GROWTH_STEP / EXCESS_FACTOR) * (mixed[0][l][b] * decay) - GROWTH_STEP
            return mixed, humid

        mixed, humid = humidity(reach)
        terms = [differences({(a, b): turn(humid[l][b], -a, 0) for a, b in keys}) for l in range(levels)]
        _, column = humidity(brink)
        wide_level = mod(div(deep_lane, 2), 2) == 1
        column = {b: jnp.where(wide_level, column[1][b], column[0][b]) for b in SHIFTS}
        return mixed, terms, column

    def from_row(value, a):
        return take(value, mod(group + a, cx), 0)

    def mate(weight, turns):
        rank = jnp.zeros((sd, cy), jnp.int32)
        for p in range(1, sd):
            rank = jnp.where(jnp.broadcast_to(turns[p : p + 1], (sd, cy)) == seat, p, rank)
        partner = take(turns, rank ^ 1, 0)
        return partner, match(weight, take(weight, partner, 0), mod(rank, 2) == 0)

    def expand(prepared, east, north, around):
        base, top, bottom, strength, lowest, cube = prepared
        level = base + interpolate(around, east, north, jnp.abs(east - 0.5), jnp.abs(north - 0.5))
        root, volume = settle(level, top, bottom, strength, lowest)
        return root, volume, volume - cube

    across_pair = seat ^ 1

    def pair(weight):
        return across_pair, match(weight, take(weight, across_pair, 0), mod(seat, 2) == 0)

    def merge(root, volume, weight, mated):
        partner, (rate, eaten) = mated
        after, lost = collide(root, volume, take(root, partner, 0), rate, eaten)
        return after, weight - lost

    def surround(ref, l, r):
        return {key: jnp.broadcast_to(ref[l, n, r : r + 1, :], (sd, cy)) for n, key in enumerate(keys)}

    def side_growth(s):
        ref, r = ((near, cx - 1), (near_up, 0))[s]
        found = []
        for l in range(levels):
            radius, dry, east, north = (row_x[s, n, pl.ds(l * sd, sd), :] for n in range(4))
            found.append(expand(prepare(radius, dry), east, north, surround(ref, l, r)))
        return found

    def side_rows(s, found):
        home = (0, cx - 1)[s]
        for l in range(levels):
            stretch = pl.ds(l * sd, sd)
            root, volume, gain = found[l]
            weight = row_x[s, 4, stretch, :]
            radius, weight_left = merge(root, volume, weight, pair(weight))
            late_x[s, 0, stretch, :] = radius
            late_x[s, 1, stretch, :] = weight_left
            wx, wy = kernel_weights(row_x[s, 2, stretch, :]), kernel_weights(row_x[s, 3, stretch, :])
            along = wx[MOVES[s]] * (weight * gain)
            for b in SHIFTS:
                fall[b + 1, l, home : home + 1, :] += jnp.sum(wy[b] * along, 0, keepdims=True)

    def side_records(s):
        slots = list_x[s].reshape(deep, cy)
        level = mod(div(slots, block), levels)
        live = slots >= 0
        row = level * sd + div(slots, block * levels)
        column = mod(slots, cy)
        fields = [(2, row_x, 1), (3, row_x, 2), (4, row_x, 3), (0, late_x, 0), (1, late_x, 1)]
        for n, source, from_n in fields:
            got = look_up(lambda r: source[s, from_n, r : r + 1, :], row, column)
            rec_out[n, :, pl.ds(s * kx, kx)] = jnp.where(live, got, 0.0).reshape(1, kx)
        box_out[:, pl.ds(s * kx, kx)] = land(slots, MOVES[s], 0).reshape(1, kx)

    pl.semaphore_wait(lower_in, len(beside))
    send_fields(1)
    send_first(1)
    send_rows(1)
    send_rest(1)
    send_corner(1)

    wait_rows(due[0], recv_sem.at[0])
    fields = []
    for f in range(2):
        fields.append([])
        for l in range(levels):
            side_y = blend([state_y[t, f, l] for t in range(len(ys))], left_lanes)
            far = blend([diag_in[1, t, f, l] for t in range(len(ys))], left_lanes)
            fields[f].append(
                (jnp.concatenate([state[f, l], state_x[1, f, l]], 0), jnp.concatenate([side_y, far], 0))
            )
    mixed, terms, column = climate(fields)
    window = {key: jnp.concatenate([t[key][:cx] for t in terms], 0) for key in keys}
    for l in range(levels):
        for n, key in enumerate(keys):
            near_up[l, n] = terms[l][key][cx:]
        moist_out[l] = mixed[0][l][0][:cx]
        warm_out[l] = mixed[1][l][0][:cx]
    inside = {
        (a, b): jnp.where(
            mod(group + a, cy // 4) < cx, from_row(column[b][:cx], a), from_row(column[b][cx:], a)
        )
        for a, b in keys
    }

    grown = []
    cubes = []
    deposit = {}
    for k in range(sd):
        part = pl.ds(k * tall, tall)
        base, top, bottom, strength, lowest, cube, reach_x, reach_y = (ready[span(n, k), :] for n in range(8))
        level = base + interpolate(window, drops[3, part, :], drops[4, part, :], reach_x, reach_y)
        root, volume = settle(level, top, bottom, strength, lowest)
        gain = volume - cube
        for a, b in keys:
            term = share[3 * a + b + 4, part, :] * gain
            deposit[a, b] = term if k == 0 else deposit[a, b] + term
        grown.append(root)
        cubes.append(volume)

    for l in range(levels):
        for b in SHIFTS:
            parts = {a: jnp.where(line < 2, 0.0, deposit[a, b][l * cx : (l + 1) * cx]) for a in SHIFTS}
            fall[b + 1, l] = spread(parts, 0, line)

    for m in range(sd):
        part = pl.ds(m * tall, tall)
        found = grown
        for n in range(3):
            odd = bits[n, part, :] > 0
            found = [jnp.where(odd, found[2 * i + 1], found[2 * i]) for i in range(len(found) // 2)]
        radius, lost = collide(grown[m], cubes[m], found[0], ready[span(8, m), :], ready[span(9, m), :])
        size_out[part, :] = radius
        mult_out[part, :] = mask[part, :] * (drops[1, part, :] - lost)

    def upper_side():
        wait_rows(due[3], recv_sem.at[3])
        side_rows(1, side_growth(1))
        side_records(1)

    pl.when(me_x != nx - 1)(upper_side)

    redo = [(l, i) for l in range(levels) for i in range(2)]
    waiting = {}
    for l, i in redo:
        picked = pl.ds(l * cx + i, sd, stride=tall)
        radius, weight, dry, east, north = (drops[n, picked, :] for n in range(5))
        waiting[l, i] = (
            prepare(radius, dry), weight, east, north, mate(weight, perm[picked, :]), mask[picked, :]
        )

    wait_rows(due[1], recv_sem.at[1])
    fields = []
    for f in range(2):
        fields.append([])
        for l in range(levels):
            side_y = blend([state_y[t, f, l] for t in range(len(ys))], left_lanes)
            far = blend([diag_in[0, t, f, l] for t in range(len(ys))], left_lanes)
            fields[f].append(
                (jnp.where(low_half, state[f, l], state_x[0, f, l]), jnp.where(low_half, side_y, far))
            )
    mixed, terms, column = climate(fields)
    for l in range(levels):
        for n, key in enumerate(keys):
            near[l, n] = terms[l][key]
        moist_out[l, 0:1, :] = mixed[0][l][0][0:1]
        warm_out[l, 0:1, :] = mixed[1][l][0][0:1]
    col_terms = differences(
        {
            (a, b): jnp.where(mod(group + a + 2, cy // 4) < 4, from_row(column[b], a), inside[a, b])
            for a, b in keys
        }
    )
    for l in range(levels):
        landing = [None] * 3
        for i in range(2):
            picked = pl.ds(l * cx + i, sd, stride=tall)
            prepared, weight, east, north, mated, keep = waiting[l, i]
            root, volume, gain = expand(prepared, east, north, surround(near, l, i))
            radius, weight_left = merge(root, volume, weight, mated)
            size_out[picked, :] = radius
            mult_out[picked, :] = keep * weight_left
            wx, wy = kernel_weights(east), kernel_weights(north)
            for a in SHIFTS:
                if i + a < 0:
                    continue
                along = wx[a] * (weight * gain)
                parts = {b: wy[b] * along for b in SHIFTS}
                if landing[i + a] is not None:
                    parts = {b: parts[b] + landing[i + a][b] for b in SHIFTS}
                landing[i + a] = parts
        for r in range(3):
            for b in SHIFTS:
                fall[b + 1, l, r : r + 1, :] += jnp.sum(landing[r][b], 0, keepdims=True)

    pl.when(me_x == nx - 1)(upper_side)

    def columns():
        wait_rows(due[2], recv_sem.at[2])
        corner = [blend([corner_in[s, t] for t in range(len(ys))], odd_lane) for s in range(2)]
        values = []
        for n in range(6):
            beside = blend([col_in[t, n] for t in range(len(ys))], odd_lane)
            below = jnp.where(lane < 4 * cx, beside, turn(corner[1], 4 * (cx - 1) - 8 * n, 1))
            values.append(jnp.where(lane >= cy - 4, turn(corner[0], cy - 4 - 8 * n, 1), below))
        radius, dry, east, north, weight, turns = values
        root, volume, gain = expand(prepare(radius, dry), east, north, col_terms)
        radius, weight_left = merge(root, volume, weight, mate(weight, turns.astype(jnp.int32)))
        wx, wy = kernel_weights(east), kernel_weights(north)
        across = jnp.where(odd_lane, wy[-1], wy[1]) * (weight * gain)
        rain = {a: jnp.broadcast_to(jnp.sum(wx[a] * across, 0, keepdims=True), (cx, cy)) for a in SHIFTS}
        outer = jnp.where(lane == cy - 1, 1, 0)
        for l in range(levels):
            sent_in = sum(take(rain[a], mod(4 * (line - a) + 2 * l + outer, cy), 1) for a in SHIFTS)
            brink_fall[l] = jnp.where((lane == 0) | (lane == cy - 1), sent_in, 0.0)

        which = div(lane_e - 2 * ky, kc)
        minus_x = mod(which, 2)
        face = lane_e < 2 * ky
        minus_y = jnp.where(face, jnp.where(lane_e < ky, 0, 1), div(which, 2))
        slots = None
        for d in range(2):
            t = d if len(ys) == 2 else 0
            faces = col_in[t, 6, d : d + 1, :]
            corners = [corner_in[s, t, 2 * s + d : 2 * s + d + 1, :] for s in range(2)]
            found = jnp.where(face, faces, jnp.where(minus_x == 0, corners[0], corners[1]))
            slots = found if d == 0 else jnp.where(minus_y == 0, slots, found)
        slots = slots.astype(jnp.int32)
        move_x = jnp.where(face, 0, 1 - 2 * minus_x)
        live = slots >= 0
        level = mod(div(slots, block), levels)
        place = jnp.where(face, mod(div(slots, cy), cx), jnp.where(minus_x == 0, cy // 4 - 1, cx))
        spot = jnp.broadcast_to(jnp.where(live, 4 * place + 2 * level + minus_y, 0), (sd, width))
        chosen = iota((sd, width), 0) == jnp.where(live, div(slots, block * levels), -1)
        for n, value in enumerate((radius, weight_left, dry, east, north)):
            rec_out[n, :, pl.ds(2 * kx, width)] = jnp.sum(jnp.where(chosen, take(value, spot, 1), 0.0), 0, keepdims=True)
        box_out[:, pl.ds(2 * kx, width)] = land(slots, move_x, 1 - 2 * minus_y)

    def rows_below():
        wait_rows(due[4], recv_sem.at[4])
        side = side_growth(0)
        wait_rows(due[5], recv_sem.at[5])
        side_rows(0, side)
        wait_rows(due[6], recv_sem.at[6])
        side_records(0)

    def total_up():
        for l in range(levels):
            total = spread({b: fall[b + 1, l] for b in SHIFTS}, 1, lane) + brink_fall[l]
            moist_out[l] = moist_out[l] - VAPOUR_PER_SOURCE * total
            warm_out[l] = warm_out[l] + WARMING_FACTOR * total

    @pl.when(me_y == 0)
    def _():
        columns()
        rows_below()
        total_up()

    @pl.when(me_y != 0)
    def _():
        rows_below()
        columns()
        total_up()

    wait_rows(sent[0], send_sem.at[0])


def publish(*refs):
    whole, sem = refs[-2:]
    count = len(refs) // 2 - 1
    for n in range(count):
        pltpu.make_async_copy(refs[n], refs[count + n], sem).start()
    pltpu.make_async_copy(whole, whole, sem).wait()


def per_device(nx, ny, moist, warm, size, mult, dry, east, north, perm, lx, ly, lc):
    levels, cx, cy = moist.shape
    sd = size.shape[0]
    kx, ky, kc = lx.shape[2], ly.shape[2], lc.shape[2]
    narr = 2 * kx + 2 * ky + 4 * kc
    slots = sd * levels * cx
    flat = [x.reshape(slots, cy) for x in (size, mult, dry, east, north, perm)]
    f32, i32 = jnp.float32, jnp.int32
    any_space = pl.BlockSpec(memory_space=pl.ANY)
    vmem_space = pl.BlockSpec(memory_space=pltpu.VMEM)
    dma = pltpu.SemaphoreType.DMA
    shapes = (
        ((levels, cx, cy), f32),
        ((levels, cx, cy), f32),
        ((slots, cy), f32),
        ((slots, cy), f32),
        ((5, 1, narr), f32),
        ((1, narr), i32),
    )
    n_y = 1 if ny == 2 else 2
    total = 2 * levels * cx + 2 * slots + 6 * narr // cy
    outs = pl.pallas_call(
        functools.partial(body, (levels, cx, cy, sd, kx, ky, kc, nx, ny)),
        out_shape=tuple(pltpu.VMEM(*s) for s in shapes),
        in_specs=[any_space] * 17,
        out_specs=[vmem_space] * 6,
        scratch_shapes=[
            pltpu.VMEM((2, levels, cx, cy), f32),
            pltpu.VMEM((5, slots, cy), f32),
            pltpu.VMEM((slots, cy), i32),
            pltpu.VMEM((2, ky), i32),
            pltpu.VMEM((4, kc), i32),
            pltpu.VMEM((2, 2, levels, cx, cy), f32),
            pltpu.VMEM((n_y, 2, levels, cx, cy), f32),
            pltpu.VMEM((2, n_y, 2, levels, cx, cy), f32),
            pltpu.VMEM((2, 1, kx), i32),
            pltpu.VMEM((2, 1, kx), i32),
            pltpu.VMEM((2, 1, kx), i32),
            pltpu.VMEM((2, 5, sd, levels, cy), f32),
            pltpu.VMEM((2, 5, sd * levels, cy), f32),
            pltpu.VMEM((2, 5, sd * levels, cy), f32),
            pltpu.VMEM((2, sd, levels, cy), i32),
            pltpu.VMEM((2, sd * levels, cy), i32),
            pltpu.VMEM((2, sd, cy), f32),
            pltpu.VMEM((2, n_y, sd, cy), f32),
            pltpu.VMEM((7, sd, cy), f32),
            pltpu.VMEM((n_y, 7, sd, cy), f32),
            pltpu.VMEM((slots, cy), f32),
            pltpu.VMEM((10 * slots, cy), f32),
            pltpu.VMEM((9, slots, cy), f32),
            pltpu.VMEM((3, slots, cy), i32),
            pltpu.VMEM((levels, 9, cx, cy), f32),
            pltpu.VMEM((levels, 9, cx, cy), f32),
            pltpu.VMEM((2, 2, sd * levels, cy), f32),
            pltpu.VMEM((3, levels, cx, cy), f32),
            pltpu.VMEM((levels, cx, cy), f32),
            dma((5,)), dma((1,)), dma((7,)), pltpu.SemaphoreType.REGULAR,
        ],
        compiler_params=pltpu.CompilerParams(collective_id=0, has_side_effects=True),
    )(moist, warm, *flat, size, mult, dry, east, north, perm, lx, ly, lc)
    outs = pl.pallas_call(
        publish,
        out_shape=tuple(jax.ShapeDtypeStruct(*s) for s in shapes),
        in_specs=[vmem_space] * 6,
        out_specs=[any_space] * 6,
        scratch_shapes=[pltpu.VMEM((total, cy), f32), dma],
    )(*[pltpu.with_memory_space_constraint(x, pltpu.VMEM) for x in outs])
    return (
        outs[0], outs[1], outs[2].reshape(size.shape), outs[3].reshape(size.shape), outs[4], outs[5],
    )


def solution(mesh):
    cell, drop, lists = P(None, "gx", "gy"), P(None, None, "gx", "gy"), P("gx", None, "gy")
    return jax.shard_map(
        functools.partial(per_device, mesh.shape["gx"], mesh.shape["gy"]),
        mesh=mesh,
        in_specs=(cell,) * 2 + (drop,) * 6 + (lists,) * 3,
        out_specs=(cell, cell, drop, drop, cell, P("gx", "gy")),
        check_vma=False,
    )
```

```python
import functools
import math

import jax
import jax.numpy as jnp
from jax import lax
from jax.experimental import pallas as pl
from jax.experimental.pallas import tpu as pltpu
from jax.sharding import PartitionSpec as P

NEWTON = 4
MIX_HORIZONTAL = 0.2
MIX_VERTICAL = 0.05
EXCESS_FACTOR = 4.2222
CURVATURE = 0.0012
KAPPA_SOLUTE = 0.6
GROWTH_STEP = 200.0
COLLIDE_RATE = 4e-07
VAPOUR_PER_SOURCE = 0.001
WARMING_FACTOR = 0.00249
LOG2E = math.log2(math.e)

MESH = pl.DeviceIdType.MESH
SHIFTS = (-1, 0, 1)
SIDES = (1, -1)
MOVES = (1, -1)


def div(x, n):
    return lax.shift_right_arithmetic(x, jnp.int32(n.bit_length() - 1))


def mod(x, n):
    return lax.bitwise_and(x, jnp.int32(n - 1))


def iota(shape, dim):
    return lax.broadcasted_iota(jnp.int32, shape, dim)


def turn(x, shift, dim):
    shift %= x.shape[dim]
    return pltpu.roll(x, shift, dim) if shift else x


def take(x, index, dim):
    return jnp.take_along_axis(x, index, axis=dim)


def kernel_weights(offset):
    return {
        -1: jnp.maximum(0.5 - offset, 0.0),
        0: 1.0 - jnp.abs(offset - 0.5),
        1: jnp.maximum(offset - 0.5, 0.0),
    }


def prepare(radius, dry):
    inverse = 1.0 / radius
    square = inverse * inverse
    lowest = dry * dry
    strength = (1.5 * GROWTH_STEP * KAPPA_SOLUTE) * (lowest * dry)
    pull = strength * (square * inverse)
    area = radius * radius
    return (
        area - (GROWTH_STEP * CURVATURE) * inverse,
        (5.0 / 3.0) * pull,
        1.0 + pull * square,
        strength,
        lowest,
        area * radius,
    )


def settle(level, top, bottom, strength, lowest):
    above = jnp.maximum(level + top, lowest * bottom)
    flat = lax.rsqrt(above * bottom)
    for sweep in range(NEWTON - 1):
        inverse_root = bottom * flat
        square = inverse_root * inverse_root
        pull = strength * (square * inverse_root)
        bottom = 1.0 + pull * square
        above = jnp.maximum(level + (5.0 / 3.0) * pull, lowest * bottom)
        flat = lax.rsqrt(above * bottom)
    root = above * flat
    return root, (root * root) * root


def differences(near):
    centre = near[0, 0]
    terms = {(0, 0): centre}
    for s in SIDES:
        terms[s, 0] = near[s, 0] - centre
        terms[0, s] = near[0, s] - centre
    for a in SIDES:
        for b in SIDES:
            terms[a, b] = near[a, b] - near[a, 0] - terms[0, b]
    return terms


def interpolate(terms, east, north, reach_x, reach_y):
    right, up = east > 0.5, north > 0.5
    slope_x = jnp.where(right, terms[1, 0], terms[-1, 0])
    slope_y = jnp.where(up, terms[0, 1], terms[0, -1])
    twist = jnp.where(
        right, jnp.where(up, terms[1, 1], terms[1, -1]), jnp.where(up, terms[-1, 1], terms[-1, -1])
    )
    return terms[0, 0] + reach_x * slope_x + reach_y * (slope_y + reach_x * twist)


def match(weight, other, first):
    big = (weight > other) | ((weight == other) & first)
    rate = (-COLLIDE_RATE * LOG2E) * jnp.where(big, weight, other)
    return rate, jnp.where(big, other, 0.0)


def collide(radius, cube, other, rate, eaten):
    total = radius + other
    chance = 1.0 - jnp.exp2(rate * (total * total) * (total * jnp.abs(radius - other)))
    volume = cube + chance * (other * other * other)
    merged = jnp.exp2(jnp.log(volume) * (LOG2E / 3.0))
    return jnp.where(eaten > 0.0, radius, merged), chance * eaten


def spread(parts, dim, index):
    size = parts[0].shape[dim]
    back, ahead = turn(parts[-1], -1, dim), turn(parts[1], 1, dim)
    return parts[0] + jnp.where(index == size - 1, 0.0, back) + jnp.where(index == 0, 0.0, ahead)


def body(
    sizes,
    moist_in, warm_in, size_in, mult_in, dry_in, east_in, north_in, perm_in,
    size_cells, mult_cells, dry_cells, east_cells, north_cells, perm_cells,
    lx_in, ly_in, lc_in,
    moist_out, warm_out, size_out, mult_out, rec_out, box_out,
    state, drops, perm, ly, lc,
    state_x, state_y, diag_in, list_pack, list_sort, list_x,
    row_pack, row_sort, row_x, turn_pack, rank_of, corner_pack, corner_in, col_pack, col_in,
    mask, ready, share, bits, near, near_up, late_x, fall, brink_fall,
    in_sem, send_sem, recv_sem, lower_in,
):
    levels, cx, cy, sd, kx, ky, kc, nx, ny = sizes
    me_x = lax.axis_index("gx")
    me_y = lax.axis_index("gy")
    ys = (1,) if ny == 2 else (1, -1)
    half = cx // 2
    rows = sd * levels
    slots_all = rows * cx
    block = cx * cy
    tall = levels * cx
    deep = kx // cy
    edges = (cx - 1, 0)
    bands = (pl.ds(cx - 3, 3), pl.ds(0, 3))

    def at(d):
        return (lax.rem(me_x + d[0] + nx, nx), lax.rem(me_y + d[1] + ny, ny))

    def wait_rows(count, sem):
        whole = ready.at[pl.ds(0, count), :]
        pltpu.make_async_copy(whole, whole, sem).wait()

    def count_rows(ref):
        total = 1
        for n in ref.shape:
            total *= n
        return total // cy

    brought = [0, 0, 0]

    def bring(source, target, group):
        pltpu.make_async_copy(source, target, in_sem.at[group]).start()
        brought[group] += count_rows(target)

    cells = (size_cells, dry_cells, east_cells, north_cells, mult_cells)

    def bring_rows(s, chosen, group):
        for n in chosen:
            for l in range(levels):
                stretch = pl.ds(l * sd, sd)
                if n < 5:
                    bring(cells[n].at[:, l, edges[s], :], row_pack.at[s, n, stretch, :], group)
                else:
                    bring(perm_cells.at[:, l, edges[s], :], turn_pack.at[s, stretch, :], group)

    bring_rows(0, (5, 0, 1), 1)
    bring_rows(0, (2, 3, 4), 2)
    bring(lx_in.at[0, pl.ds(0, 1), :], list_pack.at[0], 2)
    bring(moist_in, state.at[0], 0)
    bring(warm_in, state.at[1], 0)

    beside = [0] + list(ys)
    barrier = pltpu.get_barrier_semaphore()
    for d in [(-1, dy) for dy in beside] + [(0, dy) for dy in ys]:
        pl.semaphore_signal(barrier, inc=1, device_id=at(d), device_id_type=MESH)

    bring_rows(1, range(6), 0)
    bring(lx_in.at[0, pl.ds(1, 1), :], list_pack.at[1], 0)
    corner_list = pltpu.make_async_copy(lc_in.at[0], lc, in_sem.at[3])
    corner_list.start()
    face_list = pltpu.make_async_copy(ly_in.at[0], ly, in_sem.at[1])

    for n, source in enumerate((size_in, mult_in, dry_in, east_in, north_in)):
        bring(source, drops.at[n], 0)
    bring(perm_in, perm, 0)

    sent = [0]
    due = [0] * 7

    def send(source, target, group, d):
        pltpu.make_async_remote_copy(
            src_ref=source, dst_ref=target, send_sem=send_sem.at[0], recv_sem=recv_sem.at[group],
            device_id=at(d), device_id_type=MESH,
        ).start()
        sent[0] += count_rows(source)
        due[group] += count_rows(source)

    line = iota((cx, cy), 0)
    lane = iota((cx, cy), 1)
    low_half = line < half

    def send_fields(s):
        own, far = state.at[:, :, bands[s], :], MOVES[s]
        group = (1, 0)[s]
        send(own, state_x.at[s, :, :, bands[s], :], group, (far, 0))
        for t, dy in enumerate(ys):
            send(own, diag_in.at[s, t, :, :, bands[s], :], group, (far, dy))

    seat = iota((sd, cy), 0)

    def look_up(load_row, row, column):
        groups = 2
        found = [None] * groups
        for m in range(rows // groups):
            for n in range(groups):
                r = n * (rows // groups) + m
                value = take(jnp.broadcast_to(load_row(r), (deep, cy)), column, 1)
                found[n] = value if m == 0 else jnp.where(row == r, value, found[n])
        while len(found) > 1:
            size = rows // len(found)
            odd = mod(div(row, size), 2) == 1
            found = [jnp.where(odd, found[2 * m + 1], found[2 * m]) for m in range(len(found) // 2)]
        return found[0]

    def sort_rows(s, chosen):
        for l in range(levels):
            stretch = pl.ds(l * sd, sd)
            turns = turn_pack[s, stretch, :]
            for n in chosen:
                row_sort[s, n, stretch, :] = take(row_pack[s, n, stretch, :], turns, 0)

    def send_first(s):
        sort_rows(s, (0, 1))
        send(row_sort.at[s, 0:2], row_x.at[s, 0:2], (4, 3)[s], (MOVES[s], 0))

    def send_rows(s):
        sort_rows(s, (2, 3, 4))
        send(row_sort.at[s, 2:4], row_x.at[s, 2:4], (4, 3)[s], (MOVES[s], 0))
        send(row_sort.at[s, 4], row_x.at[s, 4], (5, 3)[s], (MOVES[s], 0))
        for l in range(levels):
            rank = jnp.zeros((sd, cy), jnp.int32)
            for p in range(1, sd):
                here = jnp.broadcast_to(turn_pack[s, l * sd + p : l * sd + p + 1, :], (sd, cy)) == seat
                rank = jnp.where(here, p, rank)
            rank_of[s, pl.ds(l * sd, sd), :] = rank
        slots = list_pack[s].reshape(deep, cy)
        k = div(slots, block * levels)
        row = mod(div(slots, block), levels) * sd + k
        place = look_up(lambda r: rank_of[s, r : r + 1, :], row, mod(slots, cy))
        moved = jnp.where(slots >= 0, slots + (place - k) * (block * levels), -1)
        list_sort[s] = moved.reshape(1, kx)
        send(list_sort.at[s], list_x.at[s], (6, 3)[s], (MOVES[s], 0))

    def send_corner(s):
        tile = None
        for n in range(6):
            for l in range(levels):
                stretch = pl.ds(l * sd, sd)
                value = row_pack[s, n, stretch, :] if n < 5 else turn_pack[s, stretch, :].astype(jnp.float32)
                spot = 8 * n + 4 * s + 2 * l
                moved = turn(value, spot + 1, 1)
                tile = moved if tile is None else jnp.where(lane >= spot, moved, tile)
        corner_pack[s] = tile
        for d in range(2):
            spot = 2 * ky + kc * (2 * d + s)
            corner_pack[s, 2 * s + d : 2 * s + d + 1, spot : spot + kc] = lc[
                2 * s + d : 2 * s + d + 1, :
            ].astype(jnp.float32)
        for t, dy in enumerate(ys):
            send(corner_pack.at[s], corner_in.at[s, t], 2, (MOVES[s], dy))

    pl.semaphore_wait(barrier, len(beside) + len(ys))
    for dy in beside:
        for f, source in enumerate((moist_in, warm_in)):
            target = state_x.at[0] if dy == 0 else diag_in.at[0, ys.index(dy)]
            send(source.at[:, bands[0], :], target.at[f, :, bands[0], :], 1, (1, dy))
    for dy in beside:
        pl.semaphore_signal(lower_in, inc=1, device_id=at((1, dy)), device_id_type=MESH)
    wait_rows(brought[1], in_sem.at[1])
    send_first(0)
    face_list.start()
    wait_rows(brought[2], in_sem.at[2])
    send_rows(0)
    corner_list.wait()
    send_corner(0)
    wait_rows(brought[0], in_sem.at[0])
    for t, dy in enumerate(ys):
        send(state, state_y.at[t], 0, (0, dy))
    attributes = (0, 2, 3, 4, 1)
    for n in range(6):
        tile = None
        for i in range(cx):
            for l in range(levels):
                picked = pl.ds(l * cx + i, sd, stride=tall)
                value = drops[attributes[n], picked, :] if n < 5 else perm[picked, :].astype(jnp.float32)
                spot = 4 * i + 2 * l
                moved = turn(value, spot + 1, 1)
                tile = moved if tile is None else jnp.where(lane >= spot, moved, tile)
        col_pack[n] = tile
    face_list.wait()
    for d in range(2):
        col_pack[6, d : d + 1, d * ky : (d + 1) * ky] = ly[d : d + 1, :].astype(jnp.float32)
    for t, dy in enumerate(ys):
        send(col_pack, col_in.at[t], 2, (0, dy))

    def span(n, k):
        return pl.ds(n * slots_all + k * tall, tall)

    order = [perm[k * tall : (k + 1) * tall, :] for k in range(sd)]
    for m in range(sd):
        part = pl.ds(m * tall, tall)
        weight = drops[1, part, :]
        partner = jnp.zeros((tall, cy), jnp.int32)
        first = jnp.zeros((tall, cy), jnp.int32)
        for p in range(sd):
            mine = order[p] == m
            partner = jnp.where(mine, order[p ^ 1], partner)
            if p % 2 == 0:
                first = jnp.where(mine, 1, first)
        other = drops[1, pl.ds(0, tall), :]
        for k in range(1, sd):
            other = jnp.where(partner == k, drops[1, pl.ds(k * tall, tall), :], other)
        rate, eaten = match(weight, other, first > 0)
        for n in range(3):
            bits[n, part, :] = mod(lax.shift_right_logical(partner, jnp.int32(n)), 2)
        for n, value in enumerate(prepare(drops[0, part, :], drops[2, part, :])):
            ready[span(n, m), :] = value
        east, north = drops[3, part, :], drops[4, part, :]
        ready[span(6, m), :] = jnp.abs(east - 0.5)
        ready[span(7, m), :] = jnp.abs(north - 0.5)
        ready[span(8, m), :] = rate
        ready[span(9, m), :] = eaten
        wx, wy = kernel_weights(east), kernel_weights(north)
        for a in SHIFTS:
            along = wx[a] * weight
            for b in SHIFTS:
                share[3 * a + b + 4, part, :] = wy[b] * along

    mask[...] = jnp.ones_like(mask)
    for r, side in enumerate(edges):
        slots = list_pack[r]
        hot_row = iota((rows, kx), 0) == div(slots, block)
        hot_lane = jnp.where(iota((cy, kx), 0) == mod(slots, cy), 1.0, 0.0).astype(jnp.bfloat16)
        named = lax.dot_general(
            jnp.where(hot_row, 1.0, 0.0).astype(jnp.bfloat16), hot_lane,
            (((1,), (1,)), ((), ())), preferred_element_type=jnp.float32,
        )
        mask[pl.ds(side, rows, stride=cx), :] = 1.0 - named

    width = 2 * ky + 4 * kc
    lane_e = iota((1, width), 1)
    high = (lane_e < ky) | ((lane_e >= 2 * ky) & (lane_e < 2 * ky + 2 * kc))
    high_all = jnp.broadcast_to(high, (slots_all, width))
    slots = jnp.concatenate(
        [ly[0:1, :], ly[1:2, :], lc[0:1, :], lc[2:3, :], lc[1:2, :], lc[3:4, :]], 1
    )
    hot_e = jnp.where(iota((slots_all, width), 0) == div(slots, cy), 1.0, 0.0)
    left_high = jnp.max(jnp.where(high_all, hot_e, 0.0), 1, keepdims=True)
    left_low = jnp.max(jnp.where(high_all, 0.0, hot_e), 1, keepdims=True)
    lane_all = iota((slots_all, cy), 1)
    mask[...] = mask[...] * (
        1.0 - jnp.where(lane_all == cy - 1, left_high, jnp.where(lane_all == 0, left_low, 0.0))
    )

    def land(slots, move_x, move_y):
        level = mod(div(slots, block), levels)
        i = mod(mod(div(slots, cy), cx) + move_x, cx)
        target = (level * cx + i) * cy + mod(mod(slots, cy) + move_y, cy)
        return jnp.where(slots >= 0, target, -1)

    def blend(parts, pick_second):
        return parts[0] if len(parts) == 1 else jnp.where(pick_second, parts[1], parts[0])

    left_lanes = lane < cy // 2
    odd_lane = mod(lane, 2) == 1
    group = div(lane, 4)
    keys = [(a, b) for a in SHIFTS for b in SHIFTS]

    def climate(fields):
        deep_lane = iota(fields[0][0][0].shape, 1)
        odd = mod(deep_lane, 2) == 1

        def fixed(value, spot):
            return take(value, jnp.full(value.shape, spot, jnp.int32), 1)

        def reach(own, other, s):
            if s == 0:
                return own
            inside = deep_lane < cy - s if s > 0 else deep_lane >= -s
            return jnp.where(inside, turn(own, -s, 1), turn(other, -s, 1))

        def brink(own, other, s):
            if s == 0:
                return take(other, jnp.where(odd, 0, cy - 1), 1)
            if s > 0:
                return jnp.where(odd, fixed(other, s), fixed(own, s - 1))
            return jnp.where(odd, fixed(own, cy + s), fixed(other, cy - 1 + s))

        def humidity(cut):
            raw = [[{s: cut(*fields[f][l], s) for s in range(-2, 3)} for l in range(levels)] for f in range(2)]
            mixed = []
            for f in range(2):
                mixed.append([])
                for l in range(levels):
                    at_shift = {}
                    for b in SHIFTS:
                        centre = raw[f][l][b]
                        around = raw[f][l][b - 1] + raw[f][l][b + 1] + (turn(centre, -1, 0) + turn(centre, 1, 0))
                        stacked = raw[f][min(l + 1, levels - 1)][b] + raw[f][max(l - 1, 0)][b]
                        at_shift[b] = (
                            (1.0 - 4.0 * MIX_HORIZONTAL - 2.0 * MIX_VERTICAL) * centre
                            + MIX_HORIZONTAL * around + MIX_VERTICAL * stacked
                        )
                    mixed[f].append(at_shift)
            humid = []
            for l in range(levels):
                humid.append({})
                for b in SHIFTS:
                    warmth = mixed[1][l][b]
                    decay = jnp.exp2((-17.27 * LOG2E) * (warmth - 273.15) / (warmth - 35.86))
                    humid[l][b] = (GROWTH_STEP / EXCESS_FACTOR) * (mixed[0][l][b] * decay) - GROWTH_STEP
            return mixed, humid

        mixed, humid = humidity(reach)
        terms = [differences({(a, b): turn(humid[l][b], -a, 0) for a, b in keys}) for l in range(levels)]
        _, column = humidity(brink)
        wide_level = mod(div(deep_lane, 2), 2) == 1
        column = {b: jnp.where(wide_level, column[1][b], column[0][b]) for b in SHIFTS}
        return mixed, terms, column

    def from_row(value, a):
        return take(value, mod(group + a, cx), 0)

    def mate(weight, turns):
        rank = jnp.zeros((sd, cy), jnp.int32)
        for p in range(1, sd):
            rank = jnp.where(jnp.broadcast_to(turns[p : p + 1], (sd, cy)) == seat, p, rank)
        partner = take(turns, rank ^ 1, 0)
        return partner, match(weight, take(weight, partner, 0), mod(rank, 2) == 0)

    def expand(prepared, east, north, around):
        base, top, bottom, strength, lowest, cube = prepared
        level = base + interpolate(around, east, north, jnp.abs(east - 0.5), jnp.abs(north - 0.5))
        root, volume = settle(level, top, bottom, strength, lowest)
        return root, volume, volume - cube

    across_pair = seat ^ 1

    def pair(weight):
        return across_pair, match(weight, take(weight, across_pair, 0), mod(seat, 2) == 0)

    def merge(root, volume, weight, mated):
        partner, (rate, eaten) = mated
        after, lost = collide(root, volume, take(root, partner, 0), rate, eaten)
        return after, weight - lost

    def surround(ref, l, r):
        return {key: jnp.broadcast_to(ref[l, n, r : r + 1, :], (sd, cy)) for n, key in enumerate(keys)}

    def side_growth(s):
        ref, r = ((near, cx - 1), (near_up, 0))[s]
        found = []
        for l in range(levels):
            radius, dry, east, north = (row_x[s, n, pl.ds(l * sd, sd), :] for n in range(4))
            found.append(expand(prepare(radius, dry), east, north, surround(ref, l, r)))
        return found

    def side_rows(s, found):
        home = (0, cx - 1)[s]
        for l in range(levels):
            stretch = pl.ds(l * sd, sd)
            root, volume, gain = found[l]
            weight = row_x[s, 4, stretch, :]
            radius, weight_left = merge(root, volume, weight, pair(weight))
            late_x[s, 0, stretch, :] = radius
            late_x[s, 1, stretch, :] = weight_left
            wx, wy = kernel_weights(row_x[s, 2, stretch, :]), kernel_weights(row_x[s, 3, stretch, :])
            along = wx[MOVES[s]] * (weight * gain)
            for b in SHIFTS:
                fall[b + 1, l, home : home + 1, :] += jnp.sum(wy[b] * along, 0, keepdims=True)

    def side_records(s):
        slots = list_x[s].reshape(deep, cy)
        level = mod(div(slots, block), levels)
        live = slots >= 0
        row = level * sd + div(slots, block * levels)
        column = mod(slots, cy)
        fields = [(2, row_x, 1), (3, row_x, 2), (4, row_x, 3), (0, late_x, 0), (1, late_x, 1)]
        for n, source, from_n in fields:
            got = look_up(lambda r: source[s, from_n, r : r + 1, :], row, column)
            rec_out[n, :, pl.ds(s * kx, kx)] = jnp.where(live, got, 0.0).reshape(1, kx)
        box_out[:, pl.ds(s * kx, kx)] = land(slots, MOVES[s], 0).reshape(1, kx)

    pl.semaphore_wait(lower_in, len(beside))
    send_fields(1)
    send_first(1)
    send_rows(1)
    send_corner(1)

    wait_rows(due[0], recv_sem.at[0])
    fields = []
    for f in range(2):
        fields.append([])
        for l in range(levels):
            side_y = blend([state_y[t, f, l] for t in range(len(ys))], left_lanes)
            far = blend([diag_in[1, t, f, l] for t in range(len(ys))], left_lanes)
            fields[f].append(
                (jnp.concatenate([state[f, l], state_x[1, f, l]], 0), jnp.concatenate([side_y, far], 0))
            )
    mixed, terms, column = climate(fields)
    window = {key: jnp.concatenate([t[key][:cx] for t in terms], 0) for key in keys}
    for l in range(levels):
        for n, key in enumerate(keys):
            near_up[l, n] = terms[l][key][cx:]
        moist_out[l] = mixed[0][l][0][:cx]
        warm_out[l] = mixed[1][l][0][:cx]
    inside = {
        (a, b): jnp.where(
            mod(group + a, cy // 4) < cx, from_row(column[b][:cx], a), from_row(column[b][cx:], a)
        )
        for a, b in keys
    }

    grown = []
    cubes = []
    deposit = {}
    for k in range(sd):
        part = pl.ds(k * tall, tall)
        base, top, bottom, strength, lowest, cube, reach_x, reach_y = (ready[span(n, k), :] for n in range(8))
        level = base + interpolate(window, drops[3, part, :], drops[4, part, :], reach_x, reach_y)
        root, volume = settle(level, top, bottom, strength, lowest)
        gain = volume - cube
        for a, b in keys:
            term = share[3 * a + b + 4, part, :] * gain
            deposit[a, b] = term if k == 0 else deposit[a, b] + term
        grown.append(root)
        cubes.append(volume)

    for l in range(levels):
        for b in SHIFTS:
            parts = {a: jnp.where(line < 2, 0.0, deposit[a, b][l * cx : (l + 1) * cx]) for a in SHIFTS}
            fall[b + 1, l] = spread(parts, 0, line)

    for m in range(sd):
        part = pl.ds(m * tall, tall)
        found = grown
        for n in range(3):
            odd = bits[n, part, :] > 0
            found = [jnp.where(odd, found[2 * i + 1], found[2 * i]) for i in range(len(found) // 2)]
        radius, lost = collide(grown[m], cubes[m], found[0], ready[span(8, m), :], ready[span(9, m), :])
        size_out[part, :] = radius
        mult_out[part, :] = mask[part, :] * (drops[1, part, :] - lost)

    def upper_side():
        wait_rows(due[3], recv_sem.at[3])
        side_rows(1, side_growth(1))
        side_records(1)

    pl.when(me_x != nx - 1)(upper_side)

    redo = [(l, i) for l in range(levels) for i in range(2)]
    waiting = {}
    for l, i in redo:
        picked = pl.ds(l * cx + i, sd, stride=tall)
        radius, weight, dry, east, north = (drops[n, picked, :] for n in range(5))
        waiting[l, i] = (
            prepare(radius, dry), weight, east, north, mate(weight, perm[picked, :]), mask[picked, :]
        )

    wait_rows(due[1], recv_sem.at[1])
    fields = []
    for f in range(2):
        fields.append([])
        for l in range(levels):
            side_y = blend([state_y[t, f, l] for t in range(len(ys))], left_lanes)
            far = blend([diag_in[0, t, f, l] for t in range(len(ys))], left_lanes)
            fields[f].append(
                (jnp.where(low_half, state[f, l], state_x[0, f, l]), jnp.where(low_half, side_y, far))
            )
    mixed, terms, column = climate(fields)
    for l in range(levels):
        for n, key in enumerate(keys):
            near[l, n] = terms[l][key]
        moist_out[l, 0:1, :] = mixed[0][l][0][0:1]
        warm_out[l, 0:1, :] = mixed[1][l][0][0:1]
    col_terms = differences(
        {
            (a, b): jnp.where(mod(group + a + 2, cy // 4) < 4, from_row(column[b], a), inside[a, b])
            for a, b in keys
        }
    )
    for l in range(levels):
        landing = [None] * 3
        for i in range(2):
            picked = pl.ds(l * cx + i, sd, stride=tall)
            prepared, weight, east, north, mated, keep = waiting[l, i]
            root, volume, gain = expand(prepared, east, north, surround(near, l, i))
            radius, weight_left = merge(root, volume, weight, mated)
            size_out[picked, :] = radius
            mult_out[picked, :] = keep * weight_left
            wx, wy = kernel_weights(east), kernel_weights(north)
            for a in SHIFTS:
                if i + a < 0:
                    continue
                along = wx[a] * (weight * gain)
                parts = {b: wy[b] * along for b in SHIFTS}
                if landing[i + a] is not None:
                    parts = {b: parts[b] + landing[i + a][b] for b in SHIFTS}
                landing[i + a] = parts
        for r in range(3):
            for b in SHIFTS:
                fall[b + 1, l, r : r + 1, :] += jnp.sum(landing[r][b], 0, keepdims=True)

    pl.when(me_x == nx - 1)(upper_side)

    def columns():
        wait_rows(due[2], recv_sem.at[2])
        corner = [blend([corner_in[s, t] for t in range(len(ys))], odd_lane) for s in range(2)]
        values = []
        for n in range(6):
            beside = blend([col_in[t, n] for t in range(len(ys))], odd_lane)
            below = jnp.where(lane < 4 * cx, beside, turn(corner[1], 4 * (cx - 1) - 8 * n, 1))
            values.append(jnp.where(lane >= cy - 4, turn(corner[0], cy - 4 - 8 * n, 1), below))
        radius, dry, east, north, weight, turns = values
        root, volume, gain = expand(prepare(radius, dry), east, north, col_terms)
        radius, weight_left = merge(root, volume, weight, mate(weight, turns.astype(jnp.int32)))
        wx, wy = kernel_weights(east), kernel_weights(north)
        across = jnp.where(odd_lane, wy[-1], wy[1]) * (weight * gain)
        rain = {a: jnp.broadcast_to(jnp.sum(wx[a] * across, 0, keepdims=True), (cx, cy)) for a in SHIFTS}
        outer = jnp.where(lane == cy - 1, 1, 0)
        for l in range(levels):
            sent_in = sum(take(rain[a], mod(4 * (line - a) + 2 * l + outer, cy), 1) for a in SHIFTS)
            brink_fall[l] = jnp.where((lane == 0) | (lane == cy - 1), sent_in, 0.0)

        which = div(lane_e - 2 * ky, kc)
        minus_x = mod(which, 2)
        face = lane_e < 2 * ky
        minus_y = jnp.where(face, jnp.where(lane_e < ky, 0, 1), div(which, 2))
        slots = None
        for d in range(2):
            t = d if len(ys) == 2 else 0
            faces = col_in[t, 6, d : d + 1, :]
            corners = [corner_in[s, t, 2 * s + d : 2 * s + d + 1, :] for s in range(2)]
            found = jnp.where(face, faces, jnp.where(minus_x == 0, corners[0], corners[1]))
            slots = found if d == 0 else jnp.where(minus_y == 0, slots, found)
        slots = slots.astype(jnp.int32)
        move_x = jnp.where(face, 0, 1 - 2 * minus_x)
        live = slots >= 0
        level = mod(div(slots, block), levels)
        place = jnp.where(face, mod(div(slots, cy), cx), jnp.where(minus_x == 0, cy // 4 - 1, cx))
        spot = jnp.broadcast_to(jnp.where(live, 4 * place + 2 * level + minus_y, 0), (sd, width))
        chosen = iota((sd, width), 0) == jnp.where(live, div(slots, block * levels), -1)
        for n, value in enumerate((radius, weight_left, dry, east, north)):
            rec_out[n, :, pl.ds(2 * kx, width)] = jnp.sum(jnp.where(chosen, take(value, spot, 1), 0.0), 0, keepdims=True)
        box_out[:, pl.ds(2 * kx, width)] = land(slots, move_x, 1 - 2 * minus_y)

    def rows_below():
        wait_rows(due[4], recv_sem.at[4])
        side = side_growth(0)
        wait_rows(due[5], recv_sem.at[5])
        side_rows(0, side)
        wait_rows(due[6], recv_sem.at[6])
        side_records(0)

    def total_up():
        for l in range(levels):
            total = spread({b: fall[b + 1, l] for b in SHIFTS}, 1, lane) + brink_fall[l]
            moist_out[l] = moist_out[l] - VAPOUR_PER_SOURCE * total
            warm_out[l] = warm_out[l] + WARMING_FACTOR * total

    @pl.when(me_y == 0)
    def _():
        columns()
        rows_below()
        total_up()

    @pl.when(me_y != 0)
    def _():
        rows_below()
        columns()
        total_up()

    wait_rows(sent[0], send_sem.at[0])


def publish(*refs):
    whole, sem = refs[-2:]
    count = len(refs) // 2 - 1
    for n in range(count):
        pltpu.make_async_copy(refs[n], refs[count + n], sem).start()
    pltpu.make_async_copy(whole, whole, sem).wait()


def per_device(nx, ny, moist, warm, size, mult, dry, east, north, perm, lx, ly, lc):
    levels, cx, cy = moist.shape
    sd = size.shape[0]
    kx, ky, kc = lx.shape[2], ly.shape[2], lc.shape[2]
    narr = 2 * kx + 2 * ky + 4 * kc
    slots = sd * levels * cx
    flat = [x.reshape(slots, cy) for x in (size, mult, dry, east, north, perm)]
    f32, i32 = jnp.float32, jnp.int32
    any_space = pl.BlockSpec(memory_space=pl.ANY)
    vmem_space = pl.BlockSpec(memory_space=pltpu.VMEM)
    dma = pltpu.SemaphoreType.DMA
    shapes = (
        ((levels, cx, cy), f32),
        ((levels, cx, cy), f32),
        ((slots, cy), f32),
        ((slots, cy), f32),
        ((5, 1, narr), f32),
        ((1, narr), i32),
    )
    n_y = 1 if ny == 2 else 2
    total = 2 * levels * cx + 2 * slots + 6 * narr // cy
    outs = pl.pallas_call(
        functools.partial(body, (levels, cx, cy, sd, kx, ky, kc, nx, ny)),
        out_shape=tuple(pltpu.VMEM(*s) for s in shapes),
        in_specs=[any_space] * 17,
        out_specs=[vmem_space] * 6,
        scratch_shapes=[
            pltpu.VMEM((2, levels, cx, cy), f32),
            pltpu.VMEM((5, slots, cy), f32),
            pltpu.VMEM((slots, cy), i32),
            pltpu.VMEM((2, ky), i32),
            pltpu.VMEM((4, kc), i32),
            pltpu.VMEM((2, 2, levels, cx, cy), f32),
            pltpu.VMEM((n_y, 2, levels, cx, cy), f32),
            pltpu.VMEM((2, n_y, 2, levels, cx, cy), f32),
            pltpu.VMEM((2, 1, kx), i32),
            pltpu.VMEM((2, 1, kx), i32),
            pltpu.VMEM((2, 1, kx), i32),
            pltpu.VMEM((2, 5, sd * levels, cy), f32),
            pltpu.VMEM((2, 5, sd * levels, cy), f32),
            pltpu.VMEM((2, 5, sd * levels, cy), f32),
            pltpu.VMEM((2, sd * levels, cy), i32),
            pltpu.VMEM((2, sd * levels, cy), i32),
            pltpu.VMEM((2, sd, cy), f32),
            pltpu.VMEM((2, n_y, sd, cy), f32),
            pltpu.VMEM((7, sd, cy), f32),
            pltpu.VMEM((n_y, 7, sd, cy), f32),
            pltpu.VMEM((slots, cy), f32),
            pltpu.VMEM((10 * slots, cy), f32),
            pltpu.VMEM((9, slots, cy), f32),
            pltpu.VMEM((3, slots, cy), i32),
            pltpu.VMEM((levels, 9, cx, cy), f32),
            pltpu.VMEM((levels, 9, cx, cy), f32),
            pltpu.VMEM((2, 2, sd * levels, cy), f32),
            pltpu.VMEM((3, levels, cx, cy), f32),
            pltpu.VMEM((levels, cx, cy), f32),
            dma((4,)), dma((1,)), dma((7,)), pltpu.SemaphoreType.REGULAR,
        ],
        compiler_params=pltpu.CompilerParams(collective_id=0, has_side_effects=True),
    )(moist, warm, *flat, size, mult, dry, east, north, perm, lx, ly, lc)
    outs = pl.pallas_call(
        publish,
        out_shape=tuple(jax.ShapeDtypeStruct(*s) for s in shapes),
        in_specs=[vmem_space] * 6,
        out_specs=[any_space] * 6,
        scratch_shapes=[pltpu.VMEM((total, cy), f32), dma],
    )(*[pltpu.with_memory_space_constraint(x, pltpu.VMEM) for x in outs])
    return (
        outs[0], outs[1], outs[2].reshape(size.shape), outs[3].reshape(size.shape), outs[4], outs[5],
    )


def solution(mesh):
    cell, drop, lists = P(None, "gx", "gy"), P(None, None, "gx", "gy"), P("gx", None, "gy")
    return jax.shard_map(
        functools.partial(per_device, mesh.shape["gx"], mesh.shape["gy"]),
        mesh=mesh,
        in_specs=(cell,) * 2 + (drop,) * 6 + (lists,) * 3,
        out_specs=(cell, cell, drop, drop, cell, P("gx", "gy")),
        check_vma=False,
    )
```
